32 devices in a mesh: dp: 8 (over y, x, core), seq: 4 (over z).
Axes of the slice: x: 2, y: 2, z: 4, core: 2. Of those that a mesh axis runs over, the one named last changes fastest.
Arguments:
- image_in: bfloat16 [8, 1024, 1536], P('dp', 'seq'), may hold values from -16 to 16
- text_input: bfloat16 [8, 128, 1536], P('dp', 'seq'), may hold values from -16 to 16
- condition: bfloat16 [8, 1536], P(None, ('dp', 'seq')), may hold values from -6 to 6
- ada_weight: bfloat16 [2, 2, 1536, 9216], P(None, None, ('dp', 'seq')), may hold values from -0.15625 to 0.15625
- qkv_weight: bfloat16 [2, 2, 1536, 3, 1536], P(None, None, 'dp', None, 'seq'), as said below
- out_weight: bfloat16 [2, 2, 1536, 1536], P(None, None, 'seq', 'dp'), may hold values from -2.5 to 2.5
- up_weight: bfloat16 [2, 2, 1536, 6144], P(None, None, 'dp', 'seq'), may hold values from -0.15625 to 0.15625
- down_weight: bfloat16 [2, 2, 6144, 1536], P(None, None, 'seq', 'dp'), may hold values from -0.078125 to 0.078125
- norm_gain: bfloat16 [2, 2, 2, 64], replicated, may hold values from 0.5 to 5
- image_cotangent: bfloat16 [8, 1024, 1536], P('dp', 'seq'), may hold values from -6 to 6
- text_cotangent: bfloat16 [8, 128, 1536], P('dp', 'seq'), may hold values from -6 to 6
Outputs:
- image_out: bfloat16 [8, 1024, 1536], P('dp', 'seq')
- text_out: bfloat16 [8, 128, 1536], P('dp', 'seq')
- image_grad: float32 [8, 1024, 1536], P('dp', 'seq')
- text_grad: float32 [8, 128, 1536], P('dp', 'seq')
- condition_grad: float32 [8, 1536], P(None, ('dp', 'seq'))
- ada_grad: float32 [2, 2, 1536, 9216], P(None, None, ('dp', 'seq'))
- qkv_grad: float32 [2, 2, 1536, 3, 1536], P(None, None, 'dp', None, 'seq')
- out_grad: float32 [2, 2, 1536, 1536], P(None, None, 'seq', 'dp')
- up_grad: float32 [2, 2, 1536, 6144], P(None, None, 'dp', 'seq')
- down_grad: float32 [2, 2, 6144, 1536], P(None, None, 'seq', 'dp')
- gain_grad: float32 [2, 2, 2, 64], replicated
The draws below stay inside these ranges and needn't reach their ends.
Inputs may be any that keep to these rules, and one draw needn't show every extreme that they name: `qkv_weight`: each entry lies within plus or minus 4 / sqrt(1536).
All inputs are finite; a program needn't handle non-finite values.
Results may differ from the reference program's by a relative error of at most 0.03.
Values may be sent and summed in bfloat16 or wider, within the bound.
A program may use at most 384 MiB of HBM per device.

```python
import jax
import jax.numpy as jnp
from jax import lax

D = 1536
HD = 64
FF = 6144
LAYERS = 2
IMG_LEN = 1024
TXT_LEN = 128
SEQS = 8
SEQ_LEN = 1152


def scaled_tokens(key, array_shape):
    key_values, key_rows, key_columns = jax.random.split(key, 3)
    values_raw = jax.random.normal(key_values, array_shape, jnp.float32)
    row_scale = jnp.exp(jax.random.uniform(key_rows, (array_shape[0], array_shape[1], 1), jnp.float32, -1.2039728, 1.0986123))
    column_scale = jnp.exp(jax.random.uniform(key_columns, (1, 1, array_shape[2]), jnp.float32, -0.6931472, 0.6931472))
    return jnp.clip(values_raw * row_scale * column_scale, -16.0, 16.0)


def draw_image_in(key, part):
    return scaled_tokens(jax.random.fold_in(key, 1), (SEQS, IMG_LEN, D)).astype(jnp.bfloat16)


def draw_text_input(key, part):
    return scaled_tokens(jax.random.fold_in(key, 2), (SEQS, TXT_LEN, D)).astype(jnp.bfloat16)


def draw_qkv_weight(key, part):
    base_key = jax.random.fold_in(key, 3)
    key_main = jax.random.fold_in(base_key, 0)
    weights_raw = jax.random.normal(key_main, (LAYERS, 2, D, 3, D), jnp.float32)
    return (jnp.clip(weights_raw, -4.0, 4.0) * D ** (-0.5)).astype(jnp.bfloat16)


def draw_norm_gain(key, part):
    base_key = jax.random.fold_in(key, 4)
    return jax.random.uniform(base_key, (LAYERS, 2, 2, HD), jnp.float32, 0.5, 1.5).astype(jnp.bfloat16)


def steps_of(key, extent, pieces, low, top_value):
    def one(dim, shards_of):
        steps = jax.random.uniform(jax.random.fold_in(jax.random.fold_in(key, 6), dim), (shards_of,), jnp.float32, low / len(pieces), top_value / len(pieces))
        return jnp.repeat(jnp.exp(steps), extent[dim] // shards_of).reshape((-1,) + (1,) * (len(extent) - dim - 1))

    gain = one(*pieces[0])
    for cut in pieces[1:]:
        gain = gain * one(*cut)
    return gain


def noise(stream_key, dims, deviation, limit, shards=(), held_as=jnp.bfloat16):
    array = deviation * jax.random.normal(stream_key, dims, jnp.float32)
    if shards:
        array = array * steps_of(stream_key, dims, shards, -0.22, 0.18)
    return jnp.clip(array, -limit, limit).astype(held_as)


def setup_inputs(seed: int = 0) -> dict:
    arg_keys = jax.random.split(jax.random.key(seed), 12)
    image_in = draw_image_in(jax.random.fold_in(arg_keys[11], 71), 0)
    text_input = draw_text_input(jax.random.fold_in(arg_keys[11], 71), 0)
    condition = noise(arg_keys[2], (SEQS, D), 1.0, 6.0, ((1, 32),))
    ada_weight = noise(arg_keys[3], (LAYERS, 2, D, 6 * D), D ** -0.5, 0.15625, ((2, 32),))
    qkv_weight = draw_qkv_weight(jax.random.fold_in(arg_keys[11], 71), 0)
    out_weight = noise(arg_keys[5], (LAYERS, 2, D, D), (max(1, 4 * D // SEQ_LEN)) ** -0.5, 2.5, ((2, 4), (3, 8)))
    up_weight = noise(arg_keys[6], (LAYERS, 2, D, FF), D ** -0.5, 0.15625, ((2, 8), (3, 4)))
    down_weight = noise(arg_keys[7], (LAYERS, 2, FF, D), FF ** -0.5, 0.078125, ((2, 4), (3, 8)))
    norm_gain = draw_norm_gain(jax.random.fold_in(arg_keys[11], 71), 0)
    image_cotangent = noise(arg_keys[9], (SEQS, IMG_LEN, D), 1.0, 6.0, ((0, 8), (1, 4)))
    text_cotangent = noise(arg_keys[10], (SEQS, TXT_LEN, D), 1.0, 6.0, ((0, 8), (1, 4)))
    return {"image_in": image_in, "text_input": text_input, "condition": condition, "ada_weight": ada_weight, "qkv_weight": qkv_weight, "out_weight": out_weight, "up_weight": up_weight, "down_weight": down_weight, "norm_gain": norm_gain, "image_cotangent": image_cotangent, "text_cotangent": text_cotangent}


@jax.custom_vjp
def low(v):
    return lax.optimization_barrier(v.astype(jnp.bfloat16)).astype(jnp.float32)

@jax.custom_vjp
def low_back(v):
    return v

def low_keep(v):
    return (low(v), None)

def low_pass(kept, grad):
    return (grad,)

def back_keep(v):
    return (v, None)

def back_low(kept, grad):
    return (low(grad),)
low.defvjp(low_keep, low_pass)
low_back.defvjp(back_keep, back_low)
EPSILON = 1e-06
HIGHEST = lax.Precision.HIGHEST

def layer_norm(values):
    average = lax.optimization_barrier(jnp.mean(values, axis=-1, keepdims=True))
    centred = values - average
    return centred * lax.rsqrt(lax.optimization_barrier(jnp.mean(centred * centred, axis=-1, keepdims=True)) + EPSILON)

def rms_scale(values, gain_row):
    return values * lax.rsqrt(lax.optimization_barrier(jnp.mean(values * values, axis=-1, keepdims=True)) + EPSILON) * gain_row

def product(left, right):
    return jnp.dot(left, right, precision=HIGHEST)

def attend(queries, key_rows, value_rows):
    scores = low_back(jnp.einsum('qhd,khd->hqk', queries, key_rows, precision=HIGHEST) * HD ** (-0.5))
    attention = low(jax.nn.softmax(scores, axis=-1))
    return jnp.einsum('hqk,khd->qhd', attention, value_rows, precision=HIGHEST)

def block(streams, modulations, qkv_layer, out_layer, up_layer, down_layer, gain_layer):
    head_count = D // HD
    prepared = []
    for token_flow in range(2):
        modulation = modulations[token_flow]
        normed = low(layer_norm(streams[token_flow]) * (1.0 + modulation[1]) + modulation[0])
        joined = low_back(product(normed, qkv_layer[token_flow].reshape(D, 3 * D)))
        joined = joined.reshape(-1, 3, head_count, HD)
        queries = low(rms_scale(joined[:, 0], gain_layer[token_flow, 0]))
        key_rows = low(rms_scale(joined[:, 1], gain_layer[token_flow, 1]))
        value_rows = low(joined[:, 2])
        prepared.append((queries, key_rows, value_rows))
    image_len = streams[0].shape[0]
    queries = jnp.concatenate([prepared[0][0], prepared[1][0]], axis=0)
    key_rows = jnp.concatenate([prepared[0][1], prepared[1][1]], axis=0)
    value_rows = jnp.concatenate([prepared[0][2], prepared[1][2]], axis=0)
    combined = jax.checkpoint(attend)(queries, key_rows, value_rows)
    combined = low(low_back(combined)).reshape(-1, D)
    results = []
    for token_flow in range(2):
        modulation = modulations[token_flow]
        mixed_part = combined[:image_len] if token_flow == 0 else combined[image_len:]
        branch_index = low_back(product(mixed_part, out_layer[token_flow]))
        middle = streams[token_flow] + modulation[2] * branch_index
        normed = low(layer_norm(middle) * (1.0 + modulation[4]) + modulation[3])
        hidden = low_back(product(normed, up_layer[token_flow]))
        activated = low(jax.nn.gelu(hidden, approximate=True))
        branch_index = low_back(product(activated, down_layer[token_flow]))
        results.append(middle + modulation[5] * branch_index)
    return results

def forward(params, image_rows, text_rows, vector):
    ada_all, qkv_all, out_all, up_all, down_all, gain_all = params
    activated = low(jax.nn.silu(vector))
    streams = [image_rows, text_rows]
    for layer_index in range(LAYERS):
        modulations = jnp.einsum('d,sde->se', activated, ada_all[layer_index], precision=HIGHEST).reshape(2, 6, D)
        streams = block(streams, modulations, qkv_all[layer_index], out_all[layer_index], up_all[layer_index], down_all[layer_index], gain_all[layer_index])
    return (streams[0], streams[1])

def reference(image_in, text_input, condition, ada_weight, qkv_weight, out_weight, up_weight, down_weight, norm_gain, image_cotangent, text_cotangent):
    params = tuple((weight.astype(jnp.float32) for weight in (ada_weight, qkv_weight, out_weight, up_weight, down_weight, norm_gain)))

    def one_sequence(totals, item_all):
        image_rows, text_rows, vector, image_seed, text_seed = item_all
        produced, pullback = jax.vjp(forward, params, image_rows.astype(jnp.float32), text_rows.astype(jnp.float32), vector.astype(jnp.float32))
        gradients, image_back, text_back, vector_back = pullback((image_seed.astype(jnp.float32), text_seed.astype(jnp.float32)))
        totals = jax.tree.map(lambda first, second: first + second, totals, gradients)
        return (totals, (produced[0].astype(jnp.bfloat16), produced[1].astype(jnp.bfloat16), image_back, text_back, vector_back))
    zero_grads = jax.tree.map(jnp.zeros_like, params)
    totals, results = lax.scan(one_sequence, zero_grads, (image_in, text_input, condition, image_cotangent, text_cotangent))
    return (results[0], results[1], results[2], results[3], results[4], totals[0], totals[1], totals[2], totals[3], totals[4], totals[5])
```

```python
import functools

import jax
import jax.numpy as jnp
from jax import lax
from jax.experimental import pallas as pl
from jax.experimental.pallas import tpu as pltpu
from jax.sharding import PartitionSpec as P

EPSILON = 1e-06
HIGHEST = lax.Precision.HIGHEST
F32 = jnp.float32
BF16 = jnp.bfloat16
HEAD = 64


def layer_stats(values):
    centred = values - jnp.mean(values, axis=-1, keepdims=True)
    root = lax.rsqrt(jnp.mean(centred * centred, axis=-1, keepdims=True) + EPSILON)
    return centred * root, root


def modulate(values, shift, scale):
    return layer_stats(values)[0] * (1.0 + scale) + shift


def modulate_back(values, grad, scale):
    normed, root = layer_stats(values)
    inner = grad * (1.0 + scale)
    first = jnp.mean(inner, axis=-1, keepdims=True)
    second = jnp.mean(inner * normed, axis=-1, keepdims=True)
    d_values = root * (inner - first - normed * second)
    return d_values, jnp.sum(grad, axis=0), jnp.sum(grad * normed, axis=0)


def mm(left, right):
    return lax.dot_general(left, right, (((1,), (0,)), ((), ())), preferred_element_type=F32)


def mm_nt(left, right):
    return lax.dot_general(left, right, (((1,), (1,)), ((), ())), preferred_element_type=F32)


def mm_tn(left, right):
    return lax.dot_general(left, right, (((0,), (0,)), ((), ())), preferred_element_type=F32)


def gelu(values):
    return jax.nn.gelu(values, approximate=True)


def head_factors(raw_t, gain_image, gain_text, image_len):
    root = lax.rsqrt(jnp.mean(raw_t * raw_t, axis=0, keepdims=True) + EPSILON)
    lanes = lax.broadcasted_iota(jnp.int32, raw_t.shape, 1)
    gain = jnp.where(lanes < image_len, gain_image, gain_text)
    return raw_t * root, root, gain


def transposed(first, second, low, high):
    return jnp.concatenate(
        [first[:, low:high].astype(F32).T, second[:, low:high].astype(F32).T], axis=1
    )


def attention_forward_kernel(step, image_ref, text_ref, gain_ref, o_image, o_text, lse_ref, o_scr):
    image_len, text_len = image_ref.shape[0], text_ref.shape[0]
    total = image_len + text_len
    wide = image_ref.shape[1] // 3
    factor = HEAD ** (-0.5)
    raw_q = transposed(image_ref, text_ref, 0, wide)
    raw_k = transposed(image_ref, text_ref, wide, 2 * wide)
    values_t = transposed(image_ref, text_ref, 2 * wide, 3 * wide).astype(BF16)
    for head in range(wide // HEAD):
        rows = slice(head * HEAD, (head + 1) * HEAD)
        q_hat, _, q_gain = head_factors(raw_q[rows], gain_ref[:, 0:1], gain_ref[:, 1:2], image_len)
        k_hat, _, k_gain = head_factors(raw_k[rows], gain_ref[:, 2:3], gain_ref[:, 3:4], image_len)
        q_t = ((q_hat * q_gain).astype(BF16).astype(F32) * factor).astype(BF16)
        keys = (k_hat * k_gain).T.astype(BF16)
        v_t = values_t[rows]
        for start in range(0, total, step):
            part = slice(start, start + step)
            scores = mm(keys, q_t[:, part])
            largest = jnp.max(scores, axis=0, keepdims=True)
            weights = jnp.exp(scores - largest)
            total_w = jnp.sum(weights, axis=0, keepdims=True)
            out = mm(v_t, weights.astype(BF16)) * (1.0 / total_w)
            o_scr[rows, part] = out
            lse_ref[head, :, part] = largest + jnp.log(total_w)
    o_image[...] = o_scr[:, :image_len].T.astype(BF16)
    o_text[...] = o_scr[:, image_len:].T.astype(BF16)


def attention_backward_kernel(
    step,
    image_ref,
    text_ref,
    gain_ref,
    o_image,
    o_text,
    do_image,
    do_text,
    lse_ref,
    d_image,
    d_text,
    gain_grad,
    dq_scr,
    dk_scr,
    dv_scr,
):
    image_len, text_len = image_ref.shape[0], text_ref.shape[0]
    total = image_len + text_len
    wide = image_ref.shape[1] // 3
    factor = HEAD ** (-0.5)
    raw_q = transposed(image_ref, text_ref, 0, wide)
    raw_k = transposed(image_ref, text_ref, wide, 2 * wide)
    o_t = transposed(o_image, o_text, 0, wide)
    do_t = transposed(do_image, do_text, 0, wide)
    lane_row = lax.broadcasted_iota(jnp.int32, (HEAD, 128), 1)
    gains_total = jnp.zeros((HEAD, 128), F32)
    for head in range(wide // HEAD):
        rows = slice(head * HEAD, (head + 1) * HEAD)
        low, high = 2 * wide + head * HEAD, 2 * wide + (head + 1) * HEAD
        q_hat, q_root, q_gain = head_factors(
            raw_q[rows], gain_ref[:, 0:1], gain_ref[:, 1:2], image_len
        )
        k_hat, k_root, k_gain = head_factors(
            raw_k[rows], gain_ref[:, 2:3], gain_ref[:, 3:4], image_len
        )
        q_full = (q_hat * q_gain).astype(BF16).astype(F32) * factor
        q_t = q_full.astype(BF16)
        queries = q_full.T.astype(BF16)
        k_t = (k_hat * k_gain).astype(BF16)
        keys = (k_hat * k_gain).T.astype(BF16)
        values = jnp.concatenate([image_ref[:, low:high], text_ref[:, low:high]], axis=0)
        d_out = jnp.concatenate([do_image[:, rows], do_text[:, rows]], axis=0)
        delta = jnp.sum(do_t[rows] * o_t[rows], axis=0, keepdims=True)
        d_out_t = do_t[rows].astype(BF16)
        d_keys = jnp.zeros((total, HEAD), F32)
        d_values = jnp.zeros((total, HEAD), F32)
        for start in range(0, total, step):
            part = slice(start, start + step)
            weights = jnp.exp(mm(keys, q_t[:, part]) - lse_ref[head, :, part])
            d_weights = mm(values, d_out_t[:, part])
            d_scores = (weights * (d_weights - delta[:, part])).astype(BF16)
            d_values += mm(weights.astype(BF16), d_out[part])
            d_keys += mm(d_scores, queries[part])
            dq_scr[rows, part] = mm(k_t, d_scores) * factor
        dv_scr[:, rows] = d_values
        dq = dq_scr[rows, :]
        dk = d_keys.T
        for slot, (grad, hat) in enumerate(((dq, q_hat), (dk, k_hat))):
            product = grad * hat
            image_sum = jnp.sum(product[:, :image_len], axis=1, keepdims=True)
            text_sum = jnp.sum(product[:, image_len:], axis=1, keepdims=True)
            gains_total += jnp.where(lane_row == 2 * slot, image_sum, 0.0)
            gains_total += jnp.where(lane_row == 2 * slot + 1, text_sum, 0.0)
        scaled = dq * q_gain
        dq_scr[rows, :] = q_root * (
            scaled - q_hat * jnp.mean(scaled * q_hat, axis=0, keepdims=True)
        )
        scaled = dk * k_gain
        dk_scr[rows, :] = k_root * (
            scaled - k_hat * jnp.mean(scaled * k_hat, axis=0, keepdims=True)
        )
    d_image[:, :wide] = dq_scr[:, :image_len].T.astype(BF16)
    d_text[:, :wide] = dq_scr[:, image_len:].T.astype(BF16)
    d_image[:, wide : 2 * wide] = dk_scr[:, :image_len].T.astype(BF16)
    d_text[:, wide : 2 * wide] = dk_scr[:, image_len:].T.astype(BF16)
    d_image[:, 2 * wide :] = dv_scr[:image_len].astype(BF16)
    d_text[:, 2 * wide :] = dv_scr[image_len:].astype(BF16)
    gain_grad[0] = gains_total


def query_step(total):
    for count in (3, 4, 2, 6, 9, 1):
        if total % (count * 128) == 0:
            return total // count
    return total


def kernel_cost(tokens, heads, products):
    return pl.CostEstimate(
        flops=2 * products * heads * tokens * tokens * HEAD * 4,
        transcendentals=heads * tokens * tokens,
        bytes_accessed=tokens * heads * HEAD * 2 * 8,
    )


def attention_forward(raw_image, raw_text, gains):
    groups = raw_image.shape[1] // (3 * 128)
    image_len, text_len = raw_image.shape[0], raw_text.shape[0]
    total = image_len + text_len
    return pl.pallas_call(
        functools.partial(attention_forward_kernel, query_step(total)),
        grid=(groups,),
        out_shape=(
            jax.ShapeDtypeStruct((image_len, groups * 128), BF16),
            jax.ShapeDtypeStruct((text_len, groups * 128), BF16),
            jax.ShapeDtypeStruct((groups * 2, 1, total), F32),
        ),
        in_specs=[
            pl.BlockSpec((image_len, 384), lambda g: (0, g)),
            pl.BlockSpec((text_len, 384), lambda g: (0, g)),
            pl.BlockSpec((HEAD, 4), lambda g: (0, 0)),
        ],
        out_specs=(
            pl.BlockSpec((image_len, 128), lambda g: (0, g)),
            pl.BlockSpec((text_len, 128), lambda g: (0, g)),
            pl.BlockSpec((2, 1, total), lambda g: (g, 0, 0)),
        ),
        scratch_shapes=[pltpu.VMEM((128, total), F32)],
        cost_estimate=kernel_cost(total, groups * 2, 2),
        name="attend_forward",
    )(raw_image, raw_text, gains)


def attention_backward(raw_image, raw_text, gains, o_image, o_text, do_image, do_text, lse):
    groups = raw_image.shape[1] // (3 * 128)
    image_len, text_len = raw_image.shape[0], raw_text.shape[0]
    total = image_len + text_len
    wide_image = pl.BlockSpec((image_len, 384), lambda g: (0, g))
    wide_text = pl.BlockSpec((text_len, 384), lambda g: (0, g))
    slim_image = pl.BlockSpec((image_len, 128), lambda g: (0, g))
    slim_text = pl.BlockSpec((text_len, 128), lambda g: (0, g))
    d_image, d_text, gain_grad = pl.pallas_call(
        functools.partial(attention_backward_kernel, query_step(total)),
        grid=(groups,),
        out_shape=(
            jax.ShapeDtypeStruct(raw_image.shape, BF16),
            jax.ShapeDtypeStruct(raw_text.shape, BF16),
            jax.ShapeDtypeStruct((groups, HEAD, 128), F32),
        ),
        in_specs=[
            wide_image,
            wide_text,
            pl.BlockSpec((HEAD, 4), lambda g: (0, 0)),
            slim_image,
            slim_text,
            slim_image,
            slim_text,
            pl.BlockSpec((2, 1, total), lambda g: (g, 0, 0)),
        ],
        out_specs=(wide_image, wide_text, pl.BlockSpec((1, HEAD, 128), lambda g: (g, 0, 0))),
        scratch_shapes=[
            pltpu.VMEM((128, total), F32),
            pltpu.VMEM((128, total), F32),
            pltpu.VMEM((total, 128), F32),
        ],
        cost_estimate=kernel_cost(total, groups * 2, 5),
        name="attend_backward",
    )(raw_image, raw_text, gains, o_image, o_text, do_image, do_text, lse)
    return d_image, d_text, jnp.sum(gain_grad, axis=0)[:, :4].T


def plain_parts(raw_image, raw_text, gains):
    raw = jnp.concatenate([raw_image, raw_text], axis=0).astype(F32)
    raw = raw.reshape(raw.shape[0], -1, 3, HEAD)
    is_image = (jnp.arange(raw.shape[0]) < raw_image.shape[0])[:, None, None]
    hats, roots, scales, rounded = [], [], [], []
    for slot in range(2):
        part = raw[:, :, slot]
        root = lax.rsqrt(jnp.mean(part * part, axis=-1, keepdims=True) + EPSILON)
        scale = jnp.where(is_image, gains[:, 2 * slot], gains[:, 2 * slot + 1])
        hats.append(part * root)
        roots.append(root)
        scales.append(scale)
        rounded.append((part * root * scale).astype(BF16))
    return hats, roots, scales, rounded, raw[:, :, 2].astype(BF16)


def plain_forward(raw_image, raw_text, gains):
    _, _, _, (queries, keys), values = plain_parts(raw_image, raw_text, gains)
    scores = jnp.einsum("qhd,khd->hqk", queries, keys, preferred_element_type=F32)
    scores = scores * HEAD ** (-0.5)
    largest = jnp.max(scores, axis=-1, keepdims=True)
    lse = largest + jnp.log(jnp.sum(jnp.exp(scores - largest), axis=-1, keepdims=True))
    weights = jnp.exp(scores - lse).astype(BF16)
    out = jnp.einsum("hqk,khd->qhd", weights, values, preferred_element_type=F32)
    out = out.astype(BF16).reshape(out.shape[0], -1)
    return out[: raw_image.shape[0]], out[raw_image.shape[0] :], lse


def plain_backward(raw_image, raw_text, gains, o_image, o_text, do_image, do_text, lse):
    hats, roots, scales, (queries, keys), values = plain_parts(raw_image, raw_text, gains)
    factor = HEAD ** (-0.5)
    image_len = raw_image.shape[0]
    d_out = jnp.concatenate([do_image, do_text], axis=0).reshape(queries.shape)
    scores = jnp.einsum("qhd,khd->hqk", queries, keys, preferred_element_type=F32) * factor
    weights = jnp.exp(scores - lse)
    d_weights = jnp.einsum("qhd,khd->hqk", d_out, values, preferred_element_type=F32)
    inner = jnp.sum(weights * d_weights, axis=-1, keepdims=True)
    d_scores = (weights * (d_weights - inner)).astype(BF16)
    dq = jnp.einsum("hqk,khd->qhd", d_scores, keys, preferred_element_type=F32) * factor
    dk = jnp.einsum("hqk,qhd->khd", d_scores, queries, preferred_element_type=F32) * factor
    dv = jnp.einsum("hqk,qhd->khd", weights.astype(BF16), d_out, preferred_element_type=F32)
    gain_rows, parts = [], []
    for grad, hat, root, scale in zip((dq, dk), hats, roots, scales):
        product = grad * hat
        gain_rows += [jnp.sum(product[:image_len], (0, 1)), jnp.sum(product[image_len:], (0, 1))]
        scaled = grad * scale
        parts.append(root * (scaled - hat * jnp.mean(scaled * hat, axis=-1, keepdims=True)))
    joined = jnp.stack(parts + [dv], axis=2).astype(BF16).reshape(d_out.shape[0], -1)
    return joined[:image_len], joined[image_len:], jnp.stack(gain_rows)


def gather_tokens(own, axis, size):
    if size == 1:
        return [own]
    after, before = [], []
    down = up = own
    for _ in range(size - 1):
        down = lax.ppermute(down, axis, [(i, i - 1) for i in range(1, size)])
        up = lax.ppermute(up, axis, [(i, i + 1) for i in range(size - 1)])
        after.append(down)
        before.append(up)
    me = lax.axis_index(axis)
    return [own] + [
        jnp.where(me + k < size, after[k - 1], before[size - k - 1]) for k in range(1, size)
    ]


def scatter_tokens(blocks, axis, size):
    up = down = None
    for step in range(size - 1):
        k = size - 1 - step
        send_up = blocks[k] if up is None else (blocks[k].astype(F32) + up).astype(BF16)
        send_down = (
            blocks[size - k]
            if down is None
            else (blocks[size - k].astype(F32) + down).astype(BF16)
        )
        up = lax.ppermute(send_up, axis, [(i, i + 1) for i in range(step + 1)]).astype(F32)
        down = lax.ppermute(
            send_down, axis, [(i, i - 1) for i in range(size - 1 - step, size)]
        ).astype(F32)
    total = blocks[0].astype(F32)
    return total if up is None else total + up + down


def bit_order(size):
    bits = [b for b in range(size.bit_length() - 1)]
    masks = [0]
    for b in bits:
        masks += [m | (1 << b) for m in masks]
    return bits, masks


def swap_bit(value, axis, size, bit):
    return lax.ppermute(value, axis, [(i, i ^ (1 << bit)) for i in range(size)])


def bit_gather(own, axis, size):
    blocks = own[None]
    for b in bit_order(size)[0]:
        blocks = jnp.concatenate([blocks, swap_bit(blocks, axis, size, b)], axis=0)
    return blocks


def bit_scatter(parts, axis, size):
    me = lax.axis_index(axis)
    for b in reversed(bit_order(size)[0]):
        half = parts.shape[0] // 2
        upper = ((me >> b) & 1) == 1
        keep = jnp.where(upper, parts[half:], parts[:half])
        send = jnp.where(upper, parts[:half], parts[half:])
        parts = keep + swap_bit(send, axis, size, b)
    return parts[0]


def add_up(values):
    total = values[0]
    for value in values[1:]:
        total = total + value
    return total


def tie(*groups):
    return lax.optimization_barrier(groups)


class Streams:
    def __init__(self, image_len, text_len, axis, size):
        self.lengths = (image_len, text_len)
        self.axis, self.size = axis, size

    def gather(self, pair):
        cut = self.lengths[0]
        blocks = gather_tokens(jnp.concatenate(pair, axis=0), self.axis, self.size)
        return (
            jnp.concatenate([b[:cut] for b in blocks], axis=0),
            jnp.concatenate([b[cut:] for b in blocks], axis=0),
        )

    def scatter(self, pair):
        cut = self.lengths[0]
        low = [part.astype(BF16) for part in pair]
        blocks = [
            jnp.concatenate(
                [low[s][k * n : (k + 1) * n] for s, n in enumerate(self.lengths)], axis=0
            )
            for k in range(self.size)
        ]
        total = scatter_tokens(blocks, self.axis, self.size)
        return total[:cut], total[cut:]


def forward_layer(streams, x, mods, weights, gains, attend, first):
    qkv, out_t, up, down_t = weights
    if first:
        plain = streams.gather([layer_stats(x[s])[0].astype(BF16) for s in range(2)])
        normed = [
            (plain[s].astype(F32) * (1.0 + mods[s, 1]) + mods[s, 0]).astype(BF16)
            for s in range(2)
        ]
    else:
        normed = streams.gather(
            [modulate(x[s], mods[s, 0], mods[s, 1]).astype(BF16) for s in range(2)]
        )
    raw = [mm(normed[s], qkv[s]).astype(BF16) for s in range(2)]
    o_image, o_text, lse = attend(raw[0], raw[1], gains)
    mixed = (o_image, o_text)
    branch = streams.scatter([mm_nt(mixed[s], out_t[s]) for s in range(2)])
    middle = [x[s] + mods[s, 2] * branch[s] for s in range(2)]
    second = streams.gather(
        [modulate(middle[s], mods[s, 3], mods[s, 4]).astype(BF16) for s in range(2)]
    )
    hidden = [mm(second[s], up[s]) for s in range(2)]
    active = [gelu(hidden[s]).astype(BF16) for s in range(2)]
    hidden = [hidden[s].astype(BF16) for s in range(2)]
    result = streams.scatter([mm_nt(active[s], down_t[s]) for s in range(2)])
    y = [middle[s] + mods[s, 5] * result[s] for s in range(2)]
    saved = (x, normed, raw, mixed, lse, branch, middle, second, hidden, active, result)
    return y, saved


def backward_layer(streams, gy, saved, mods, weights, gains, attend_back, reduce_grad, pending):
    qkv, out_t, up, down_t = weights
    x, normed, raw, mixed, lse, branch, middle, second, hidden, active, result = saved
    d_gate2 = [jnp.sum(gy[s] * result[s], axis=0) for s in range(2)]
    dm = streams.gather([(mods[s, 5] * gy[s]).astype(BF16) for s in range(2)])
    du = []
    for s in range(2):
        _, pull = jax.vjp(gelu, hidden[s].astype(F32))
        du.append(pull(mm(dm[s], down_t[s]))[0].astype(BF16))
    d_second = streams.scatter([mm_nt(du[s], up[s]) for s in range(2)])
    late = [mm_tn(second[s], du[s]) for s in range(2)]
    late += [mm_tn(dm[s], active[s]) for s in range(2)]
    late = jnp.concatenate([part.astype(BF16) for part in late], axis=1)
    late, pending = tie(late, pending)
    reduced_mlp = reduce_grad(late)
    d_middle, d_shift2, d_scale2 = [], [], []
    for s in range(2):
        inner, d_shift, d_scale = modulate_back(middle[s], d_second[s], mods[s, 4])
        d_middle.append(gy[s] + inner)
        d_shift2.append(d_shift)
        d_scale2.append(d_scale)
    d_gate1 = [jnp.sum(d_middle[s] * branch[s], axis=0) for s in range(2)]
    da = streams.gather([(mods[s, 2] * d_middle[s]).astype(BF16) for s in range(2)])
    d_mixed = [mm(da[s], out_t[s]).astype(BF16) for s in range(2)]
    d_image, d_text, gain_rows = attend_back(
        raw[0], raw[1], gains, mixed[0], mixed[1], d_mixed[0], d_mixed[1], lse
    )
    d_raw = (d_image, d_text)
    d_first = streams.scatter([mm_nt(d_raw[s], qkv[s]) for s in range(2)])
    late = [mm_tn(normed[s], d_raw[s]) for s in range(2)]
    late += [mm_tn(da[s], mixed[s]) for s in range(2)]
    late = jnp.concatenate([part.astype(BF16) for part in late], axis=1)
    late, reduced_mlp = tie(late, reduced_mlp)
    reduced_attention = reduce_grad(late)
    gx, d_mods = [], []
    for s in range(2):
        inner, d_shift, d_scale = modulate_back(x[s], d_first[s], mods[s, 1])
        gx.append(d_middle[s] + inner)
        d_mods.append(
            jnp.stack([d_shift, d_scale, d_gate1[s], d_shift2[s], d_scale2[s], d_gate2[s]])
        )
    d_gains = gain_rows.reshape(2, 2, HEAD).transpose(1, 0, 2)
    return gx, jnp.stack(d_mods), d_gains, (reduced_attention, reduced_mlp), pending


def on_device(dp, seq, width_of_group, *args):
    (
        image_in,
        text_input,
        condition,
        ada_weight,
        qkv_weight,
        out_weight,
        up_weight,
        down_weight,
        norm_gain,
        image_cotangent,
        text_cotangent,
    ) = args
    dp_axis, dp_size = dp
    seq_axis, seq_size = seq
    layers = qkv_weight.shape[0]
    width = image_in.shape[2]
    streams = Streams(image_in.shape[1], text_input.shape[1], seq_axis, seq_size)
    attend, attend_back = (
        (attention_forward, attention_backward)
        if width_of_group % 128 == 0
        else (plain_forward, plain_backward)
    )
    rows = qkv_weight.shape[2]

    def fetch(local):
        return lax.all_gather(local, dp_axis, axis=1, tiled=True)

    qkv_local = qkv_weight.reshape(layers, 2, rows, 3, -1, width_of_group)
    qkv_local = qkv_local.transpose(0, 1, 2, 4, 3, 5).reshape(layers, 2, rows, -1)
    out_local = out_weight.transpose(0, 1, 3, 2)
    down_local = down_weight.transpose(0, 1, 3, 2)
    weights = [
        tuple(fetch(w[l]) for w in (qkv_local, out_local, up_weight, down_local))
        for l in range(layers)
    ]

    act_cond, silu_pull = jax.vjp(jax.nn.silu, condition.astype(F32))
    act_low = act_cond.astype(BF16)
    partial_mods = jnp.einsum("nd,lsde->nlse", act_low, ada_weight, preferred_element_type=F32)
    own_mods = bit_scatter(partial_mods.reshape(dp_size, -1), dp_axis, dp_size)
    own_mods = add_up(gather_tokens(own_mods, seq_axis, seq_size))
    own_mods = own_mods.reshape(layers, 2, 6, width)
    gains_all = norm_gain.astype(F32)
    gain_columns = [gains_all[l].transpose(1, 0, 2).reshape(4, HEAD).T for l in range(layers)]

    x = [image_in[0].astype(F32), text_input[0].astype(F32)]
    saved_list = []
    for l in range(layers):
        x, saved = forward_layer(streams, x, own_mods[l], weights[l], gain_columns[l], attend, l == 0)
        saved_list.append(saved)
    outputs = [part.astype(BF16)[None] for part in x]

    def reduce_grad(grad):
        return lax.psum_scatter(grad, dp_axis, scatter_dimension=0, tiled=True)

    gy = [image_cotangent[0].astype(F32), text_cotangent[0].astype(F32)]
    d_mods, d_gains, grads = [None] * layers, [None] * layers, [None] * layers
    pending = ()
    for l in reversed(range(layers)):
        gy, d_mods[l], d_gains[l], grads[l], done = backward_layer(
            streams,
            gy,
            saved_list[l],
            own_mods[l],
            weights[l],
            gain_columns[l],
            attend_back,
            reduce_grad,
            pending,
        )
        if l + 1 < layers:
            grads[l + 1] = (done[0], grads[l + 1][1])
        pending = (grads[l][0],)

    masks = jnp.array(bit_order(dp_size)[1], jnp.int32) ^ lax.axis_index(dp_axis)
    small = jnp.concatenate([jnp.stack(d_mods).reshape(-1), jnp.stack(d_gains).reshape(-1)])
    small = add_up(gather_tokens(small, seq_axis, seq_size))
    small = bit_gather(small, dp_axis, dp_size)
    count = layers * 2 * 6 * width
    total_mods = small[:, :count].reshape(dp_size, layers, 2, 6 * width)
    total_gains = lax.all_gather(jnp.sum(small[:, count:], axis=0), seq_axis)[0]
    total_gains = total_gains.reshape(layers, 2, 2, HEAD)
    act_there = act_low.astype(F32)[masks]
    ada_grad = jnp.einsum("nd,nlse->lsde", act_there, total_mods, precision=HIGHEST)
    d_act = jnp.einsum("nlse,lsde->nd", total_mods, ada_weight.astype(F32), precision=HIGHEST)
    d_act = d_act[masks]
    condition_grad = silu_pull(d_act)[0]

    sizes = [qkv_local.shape[3], out_local.shape[3]], [up_weight.shape[3], down_local.shape[3]]

    def pieces(group, slot):
        size = sizes[group][slot]
        start = 2 * slot * sizes[group][0]
        return jnp.stack(
            [
                jnp.stack(
                    [
                        grads[l][group][:, start + s * size : start + (s + 1) * size].astype(F32)
                        for s in range(2)
                    ]
                )
                for l in range(layers)
            ]
        )

    qkv_grad = pieces(0, 0).reshape(layers, 2, rows, -1, 3, width_of_group)
    qkv_grad = qkv_grad.transpose(0, 1, 2, 4, 3, 5).reshape(qkv_weight.shape)
    return (
        outputs[0],
        outputs[1],
        gy[0][None],
        gy[1][None],
        condition_grad,
        ada_grad,
        qkv_grad,
        pieces(0, 1).transpose(0, 1, 3, 2),
        pieces(1, 0),
        pieces(1, 1).transpose(0, 1, 3, 2),
        total_gains,
    )


def solution(mesh):
    tokens = P("dp", "seq", None)
    placed = (
        tokens,
        tokens,
        P(None, ("dp", "seq")),
        P(None, None, ("dp", "seq"), None),
        P(None, None, "dp", None, "seq"),
        P(None, None, "seq", "dp"),
        P(None, None, "dp", "seq"),
        P(None, None, "seq", "dp"),
        P(),
        tokens,
        tokens,
    )
    results = (tokens, tokens, tokens, tokens) + placed[2:8] + (P(),)

    def step(*args):
        heads = args[4].shape[4] // mesh.shape["seq"] // HEAD
        group = 2 * HEAD if heads % 2 == 0 else HEAD
        body = functools.partial(
            on_device, ("dp", mesh.shape["dp"]), ("seq", mesh.shape["seq"]), group
        )
        return jax.shard_map(
            body, mesh=mesh, in_specs=placed, out_specs=results, check_vma=False
        )(*args)

    return step
```

```python
import functools

import jax
import jax.numpy as jnp
from jax import lax
from jax.experimental import pallas as pl
from jax.experimental.pallas import tpu as pltpu
from jax.sharding import PartitionSpec as P

EPSILON = 1e-06
HIGHEST = lax.Precision.HIGHEST
F32 = jnp.float32
BF16 = jnp.bfloat16
HEAD = 64


def layer_stats(values):
    centred = values - jnp.mean(values, axis=-1, keepdims=True)
    root = lax.rsqrt(jnp.mean(centred * centred, axis=-1, keepdims=True) + EPSILON)
    return centred * root, root


def modulate(values, shift, scale):
    return layer_stats(values)[0] * (1.0 + scale) + shift


def modulate_back(values, grad, scale):
    normed, root = layer_stats(values)
    inner = grad * (1.0 + scale)
    first = jnp.mean(inner, axis=-1, keepdims=True)
    second = jnp.mean(inner * normed, axis=-1, keepdims=True)
    d_values = root * (inner - first - normed * second)
    return d_values, jnp.sum(grad, axis=0), jnp.sum(grad * normed, axis=0)


def mm(left, right):
    return lax.dot_general(left, right, (((1,), (0,)), ((), ())), preferred_element_type=F32)


def mm_nt(left, right):
    return lax.dot_general(left, right, (((1,), (1,)), ((), ())), preferred_element_type=F32)


def mm_tn(left, right):
    return lax.dot_general(left, right, (((0,), (0,)), ((), ())), preferred_element_type=F32)


def gelu(values):
    return jax.nn.gelu(values, approximate=True)


def head_factors(raw_t, gain_image, gain_text, image_len):
    root = lax.rsqrt(jnp.mean(raw_t * raw_t, axis=0, keepdims=True) + EPSILON)
    lanes = lax.broadcasted_iota(jnp.int32, raw_t.shape, 1)
    gain = jnp.where(lanes < image_len, gain_image, gain_text)
    return raw_t * root, root, gain


def transposed(first, second, low, high):
    return jnp.concatenate(
        [first[:, low:high].astype(F32).T, second[:, low:high].astype(F32).T], axis=1
    )


def attention_forward_kernel(step, image_ref, text_ref, gain_ref, o_image, o_text, lse_ref, o_scr):
    image_len, text_len = image_ref.shape[0], text_ref.shape[0]
    total = image_len + text_len
    wide = image_ref.shape[1] // 3
    factor = HEAD ** (-0.5)
    raw_q = transposed(image_ref, text_ref, 0, wide)
    raw_k = transposed(image_ref, text_ref, wide, 2 * wide)
    values_t = transposed(image_ref, text_ref, 2 * wide, 3 * wide).astype(BF16)
    for head in range(wide // HEAD):
        rows = slice(head * HEAD, (head + 1) * HEAD)
        q_hat, _, q_gain = head_factors(raw_q[rows], gain_ref[:, 0:1], gain_ref[:, 1:2], image_len)
        k_hat, _, k_gain = head_factors(raw_k[rows], gain_ref[:, 2:3], gain_ref[:, 3:4], image_len)
        q_t = ((q_hat * q_gain).astype(BF16).astype(F32) * factor).astype(BF16)
        keys = (k_hat * k_gain).T.astype(BF16)
        v_t = values_t[rows]
        for start in range(0, total, step):
            part = slice(start, start + step)
            scores = mm(keys, q_t[:, part])
            largest = jnp.max(scores, axis=0, keepdims=True)
            weights = jnp.exp(scores - largest)
            total_w = jnp.sum(weights, axis=0, keepdims=True)
            out = mm(v_t, weights.astype(BF16)) * (1.0 / total_w)
            o_scr[rows, part] = out
            lse_ref[head, :, part] = largest + jnp.log(total_w)
    o_image[...] = o_scr[:, :image_len].T.astype(BF16)
    o_text[...] = o_scr[:, image_len:].T.astype(BF16)


def attention_backward_kernel(
    step,
    image_ref,
    text_ref,
    gain_ref,
    o_image,
    o_text,
    do_image,
    do_text,
    lse_ref,
    d_image,
    d_text,
    gain_grad,
    dq_scr,
    dk_scr,
    dv_scr,
):
    image_len, text_len = image_ref.shape[0], text_ref.shape[0]
    total = image_len + text_len
    wide = image_ref.shape[1] // 3
    factor = HEAD ** (-0.5)
    raw_q = transposed(image_ref, text_ref, 0, wide)
    raw_k = transposed(image_ref, text_ref, wide, 2 * wide)
    o_t = transposed(o_image, o_text, 0, wide)
    do_t = transposed(do_image, do_text, 0, wide)
    lane_row = lax.broadcasted_iota(jnp.int32, (HEAD, 128), 1)
    gains_total = jnp.zeros((HEAD, 128), F32)
    for head in range(wide // HEAD):
        rows = slice(head * HEAD, (head + 1) * HEAD)
        low, high = 2 * wide + head * HEAD, 2 * wide + (head + 1) * HEAD
        q_hat, q_root, q_gain = head_factors(
            raw_q[rows], gain_ref[:, 0:1], gain_ref[:, 1:2], image_len
        )
        k_hat, k_root, k_gain = head_factors(
            raw_k[rows], gain_ref[:, 2:3], gain_ref[:, 3:4], image_len
        )
        q_full = (q_hat * q_gain).astype(BF16).astype(F32) * factor
        q_t = q_full.astype(BF16)
        queries = q_full.T.astype(BF16)
        k_t = (k_hat * k_gain).astype(BF16)
        keys = (k_hat * k_gain).T.astype(BF16)
        values = jnp.concatenate([image_ref[:, low:high], text_ref[:, low:high]], axis=0)
        d_out = jnp.concatenate([do_image[:, rows], do_text[:, rows]], axis=0)
        delta = jnp.sum(do_t[rows] * o_t[rows], axis=0, keepdims=True)
        d_out_t = do_t[rows].astype(BF16)
        d_keys = jnp.zeros((total, HEAD), F32)
        d_values = jnp.zeros((total, HEAD), F32)
        for start in range(0, total, step):
            part = slice(start, start + step)
            weights = jnp.exp(mm(keys, q_t[:, part]) - lse_ref[head, :, part])
            d_weights = mm(values, d_out_t[:, part])
            d_scores = (weights * (d_weights - delta[:, part])).astype(BF16)
            d_values += mm(weights.astype(BF16), d_out[part])
            d_keys += mm(d_scores, queries[part])
            dq_scr[rows, part] = mm(k_t, d_scores) * factor
        dv_scr[:, rows] = d_values
        dq = dq_scr[rows, :]
        dk = d_keys.T
        for slot, (grad, hat) in enumerate(((dq, q_hat), (dk, k_hat))):
            product = grad * hat
            image_sum = jnp.sum(product[:, :image_len], axis=1, keepdims=True)
            text_sum = jnp.sum(product[:, image_len:], axis=1, keepdims=True)
            gains_total += jnp.where(lane_row == 2 * slot, image_sum, 0.0)
            gains_total += jnp.where(lane_row == 2 * slot + 1, text_sum, 0.0)
        scaled = dq * q_gain
        dq_scr[rows, :] = q_root * (
            scaled - q_hat * jnp.mean(scaled * q_hat, axis=0, keepdims=True)
        )
        scaled = dk * k_gain
        dk_scr[rows, :] = k_root * (
            scaled - k_hat * jnp.mean(scaled * k_hat, axis=0, keepdims=True)
        )
    d_image[:, :wide] = dq_scr[:, :image_len].T.astype(BF16)
    d_text[:, :wide] = dq_scr[:, image_len:].T.astype(BF16)
    d_image[:, wide : 2 * wide] = dk_scr[:, :image_len].T.astype(BF16)
    d_text[:, wide : 2 * wide] = dk_scr[:, image_len:].T.astype(BF16)
    d_image[:, 2 * wide :] = dv_scr[:image_len].astype(BF16)
    d_text[:, 2 * wide :] = dv_scr[image_len:].astype(BF16)
    gain_grad[0] = gains_total


def query_step(total):
    for count in (3, 4, 2, 6, 9, 1):
        if total % (count * 128) == 0:
            return total // count
    return total


def kernel_cost(tokens, heads, products):
    return pl.CostEstimate(
        flops=2 * products * heads * tokens * tokens * HEAD * 4,
        transcendentals=heads * tokens * tokens,
        bytes_accessed=tokens * heads * HEAD * 2 * 8,
    )


def attention_forward(raw_image, raw_text, gains):
    groups = raw_image.shape[1] // (3 * 128)
    image_len, text_len = raw_image.shape[0], raw_text.shape[0]
    total = image_len + text_len
    return pl.pallas_call(
        functools.partial(attention_forward_kernel, query_step(total)),
        grid=(groups,),
        out_shape=(
            jax.ShapeDtypeStruct((image_len, groups * 128), BF16),
            jax.ShapeDtypeStruct((text_len, groups * 128), BF16),
            jax.ShapeDtypeStruct((groups * 2, 1, total), F32),
        ),
        in_specs=[
            pl.BlockSpec((image_len, 384), lambda g: (0, g)),
            pl.BlockSpec((text_len, 384), lambda g: (0, g)),
            pl.BlockSpec((HEAD, 4), lambda g: (0, 0)),
        ],
        out_specs=(
            pl.BlockSpec((image_len, 128), lambda g: (0, g)),
            pl.BlockSpec((text_len, 128), lambda g: (0, g)),
            pl.BlockSpec((2, 1, total), lambda g: (g, 0, 0)),
        ),
        scratch_shapes=[pltpu.VMEM((128, total), F32)],
        cost_estimate=kernel_cost(total, groups * 2, 2),
        name="attend_forward",
    )(raw_image, raw_text, gains)


def attention_backward(raw_image, raw_text, gains, o_image, o_text, do_image, do_text, lse):
    groups = raw_image.shape[1] // (3 * 128)
    image_len, text_len = raw_image.shape[0], raw_text.shape[0]
    total = image_len + text_len
    wide_image = pl.BlockSpec((image_len, 384), lambda g: (0, g))
    wide_text = pl.BlockSpec((text_len, 384), lambda g: (0, g))
    slim_image = pl.BlockSpec((image_len, 128), lambda g: (0, g))
    slim_text = pl.BlockSpec((text_len, 128), lambda g: (0, g))
    d_image, d_text, gain_grad = pl.pallas_call(
        functools.partial(attention_backward_kernel, query_step(total)),
        grid=(groups,),
        out_shape=(
            jax.ShapeDtypeStruct(raw_image.shape, BF16),
            jax.ShapeDtypeStruct(raw_text.shape, BF16),
            jax.ShapeDtypeStruct((groups, HEAD, 128), F32),
        ),
        in_specs=[
            wide_image,
            wide_text,
            pl.BlockSpec((HEAD, 4), lambda g: (0, 0)),
            slim_image,
            slim_text,
            slim_image,
            slim_text,
            pl.BlockSpec((2, 1, total), lambda g: (g, 0, 0)),
        ],
        out_specs=(wide_image, wide_text, pl.BlockSpec((1, HEAD, 128), lambda g: (g, 0, 0))),
        scratch_shapes=[
            pltpu.VMEM((128, total), F32),
            pltpu.VMEM((128, total), F32),
            pltpu.VMEM((total, 128), F32),
        ],
        cost_estimate=kernel_cost(total, groups * 2, 5),
        name="attend_backward",
    )(raw_image, raw_text, gains, o_image, o_text, do_image, do_text, lse)
    return d_image, d_text, jnp.sum(gain_grad, axis=0)[:, :4].T


def plain_parts(raw_image, raw_text, gains):
    raw = jnp.concatenate([raw_image, raw_text], axis=0).astype(F32)
    raw = raw.reshape(raw.shape[0], -1, 3, HEAD)
    is_image = (jnp.arange(raw.shape[0]) < raw_image.shape[0])[:, None, None]
    hats, roots, scales, rounded = [], [], [], []
    for slot in range(2):
        part = raw[:, :, slot]
        root = lax.rsqrt(jnp.mean(part * part, axis=-1, keepdims=True) + EPSILON)
        scale = jnp.where(is_image, gains[:, 2 * slot], gains[:, 2 * slot + 1])
        hats.append(part * root)
        roots.append(root)
        scales.append(scale)
        rounded.append((part * root * scale).astype(BF16))
    return hats, roots, scales, rounded, raw[:, :, 2].astype(BF16)


def plain_forward(raw_image, raw_text, gains):
    _, _, _, (queries, keys), values = plain_parts(raw_image, raw_text, gains)
    scores = jnp.einsum("qhd,khd->hqk", queries, keys, preferred_element_type=F32)
    scores = scores * HEAD ** (-0.5)
    largest = jnp.max(scores, axis=-1, keepdims=True)
    lse = largest + jnp.log(jnp.sum(jnp.exp(scores - largest), axis=-1, keepdims=True))
    weights = jnp.exp(scores - lse).astype(BF16)
    out = jnp.einsum("hqk,khd->qhd", weights, values, preferred_element_type=F32)
    out = out.astype(BF16).reshape(out.shape[0], -1)
    return out[: raw_image.shape[0]], out[raw_image.shape[0] :], lse


def plain_backward(raw_image, raw_text, gains, o_image, o_text, do_image, do_text, lse):
    hats, roots, scales, (queries, keys), values = plain_parts(raw_image, raw_text, gains)
    factor = HEAD ** (-0.5)
    image_len = raw_image.shape[0]
    d_out = jnp.concatenate([do_image, do_text], axis=0).reshape(queries.shape)
    scores = jnp.einsum("qhd,khd->hqk", queries, keys, preferred_element_type=F32) * factor
    weights = jnp.exp(scores - lse)
    d_weights = jnp.einsum("qhd,khd->hqk", d_out, values, preferred_element_type=F32)
    inner = jnp.sum(weights * d_weights, axis=-1, keepdims=True)
    d_scores = (weights * (d_weights - inner)).astype(BF16)
    dq = jnp.einsum("hqk,khd->qhd", d_scores, keys, preferred_element_type=F32) * factor
    dk = jnp.einsum("hqk,qhd->khd", d_scores, queries, preferred_element_type=F32) * factor
    dv = jnp.einsum("hqk,qhd->khd", weights.astype(BF16), d_out, preferred_element_type=F32)
    gain_rows, parts = [], []
    for grad, hat, root, scale in zip((dq, dk), hats, roots, scales):
        product = grad * hat
        gain_rows += [jnp.sum(product[:image_len], (0, 1)), jnp.sum(product[image_len:], (0, 1))]
        scaled = grad * scale
        parts.append(root * (scaled - hat * jnp.mean(scaled * hat, axis=-1, keepdims=True)))
    joined = jnp.stack(parts + [dv], axis=2).astype(BF16).reshape(d_out.shape[0], -1)
    return joined[:image_len], joined[image_len:], jnp.stack(gain_rows)


def gather_tokens(own, axis, size):
    if size == 1:
        return [own]
    after, before = [], []
    down = up = own
    for _ in range(size - 1):
        down = lax.ppermute(down, axis, [(i, i - 1) for i in range(1, size)])
        up = lax.ppermute(up, axis, [(i, i + 1) for i in range(size - 1)])
        after.append(down)
        before.append(up)
    me = lax.axis_index(axis)
    return [own] + [
        jnp.where(me + k < size, after[k - 1], before[size - k - 1]) for k in range(1, size)
    ]


def scatter_tokens(blocks, axis, size):
    up = down = None
    for step in range(size - 1):
        k = size - 1 - step
        send_up = blocks[k] if up is None else (blocks[k].astype(F32) + up).astype(BF16)
        send_down = (
            blocks[size - k]
            if down is None
            else (blocks[size - k].astype(F32) + down).astype(BF16)
        )
        up = lax.ppermute(send_up, axis, [(i, i + 1) for i in range(step + 1)]).astype(F32)
        down = lax.ppermute(
            send_down, axis, [(i, i - 1) for i in range(size - 1 - step, size)]
        ).astype(F32)
    total = blocks[0].astype(F32)
    return total if up is None else total + up + down


def bit_order(size):
    bits = [b for b in range(size.bit_length() - 1)]
    masks = [0]
    for b in bits:
        masks += [m | (1 << b) for m in masks]
    return bits, masks


def swap_bit(value, axis, size, bit):
    return lax.ppermute(value, axis, [(i, i ^ (1 << bit)) for i in range(size)])


def bit_gather(own, axis, size):
    blocks = own[None]
    for b in bit_order(size)[0]:
        blocks = jnp.concatenate([blocks, swap_bit(blocks, axis, size, b)], axis=0)
    return blocks


def bit_scatter(parts, axis, size):
    me = lax.axis_index(axis)
    for b in reversed(bit_order(size)[0]):
        half = parts.shape[0] // 2
        upper = ((me >> b) & 1) == 1
        keep = jnp.where(upper, parts[half:], parts[:half])
        send = jnp.where(upper, parts[:half], parts[half:])
        parts = keep + swap_bit(send, axis, size, b)
    return parts[0]


def bit_sum(value, axis, size):
    for b in bit_order(size)[0]:
        value = value + swap_bit(value, axis, size, b)
    return value


def tie(*groups):
    return lax.optimization_barrier(groups)


class Streams:
    def __init__(self, image_len, text_len, axis, size):
        self.lengths = (image_len, text_len)
        self.axis, self.size = axis, size

    def gather(self, pair):
        cut = self.lengths[0]
        blocks = gather_tokens(jnp.concatenate(pair, axis=0), self.axis, self.size)
        return (
            jnp.concatenate([b[:cut] for b in blocks], axis=0),
            jnp.concatenate([b[cut:] for b in blocks], axis=0),
        )

    def scatter(self, pair):
        cut = self.lengths[0]
        low = [part.astype(BF16) for part in pair]
        blocks = [
            jnp.concatenate(
                [low[s][k * n : (k + 1) * n] for s, n in enumerate(self.lengths)], axis=0
            )
            for k in range(self.size)
        ]
        total = scatter_tokens(blocks, self.axis, self.size)
        return total[:cut], total[cut:]


def forward_layer(streams, x, mods, weights, gains, attend, first):
    qkv, out_t, up, down_t = weights
    if first:
        plain = streams.gather([layer_stats(x[s])[0].astype(BF16) for s in range(2)])
        normed = [
            (plain[s].astype(F32) * (1.0 + mods[s, 1]) + mods[s, 0]).astype(BF16)
            for s in range(2)
        ]
    else:
        normed = streams.gather(
            [modulate(x[s], mods[s, 0], mods[s, 1]).astype(BF16) for s in range(2)]
        )
    raw = [mm(normed[s], qkv[s]).astype(BF16) for s in range(2)]
    o_image, o_text, lse = attend(raw[0], raw[1], gains)
    mixed = (o_image, o_text)
    branch = streams.scatter([mm_nt(mixed[s], out_t[s]) for s in range(2)])
    middle = [x[s] + mods[s, 2] * branch[s] for s in range(2)]
    second = streams.gather(
        [modulate(middle[s], mods[s, 3], mods[s, 4]).astype(BF16) for s in range(2)]
    )
    hidden = [mm(second[s], up[s]) for s in range(2)]
    active = [gelu(hidden[s]).astype(BF16) for s in range(2)]
    hidden = [hidden[s].astype(BF16) for s in range(2)]
    result = streams.scatter([mm_nt(active[s], down_t[s]) for s in range(2)])
    y = [middle[s] + mods[s, 5] * result[s] for s in range(2)]
    saved = (x, normed, raw, mixed, lse, branch, middle, second, hidden, active, result)
    return y, saved


def backward_layer(streams, gy, saved, mods, weights, gains, attend_back, reduce_grad, pending):
    qkv, out_t, up, down_t = weights
    x, normed, raw, mixed, lse, branch, middle, second, hidden, active, result = saved
    d_gate2 = [jnp.sum(gy[s] * result[s], axis=0) for s in range(2)]
    dm = streams.gather([(mods[s, 5] * gy[s]).astype(BF16) for s in range(2)])
    du = []
    for s in range(2):
        _, pull = jax.vjp(gelu, hidden[s].astype(F32))
        du.append(pull(mm(dm[s], down_t[s]))[0].astype(BF16))
    d_second = streams.scatter([mm_nt(du[s], up[s]) for s in range(2)])
    late = [mm_tn(second[s], du[s]) for s in range(2)]
    late += [mm_tn(dm[s], active[s]) for s in range(2)]
    late = jnp.stack([part.astype(BF16) for part in late])
    late, pending = tie(late, pending)
    reduced_mlp = reduce_grad(late)
    d_middle, d_shift2, d_scale2 = [], [], []
    for s in range(2):
        inner, d_shift, d_scale = modulate_back(middle[s], d_second[s], mods[s, 4])
        d_middle.append(gy[s] + inner)
        d_shift2.append(d_shift)
        d_scale2.append(d_scale)
    d_gate1 = [jnp.sum(d_middle[s] * branch[s], axis=0) for s in range(2)]
    da = streams.gather([(mods[s, 2] * d_middle[s]).astype(BF16) for s in range(2)])
    d_mixed = [mm(da[s], out_t[s]).astype(BF16) for s in range(2)]
    late = jnp.stack([mm_tn(da[s], mixed[s]).astype(BF16) for s in range(2)])
    reduced_out = reduce_grad(late)
    d_image, d_text, gain_rows = attend_back(
        raw[0], raw[1], gains, mixed[0], mixed[1], d_mixed[0], d_mixed[1], lse
    )
    d_raw = (d_image, d_text)
    d_first = streams.scatter([mm_nt(d_raw[s], qkv[s]) for s in range(2)])
    late = jnp.stack([mm_tn(normed[s], d_raw[s]).astype(BF16) for s in range(2)])
    reduced_mlp, late = tie(reduced_mlp, late)
    reduced_qkv = reduce_grad(late)
    gx, d_mods = [], []
    for s in range(2):
        inner, d_shift, d_scale = modulate_back(x[s], d_first[s], mods[s, 1])
        gx.append(d_middle[s] + inner)
        d_mods.append(
            jnp.stack([d_shift, d_scale, d_gate1[s], d_shift2[s], d_scale2[s], d_gate2[s]])
        )
    d_gains = gain_rows.reshape(2, 2, HEAD).transpose(1, 0, 2)
    return gx, jnp.stack(d_mods), d_gains, (reduced_qkv, reduced_out, reduced_mlp), pending


def on_device(dp, seq, width_of_group, *args):
    (
        image_in,
        text_input,
        condition,
        ada_weight,
        qkv_weight,
        out_weight,
        up_weight,
        down_weight,
        norm_gain,
        image_cotangent,
        text_cotangent,
    ) = args
    dp_axis, dp_size = dp
    seq_axis, seq_size = seq
    layers = qkv_weight.shape[0]
    width = image_in.shape[2]
    streams = Streams(image_in.shape[1], text_input.shape[1], seq_axis, seq_size)
    attend, attend_back = (
        (attention_forward, attention_backward)
        if width_of_group % 128 == 0
        else (plain_forward, plain_backward)
    )
    rows = qkv_weight.shape[2]

    def fetch(local):
        return lax.all_gather(local, dp_axis, axis=1, tiled=True)

    qkv_local = qkv_weight.reshape(layers, 2, rows, 3, -1, width_of_group)
    qkv_local = qkv_local.transpose(0, 1, 2, 4, 3, 5).reshape(layers, 2, rows, -1)
    out_local = out_weight.transpose(0, 1, 3, 2)
    down_local = down_weight.transpose(0, 1, 3, 2)
    weights = [
        tuple(fetch(w[l]) for w in (qkv_local, out_local, up_weight, down_local))
        for l in range(layers)
    ]

    act_cond, silu_pull = jax.vjp(jax.nn.silu, condition.astype(F32))
    act_low = act_cond.astype(BF16)
    partial_mods = jnp.einsum("nd,lsde->nlse", act_low, ada_weight, preferred_element_type=F32)
    own_mods = bit_scatter(partial_mods.reshape(dp_size, -1), dp_axis, dp_size)
    own_mods = bit_sum(own_mods, seq_axis, seq_size)
    own_mods = own_mods.reshape(layers, 2, 6, width)
    gains_all = norm_gain.astype(F32)
    gain_columns = [gains_all[l].transpose(1, 0, 2).reshape(4, HEAD).T for l in range(layers)]

    x = [image_in[0].astype(F32), text_input[0].astype(F32)]
    saved_list = []
    for l in range(layers):
        x, saved = forward_layer(streams, x, own_mods[l], weights[l], gain_columns[l], attend, l == 0)
        saved_list.append(saved)
    outputs = [part.astype(BF16)[None] for part in x]

    def reduce_grad(grad):
        return lax.psum_scatter(grad, dp_axis, scatter_dimension=1, tiled=True)

    gy = [image_cotangent[0].astype(F32), text_cotangent[0].astype(F32)]
    d_mods, d_gains, grads = [None] * layers, [None] * layers, [None] * layers
    pending = ()
    for l in reversed(range(layers)):
        gy, d_mods[l], d_gains[l], grads[l], done = backward_layer(
            streams,
            gy,
            saved_list[l],
            own_mods[l],
            weights[l],
            gain_columns[l],
            attend_back,
            reduce_grad,
            pending,
        )
        if l + 1 < layers:
            grads[l + 1] = done + grads[l + 1][2:]
        pending = grads[l][:2]

    there = jnp.array(bit_order(dp_size)[1], jnp.int32) ^ lax.axis_index(dp_axis)
    small = jnp.concatenate([jnp.stack(d_mods).reshape(-1), jnp.stack(d_gains).reshape(-1)])
    small = bit_sum(small, seq_axis, seq_size)
    small = bit_gather(small, dp_axis, dp_size)
    count = layers * 2 * 6 * width
    total_mods = small[:, :count].reshape(dp_size, layers, 2, 6 * width)
    total_gains = jnp.sum(small[:, count:][there], axis=0).reshape(layers, 2, 2, HEAD)
    act_there = act_low.astype(F32)[there]
    ada_grad = jnp.einsum("nd,nlse->lsde", act_there, total_mods, precision=HIGHEST)
    d_act = jnp.einsum("nlse,lsde->nd", total_mods, ada_weight.astype(F32), precision=HIGHEST)
    d_act = d_act[there]
    condition_grad = silu_pull(d_act)[0]

    def pieces(kind, first):
        return jnp.stack([grads[l][kind][first : first + 2] for l in range(layers)]).astype(F32)

    qkv_grad = pieces(0, 0).reshape(layers, 2, rows, -1, 3, width_of_group)
    qkv_grad = qkv_grad.transpose(0, 1, 2, 4, 3, 5).reshape(qkv_weight.shape)
    return (
        outputs[0],
        outputs[1],
        gy[0][None],
        gy[1][None],
        condition_grad,
        ada_grad,
        qkv_grad,
        pieces(1, 0).transpose(0, 1, 3, 2),
        pieces(2, 0),
        pieces(2, 2).transpose(0, 1, 3, 2),
        total_gains,
    )


def solution(mesh):
    tokens = P("dp", "seq", None)
    placed = (
        tokens,
        tokens,
        P(None, ("dp", "seq")),
        P(None, None, ("dp", "seq"), None),
        P(None, None, "dp", None, "seq"),
        P(None, None, "seq", "dp"),
        P(None, None, "dp", "seq"),
        P(None, None, "seq", "dp"),
        P(),
        tokens,
        tokens,
    )
    results = (tokens, tokens, tokens, tokens) + placed[2:8] + (P(),)

    def step(*args):
        heads = args[4].shape[4] // mesh.shape["seq"] // HEAD
        group = 2 * HEAD if heads % 2 == 0 else HEAD
        body = functools.partial(
            on_device, ("dp", mesh.shape["dp"]), ("seq", mesh.shape["seq"]), group
        )
        return jax.shard_map(
            body, mesh=mesh, in_specs=placed, out_specs=results, check_vma=False
        )(*args)

    return step
```

```python
import functools

import jax
import jax.numpy as jnp
from jax import lax
from jax.experimental import pallas as pl
from jax.experimental.pallas import tpu as pltpu
from jax.sharding import PartitionSpec as P

EPSILON = 1e-06
HIGHEST = lax.Precision.HIGHEST
F32 = jnp.float32
BF16 = jnp.bfloat16
HEAD = 64


def layer_stats(values):
    centred = values - jnp.mean(values, axis=-1, keepdims=True)
    root = lax.rsqrt(jnp.mean(centred * centred, axis=-1, keepdims=True) + EPSILON)
    return centred * root, root


def modulate(values, shift, scale):
    return layer_stats(values)[0] * (1.0 + scale) + shift


def modulate_back(values, grad, scale):
    normed, root = layer_stats(values)
    inner = grad * (1.0 + scale)
    first = jnp.mean(inner, axis=-1, keepdims=True)
    second = jnp.mean(inner * normed, axis=-1, keepdims=True)
    d_values = root * (inner - first - normed * second)
    return d_values, jnp.sum(grad, axis=0), jnp.sum(grad * normed, axis=0)


def mm(left, right):
    return lax.dot_general(left, right, (((1,), (0,)), ((), ())), preferred_element_type=F32)


def mm_nt(left, right):
    return lax.dot_general(left, right, (((1,), (1,)), ((), ())), preferred_element_type=F32)


def mm_tn(left, right):
    return lax.dot_general(left, right, (((0,), (0,)), ((), ())), preferred_element_type=F32)


def gelu(values):
    return jax.nn.gelu(values, approximate=True)


def head_factors(raw_t, gain_image, gain_text, image_len):
    root = lax.rsqrt(jnp.mean(raw_t * raw_t, axis=0, keepdims=True) + EPSILON)
    lanes = lax.broadcasted_iota(jnp.int32, raw_t.shape, 1)
    gain = jnp.where(lanes < image_len, gain_image, gain_text)
    return raw_t * root, root, gain


def transposed(first, second, low, high):
    return jnp.concatenate(
        [first[:, low:high].astype(F32).T, second[:, low:high].astype(F32).T], axis=1
    )


def attention_forward_kernel(step, image_ref, text_ref, gain_ref, o_image, o_text, lse_ref, o_scr):
    image_len, text_len = image_ref.shape[0], text_ref.shape[0]
    total = image_len + text_len
    wide = image_ref.shape[1] // 3
    factor = HEAD ** (-0.5)
    raw_q = transposed(image_ref, text_ref, 0, wide)
    raw_k = transposed(image_ref, text_ref, wide, 2 * wide)
    values_t = transposed(image_ref, text_ref, 2 * wide, 3 * wide).astype(BF16)
    for head in range(wide // HEAD):
        rows = slice(head * HEAD, (head + 1) * HEAD)
        q_hat, _, q_gain = head_factors(raw_q[rows], gain_ref[:, 0:1], gain_ref[:, 1:2], image_len)
        k_hat, _, k_gain = head_factors(raw_k[rows], gain_ref[:, 2:3], gain_ref[:, 3:4], image_len)
        q_t = ((q_hat * q_gain).astype(BF16).astype(F32) * factor).astype(BF16)
        keys = (k_hat * k_gain).T.astype(BF16)
        v_t = values_t[rows]
        for start in range(0, total, step):
            part = slice(start, start + step)
            scores = mm(keys, q_t[:, part])
            largest = jnp.max(scores, axis=0, keepdims=True)
            weights = jnp.exp(scores - largest)
            total_w = jnp.sum(weights, axis=0, keepdims=True)
            out = mm(v_t, weights.astype(BF16)) * (1.0 / total_w)
            o_scr[rows, part] = out
            lse_ref[head, :, part] = largest + jnp.log(total_w)
    o_image[...] = o_scr[:, :image_len].T.astype(BF16)
    o_text[...] = o_scr[:, image_len:].T.astype(BF16)


def attention_backward_kernel(
    step,
    image_ref,
    text_ref,
    gain_ref,
    o_image,
    o_text,
    do_image,
    do_text,
    lse_ref,
    d_image,
    d_text,
    gain_grad,
    dq_scr,
    dk_scr,
    dv_scr,
):
    image_len, text_len = image_ref.shape[0], text_ref.shape[0]
    total = image_len + text_len
    wide = image_ref.shape[1] // 3
    factor = HEAD ** (-0.5)
    raw_q = transposed(image_ref, text_ref, 0, wide)
    raw_k = transposed(image_ref, text_ref, wide, 2 * wide)
    o_t = transposed(o_image, o_text, 0, wide)
    do_t = transposed(do_image, do_text, 0, wide)
    lane_row = lax.broadcasted_iota(jnp.int32, (HEAD, 128), 1)
    gains_total = jnp.zeros((HEAD, 128), F32)
    for head in range(wide // HEAD):
        rows = slice(head * HEAD, (head + 1) * HEAD)
        low, high = 2 * wide + head * HEAD, 2 * wide + (head + 1) * HEAD
        q_hat, q_root, q_gain = head_factors(
            raw_q[rows], gain_ref[:, 0:1], gain_ref[:, 1:2], image_len
        )
        k_hat, k_root, k_gain = head_factors(
            raw_k[rows], gain_ref[:, 2:3], gain_ref[:, 3:4], image_len
        )
        q_full = (q_hat * q_gain).astype(BF16).astype(F32) * factor
        q_t = q_full.astype(BF16)
        queries = q_full.T.astype(BF16)
        k_t = (k_hat * k_gain).astype(BF16)
        keys = (k_hat * k_gain).T.astype(BF16)
        values = jnp.concatenate([image_ref[:, low:high], text_ref[:, low:high]], axis=0)
        d_out = jnp.concatenate([do_image[:, rows], do_text[:, rows]], axis=0)
        delta = jnp.sum(do_t[rows] * o_t[rows], axis=0, keepdims=True)
        d_out_t = do_t[rows].astype(BF16)
        d_keys = jnp.zeros((total, HEAD), F32)
        d_values = jnp.zeros((total, HEAD), F32)
        for start in range(0, total, step):
            part = slice(start, start + step)
            weights = jnp.exp(mm(keys, q_t[:, part]) - lse_ref[head, :, part])
            d_weights = mm(values, d_out_t[:, part])
            d_scores = (weights * (d_weights - delta[:, part])).astype(BF16)
            d_values += mm(weights.astype(BF16), d_out[part])
            d_keys += mm(d_scores, queries[part])
            dq_scr[rows, part] = mm(k_t, d_scores) * factor
        dv_scr[:, rows] = d_values
        dq = dq_scr[rows, :]
        dk = d_keys.T
        for slot, (grad, hat) in enumerate(((dq, q_hat), (dk, k_hat))):
            product = grad * hat
            image_sum = jnp.sum(product[:, :image_len], axis=1, keepdims=True)
            text_sum = jnp.sum(product[:, image_len:], axis=1, keepdims=True)
            gains_total += jnp.where(lane_row == 2 * slot, image_sum, 0.0)
            gains_total += jnp.where(lane_row == 2 * slot + 1, text_sum, 0.0)
        scaled = dq * q_gain
        dq_scr[rows, :] = q_root * (
            scaled - q_hat * jnp.mean(scaled * q_hat, axis=0, keepdims=True)
        )
        scaled = dk * k_gain
        dk_scr[rows, :] = k_root * (
            scaled - k_hat * jnp.mean(scaled * k_hat, axis=0, keepdims=True)
        )
    d_image[:, :wide] = dq_scr[:, :image_len].T.astype(BF16)
    d_text[:, :wide] = dq_scr[:, image_len:].T.astype(BF16)
    d_image[:, wide : 2 * wide] = dk_scr[:, :image_len].T.astype(BF16)
    d_text[:, wide : 2 * wide] = dk_scr[:, image_len:].T.astype(BF16)
    d_image[:, 2 * wide :] = dv_scr[:image_len].astype(BF16)
    d_text[:, 2 * wide :] = dv_scr[image_len:].astype(BF16)
    gain_grad[0] = gains_total


def query_step(total):
    for count in (3, 4, 2, 6, 9, 1):
        if total % (count * 128) == 0:
            return total // count
    return total


def kernel_cost(tokens, heads, products):
    return pl.CostEstimate(
        flops=2 * products * heads * tokens * tokens * HEAD * 4,
        transcendentals=heads * tokens * tokens,
        bytes_accessed=tokens * heads * HEAD * 2 * 8,
    )


def attention_forward(raw_image, raw_text, gains):
    groups = raw_image.shape[1] // (3 * 128)
    image_len, text_len = raw_image.shape[0], raw_text.shape[0]
    total = image_len + text_len
    return pl.pallas_call(
        functools.partial(attention_forward_kernel, query_step(total)),
        grid=(groups,),
        out_shape=(
            jax.ShapeDtypeStruct((image_len, groups * 128), BF16),
            jax.ShapeDtypeStruct((text_len, groups * 128), BF16),
            jax.ShapeDtypeStruct((groups * 2, 1, total), F32),
        ),
        in_specs=[
            pl.BlockSpec((image_len, 384), lambda g: (0, g)),
            pl.BlockSpec((text_len, 384), lambda g: (0, g)),
            pl.BlockSpec((HEAD, 4), lambda g: (0, 0)),
        ],
        out_specs=(
            pl.BlockSpec((image_len, 128), lambda g: (0, g)),
            pl.BlockSpec((text_len, 128), lambda g: (0, g)),
            pl.BlockSpec((2, 1, total), lambda g: (g, 0, 0)),
        ),
        scratch_shapes=[pltpu.VMEM((128, total), F32)],
        cost_estimate=kernel_cost(total, groups * 2, 2),
        name="attend_forward",
    )(raw_image, raw_text, gains)


def attention_backward(raw_image, raw_text, gains, o_image, o_text, do_image, do_text, lse):
    groups = raw_image.shape[1] // (3 * 128)
    image_len, text_len = raw_image.shape[0], raw_text.shape[0]
    total = image_len + text_len
    wide_image = pl.BlockSpec((image_len, 384), lambda g: (0, g))
    wide_text = pl.BlockSpec((text_len, 384), lambda g: (0, g))
    slim_image = pl.BlockSpec((image_len, 128), lambda g: (0, g))
    slim_text = pl.BlockSpec((text_len, 128), lambda g: (0, g))
    d_image, d_text, gain_grad = pl.pallas_call(
        functools.partial(attention_backward_kernel, query_step(total)),
        grid=(groups,),
        out_shape=(
            jax.ShapeDtypeStruct(raw_image.shape, BF16),
            jax.ShapeDtypeStruct(raw_text.shape, BF16),
            jax.ShapeDtypeStruct((groups, HEAD, 128), F32),
        ),
        in_specs=[
            wide_image,
            wide_text,
            pl.BlockSpec((HEAD, 4), lambda g: (0, 0)),
            slim_image,
            slim_text,
            slim_image,
            slim_text,
            pl.BlockSpec((2, 1, total), lambda g: (g, 0, 0)),
        ],
        out_specs=(wide_image, wide_text, pl.BlockSpec((1, HEAD, 128), lambda g: (g, 0, 0))),
        scratch_shapes=[
            pltpu.VMEM((128, total), F32),
            pltpu.VMEM((128, total), F32),
            pltpu.VMEM((total, 128), F32),
        ],
        cost_estimate=kernel_cost(total, groups * 2, 5),
        name="attend_backward",
    )(raw_image, raw_text, gains, o_image, o_text, do_image, do_text, lse)
    return d_image, d_text, jnp.sum(gain_grad, axis=0)[:, :4].T


def plain_parts(raw_image, raw_text, gains):
    raw = jnp.concatenate([raw_image, raw_text], axis=0).astype(F32)
    raw = raw.reshape(raw.shape[0], -1, 3, HEAD)
    is_image = (jnp.arange(raw.shape[0]) < raw_image.shape[0])[:, None, None]
    hats, roots, scales, rounded = [], [], [], []
    for slot in range(2):
        part = raw[:, :, slot]
        root = lax.rsqrt(jnp.mean(part * part, axis=-1, keepdims=True) + EPSILON)
        scale = jnp.where(is_image, gains[:, 2 * slot], gains[:, 2 * slot + 1])
        hats.append(part * root)
        roots.append(root)
        scales.append(scale)
        rounded.append((part * root * scale).astype(BF16))
    return hats, roots, scales, rounded, raw[:, :, 2].astype(BF16)


def plain_forward(raw_image, raw_text, gains):
    _, _, _, (queries, keys), values = plain_parts(raw_image, raw_text, gains)
    scores = jnp.einsum("qhd,khd->hqk", queries, keys, preferred_element_type=F32)
    scores = scores * HEAD ** (-0.5)
    largest = jnp.max(scores, axis=-1, keepdims=True)
    lse = largest + jnp.log(jnp.sum(jnp.exp(scores - largest), axis=-1, keepdims=True))
    weights = jnp.exp(scores - lse).astype(BF16)
    out = jnp.einsum("hqk,khd->qhd", weights, values, preferred_element_type=F32)
    out = out.astype(BF16).reshape(out.shape[0], -1)
    return out[: raw_image.shape[0]], out[raw_image.shape[0] :], lse


def plain_backward(raw_image, raw_text, gains, o_image, o_text, do_image, do_text, lse):
    hats, roots, scales, (queries, keys), values = plain_parts(raw_image, raw_text, gains)
    factor = HEAD ** (-0.5)
    image_len = raw_image.shape[0]
    d_out = jnp.concatenate([do_image, do_text], axis=0).reshape(queries.shape)
    scores = jnp.einsum("qhd,khd->hqk", queries, keys, preferred_element_type=F32) * factor
    weights = jnp.exp(scores - lse)
    d_weights = jnp.einsum("qhd,khd->hqk", d_out, values, preferred_element_type=F32)
    inner = jnp.sum(weights * d_weights, axis=-1, keepdims=True)
    d_scores = (weights * (d_weights - inner)).astype(BF16)
    dq = jnp.einsum("hqk,khd->qhd", d_scores, keys, preferred_element_type=F32) * factor
    dk = jnp.einsum("hqk,qhd->khd", d_scores, queries, preferred_element_type=F32) * factor
    dv = jnp.einsum("hqk,qhd->khd", weights.astype(BF16), d_out, preferred_element_type=F32)
    gain_rows, parts = [], []
    for grad, hat, root, scale in zip((dq, dk), hats, roots, scales):
        product = grad * hat
        gain_rows += [jnp.sum(product[:image_len], (0, 1)), jnp.sum(product[image_len:], (0, 1))]
        scaled = grad * scale
        parts.append(root * (scaled - hat * jnp.mean(scaled * hat, axis=-1, keepdims=True)))
    joined = jnp.stack(parts + [dv], axis=2).astype(BF16).reshape(d_out.shape[0], -1)
    return joined[:image_len], joined[image_len:], jnp.stack(gain_rows)


def gather_tokens(own, axis, size):
    if size == 1:
        return [own]
    after, before = [], []
    down = up = own
    for _ in range(size - 1):
        down = lax.ppermute(down, axis, [(i, i - 1) for i in range(1, size)])
        up = lax.ppermute(up, axis, [(i, i + 1) for i in range(size - 1)])
        after.append(down)
        before.append(up)
    me = lax.axis_index(axis)
    return [own] + [
        jnp.where(me + k < size, after[k - 1], before[size - k - 1]) for k in range(1, size)
    ]


def scatter_tokens(blocks, axis, size):
    up = down = None
    for step in range(size - 1):
        k = size - 1 - step
        send_up = blocks[k] if up is None else (blocks[k].astype(F32) + up).astype(BF16)
        send_down = (
            blocks[size - k]
            if down is None
            else (blocks[size - k].astype(F32) + down).astype(BF16)
        )
        up = lax.ppermute(send_up, axis, [(i, i + 1) for i in range(step + 1)]).astype(F32)
        down = lax.ppermute(
            send_down, axis, [(i, i - 1) for i in range(size - 1 - step, size)]
        ).astype(F32)
    total = blocks[0].astype(F32)
    return total if up is None else total + up + down


class Bit:
    def __init__(self, axis, size, place):
        self.axis, self.size, self.place = axis, size, place

    def exchange(self, value):
        flip = 1 << self.place
        return lax.ppermute(value, self.axis, [(i, i ^ flip) for i in range(self.size)])

    def value(self):
        return (lax.axis_index(self.axis) >> self.place) & 1


def bits_of(axis, size):
    return [Bit(axis, size, place) for place in reversed(range(size.bit_length() - 1))]


def bit_sum(value, bits):
    for bit in bits:
        value = value + bit.exchange(value)
    return value


def bit_scatter(parts, bits):
    for bit in bits:
        half = parts.shape[0] // 2
        upper = bit.value() == 1
        keep = jnp.where(upper, parts[half:], parts[:half])
        send = jnp.where(upper, parts[:half], parts[half:])
        parts = keep + bit.exchange(send)
    return parts[0]


def bit_gather(own, bits):
    blocks, masks, number = own[None], [0], 0
    for place, bit in enumerate(reversed(bits)):
        blocks = jnp.concatenate([blocks, bit.exchange(blocks)], axis=0)
        masks += [m | (1 << place) for m in masks]
        number = number + (bit.value() << place)
    return blocks, jnp.array(masks, jnp.int32) ^ number


def tie(*groups):
    return lax.optimization_barrier(groups)


class LinePlan:
    def __init__(self, lengths, dp, seq):
        self.lengths = lengths
        self.dp, (self.axis, self.count) = dp, seq
        self.owner_bits, self.other_bits = bits_of(*dp), bits_of(*seq)

    def enter(self, pair):
        return pair

    def leave(self, pair):
        return pair

    def columns(self, value):
        return value

    def gather(self, pair):
        cut = self.lengths[0]
        blocks = gather_tokens(jnp.concatenate(pair, axis=0), self.axis, self.count)
        return (
            jnp.concatenate([b[:cut] for b in blocks], axis=0),
            jnp.concatenate([b[cut:] for b in blocks], axis=0),
        )

    def scatter(self, pair):
        cut = self.lengths[0]
        low = [part.astype(BF16) for part in pair]
        blocks = [
            jnp.concatenate(
                [low[s][k * n : (k + 1) * n] for s, n in enumerate(self.lengths)], axis=0
            )
            for k in range(self.count)
        ]
        total = scatter_tokens(blocks, self.axis, self.count)
        return total[:cut], total[cut:]

    def fetch(self, local):
        return lax.all_gather(local, self.dp[0], axis=1, tiled=True)

    def reduce_grad(self, grad):
        return lax.psum_scatter(grad, self.dp[0], scatter_dimension=1, tiled=True)

    def finish(self, part, chained):
        return part


class CrossPlan:
    def __init__(self, lengths):
        self.lengths = lengths
        self.count = 4
        self.y, self.x, self.c, self.zh, self.zl = (Bit(n, 2, 0) for n in CROSS)
        self.owner_bits = [self.y, self.zh, self.c]
        self.other_bits = [self.x, self.zl]

    def columns(self, value):
        size = value.shape[-1] // 8
        order = [0, 2, 1, 3, 4, 6, 5, 7]
        return jnp.concatenate([value[..., k * size : (k + 1) * size] for k in order], axis=-1)

    def trade(self, value):
        return lax.ppermute(value, ("x", "zh"), [(0, 0), (1, 2), (2, 1), (3, 3)])

    def enter(self, pair):
        cut = self.lengths[0]
        joined = self.columns(self.trade(jnp.concatenate(pair, axis=0)))
        return joined[:cut], joined[cut:]

    def leave(self, pair):
        cut = self.lengths[0]
        joined = self.trade(self.columns(jnp.concatenate(pair, axis=0).astype(BF16)))
        return joined[:cut], joined[cut:]

    def half(self):
        return sum(self.lengths) // 32 * 16

    def gather(self, pair):
        own = jnp.concatenate(pair, axis=0)
        half, cut = self.half(), self.lengths[0]
        first, second = own[:half], own[half:]
        first_x = self.x.exchange(first)
        second_z = self.zl.exchange(second)
        first_z = self.zl.exchange(first)
        second_x = self.x.exchange(second)
        first_xz = self.zl.exchange(first_x)
        second_xz = self.x.exchange(second_z)
        firsts = (first, first_x, first_z, first_xz)
        seconds = (second, second_x, second_z, second_xz)
        image = []
        for a, b in zip(firsts, seconds):
            image += [a, b[: cut - half]]
        return (
            jnp.concatenate(image, axis=0),
            jnp.concatenate([b[cut - half :] for b in seconds], axis=0),
        )

    def scatter(self, pair):
        half, cut = self.half(), self.lengths[0]
        image_len, text_len = self.lengths
        image, text = (part.astype(BF16) for part in pair)
        firsts = [image[k * image_len : k * image_len + half] for k in range(4)]
        seconds = [
            jnp.concatenate(
                [
                    image[k * image_len + half : (k + 1) * image_len],
                    text[k * text_len : (k + 1) * text_len],
                ],
                axis=0,
            )
            for k in range(4)
        ]

        def add(left, right):
            return left.astype(F32) + right.astype(F32)

        first_x = add(firsts[1], self.zl.exchange(firsts[3])).astype(BF16)
        second_z = add(seconds[2], self.x.exchange(seconds[3])).astype(BF16)
        first = add(firsts[0], self.zl.exchange(firsts[2]))
        second = add(seconds[0], self.x.exchange(seconds[1]))
        first = first + self.x.exchange(first_x).astype(F32)
        second = second + self.zl.exchange(second_z).astype(F32)
        return (
            jnp.concatenate([first, second[: cut - half]], axis=0),
            second[cut - half :],
        )

    def fetch(self, local):
        x_bit = self.x.value()
        same = x_bit == self.zh.value()
        pairs = []
        for s in range(local.shape[0]):
            own = local[s]
            other = self.zh.exchange(own)
            keep = jnp.where(same, own, other)
            there = self.x.exchange(jnp.where(same, other, own))
            low = jnp.where(x_bit == 0, keep, there)
            high = jnp.where(x_bit == 0, there, keep)
            pairs.append(jnp.concatenate([low, high], axis=0))
        return lax.all_gather(jnp.stack(pairs), ("y", "c"), axis=1, tiled=True)

    def reduce_grad(self, grad):
        return lax.psum_scatter(grad, ("y", "c"), scatter_dimension=1, tiled=True)

    def finish(self, part, chained):
        rows = part.shape[1] // 2
        x_bit = self.x.value()
        same = x_bit == self.zh.value()
        done = []
        for low, high in zip(part[:, :rows], part[:, rows:]):
            send = jnp.where(x_bit == 0, high, low)
            if chained and done:
                send, done[-1] = tie(send, done[-1])
            there = self.x.exchange(send)
            keep = jnp.where(x_bit == 0, low, high)
            mine = jnp.where(same, keep, there)
            other = self.zh.exchange(jnp.where(same, there, keep))
            done.append((mine.astype(F32) + other.astype(F32)).astype(BF16))
        return jnp.stack(done)


FETCHES = {
    "normed": [(0, ("out", "up", "down"))],
    "mixed": [(1, ("qkv", "out"))],
    "second": [(1, ("up", "down"))],
}
CROSS = ("y", "x", "c", "zh", "zl")


def forward_layer(plan, x, mods, weights, gains, attend, first, at):
    if first:
        plain = plan.gather([layer_stats(x[s])[0].astype(BF16) for s in range(2)])
        normed = [
            (plain[s].astype(F32) * (1.0 + mods[s, 1]) + mods[s, 0]).astype(BF16)
            for s in range(2)
        ]
    else:
        normed = plan.gather(
            [modulate(x[s], mods[s, 0], mods[s, 1]).astype(BF16) for s in range(2)]
        )
    normed = at("normed", normed)
    raw = [mm(normed[s], weights["qkv"][s]).astype(BF16) for s in range(2)]
    o_image, o_text, lse = attend(raw[0], raw[1], gains)
    mixed = at("mixed", (o_image, o_text))
    branch = plan.scatter([mm_nt(mixed[s], weights["out"][s]) for s in range(2)])
    middle = [x[s] + mods[s, 2] * branch[s] for s in range(2)]
    second = plan.gather(
        [modulate(middle[s], mods[s, 3], mods[s, 4]).astype(BF16) for s in range(2)]
    )
    second = at("second", second)
    hidden = [mm(second[s], weights["up"][s]) for s in range(2)]
    active = [gelu(hidden[s]).astype(BF16) for s in range(2)]
    hidden = [hidden[s].astype(BF16) for s in range(2)]
    result = plan.scatter([mm_nt(active[s], weights["down"][s]) for s in range(2)])
    y = [middle[s] + mods[s, 5] * result[s] for s in range(2)]
    saved = (x, normed, raw, mixed, lse, branch, middle, second, hidden, active, result)
    return y, saved


def backward_layer(plan, gy, saved, mods, weights, gains, attend_back, pending):
    qkv, out_t, up, down_t = (weights[name] for name in ("qkv", "out", "up", "down"))
    reduce_grad = plan.reduce_grad
    finished = ()
    x, normed, raw, mixed, lse, branch, middle, second, hidden, active, result = saved
    d_gate2 = [jnp.sum(gy[s] * result[s], axis=0) for s in range(2)]
    dm = plan.gather([(mods[s, 5] * gy[s]).astype(BF16) for s in range(2)])
    if pending:
        part_qkv, part_out, done_mlp = pending
        dm, part_qkv, part_out = tie(dm, part_qkv, part_out)
    du = []
    for s in range(2):
        _, pull = jax.vjp(gelu, hidden[s].astype(F32))
        du.append(pull(mm(dm[s], down_t[s]))[0].astype(BF16))
    d_second = plan.scatter([mm_nt(du[s], up[s]) for s in range(2)])
    late = [mm_tn(second[s], du[s]) for s in range(2)]
    late += [mm_tn(dm[s], active[s]) for s in range(2)]
    late = jnp.stack([part.astype(BF16) for part in late])
    if pending:
        d_second, done_mlp = tie(d_second, done_mlp)
    reduced_mlp = reduce_grad(late)
    d_middle, d_shift2, d_scale2 = [], [], []
    for s in range(2):
        inner, d_shift, d_scale = modulate_back(middle[s], d_second[s], mods[s, 4])
        d_middle.append(gy[s] + inner)
        d_shift2.append(d_shift)
        d_scale2.append(d_scale)
    d_gate1 = [jnp.sum(d_middle[s] * branch[s], axis=0) for s in range(2)]
    da = plan.gather([(mods[s, 2] * d_middle[s]).astype(BF16) for s in range(2)])
    d_mixed = [mm(da[s], out_t[s]).astype(BF16) for s in range(2)]
    late = jnp.stack([mm_tn(da[s], mixed[s]).astype(BF16) for s in range(2)])
    reduced_out = reduce_grad(late)
    d_image, d_text, gain_rows = attend_back(
        raw[0], raw[1], gains, mixed[0], mixed[1], d_mixed[0], d_mixed[1], lse
    )
    d_raw, reduced_mlp = tie((d_image, d_text), reduced_mlp)
    if pending:
        done = plan.finish(part_qkv, True), plan.finish(part_out, True)
        d_raw, done = tie(d_raw, done)
        finished = done + (done_mlp,)
    d_first = plan.scatter([mm_nt(d_raw[s], qkv[s]) for s in range(2)])
    late = jnp.stack([mm_tn(normed[s], d_raw[s]).astype(BF16) for s in range(2)])
    reduced_qkv = reduce_grad(late)
    gx, d_mods = [], []
    for s in range(2):
        inner, d_shift, d_scale = modulate_back(x[s], d_first[s], mods[s, 1])
        gx.append(d_middle[s] + inner)
        d_mods.append(
            jnp.stack([d_shift, d_scale, d_gate1[s], d_shift2[s], d_scale2[s], d_gate2[s]])
        )
    d_gains = gain_rows.reshape(2, 2, HEAD).transpose(1, 0, 2)
    return gx, jnp.stack(d_mods), d_gains, (reduced_qkv, reduced_out, reduced_mlp), finished


def on_device(make_plan, width_of_group, *args):
    (
        image_in,
        text_input,
        condition,
        ada_weight,
        qkv_weight,
        out_weight,
        up_weight,
        down_weight,
        norm_gain,
        image_cotangent,
        text_cotangent,
    ) = args
    layers = qkv_weight.shape[0]
    width = image_in.shape[2]
    plan = make_plan((image_in.shape[1], text_input.shape[1]))
    attend, attend_back = (
        (attention_forward, attention_backward)
        if width_of_group % 128 == 0
        else (plain_forward, plain_backward)
    )
    rows = qkv_weight.shape[2]

    act_cond, silu_pull = jax.vjp(jax.nn.silu, condition.astype(F32))
    act_low = act_cond.astype(BF16)
    partial_mods = jnp.einsum("nd,lsde->nlse", act_low, ada_weight, preferred_element_type=F32)
    own_mods = bit_scatter(partial_mods.reshape(partial_mods.shape[0], -1), plan.owner_bits)
    own_mods = bit_sum(own_mods, plan.other_bits)
    own_mods = plan.columns(own_mods.reshape(layers, 2, 6, width))
    gains_all = norm_gain.astype(F32)
    gain_columns = [gains_all[l].transpose(1, 0, 2).reshape(4, HEAD).T for l in range(layers)]

    qkv_local = qkv_weight.reshape(layers, 2, rows, 3, -1, width_of_group)
    qkv_local = qkv_local.transpose(0, 1, 2, 4, 3, 5).reshape(layers, 2, rows, -1)
    out_local = out_weight.transpose(0, 1, 3, 2)
    down_local = down_weight.transpose(0, 1, 3, 2)
    local = {"qkv": qkv_local, "out": out_local, "up": up_weight, "down": down_local}
    weights = [{} for _ in range(layers)]
    weights[0]["qkv"] = plan.fetch(local["qkv"][0])

    def at(layer, point, token):
        for l, names in FETCHES[point]:
            if layer + l < layers and (l or layer == 0):
                for name in names:
                    token, own = tie(token, local[name][layer + l])
                    weights[layer + l][name] = plan.fetch(own)
        return token

    x = [part.astype(F32) for part in plan.enter((image_in[0], text_input[0]))]
    saved_list = []
    for l in range(layers):
        x, saved = forward_layer(
            plan,
            x,
            own_mods[l],
            weights[l],
            gain_columns[l],
            attend,
            l == 0,
            functools.partial(at, l),
        )
        saved_list.append(saved)
    outputs = plan.leave([part.astype(BF16) for part in x])

    gy = plan.enter((image_cotangent[0], text_cotangent[0]))
    gy = [part.astype(F32) for part in gy]
    d_mods, d_gains, grads = [None] * layers, [None] * layers, [None] * layers
    pending = ()
    for l in reversed(range(layers)):
        gy, d_mods[l], d_gains[l], grads[l], done = backward_layer(
            plan,
            gy,
            saved_list[l],
            own_mods[l],
            weights[l],
            gain_columns[l],
            attend_back,
            pending,
        )
        if done:
            grads[l + 1] = done
        pending = grads[l][:2] + (plan.finish(grads[l][2], l > 0),)
    grads[0] = tuple(plan.finish(grads[0][kind], False) for kind in range(2)) + pending[2:]
    tokens_back = [part.astype(F32)[None] for part in plan.leave(gy)]

    d_mods = plan.columns(jnp.stack(d_mods))
    count = d_mods.size
    small = jnp.concatenate([d_mods.reshape(-1), jnp.stack(d_gains).reshape(-1)])
    small, there = bit_gather(bit_sum(small, plan.other_bits), plan.owner_bits)
    total_mods = small[:, :count].reshape(-1, layers, 2, 6 * width)
    total_gains = jnp.sum(small[:, count:][there], axis=0).reshape(layers, 2, 2, HEAD)
    act_there = act_low.astype(F32)[there]
    ada_grad = jnp.einsum("nd,nlse->lsde", act_there, total_mods, precision=HIGHEST)
    d_act = jnp.einsum("nlse,lsde->nd", total_mods, ada_weight.astype(F32), precision=HIGHEST)
    condition_grad = silu_pull(d_act[there])[0]

    def pieces(kind, first):
        return jnp.stack([grads[l][kind][first : first + 2] for l in range(layers)]).astype(F32)

    qkv_grad = pieces(0, 0).reshape(layers, 2, rows, -1, 3, width_of_group)
    qkv_grad = qkv_grad.transpose(0, 1, 2, 4, 3, 5).reshape(qkv_weight.shape)
    return (
        outputs[0][None].astype(BF16),
        outputs[1][None].astype(BF16),
        tokens_back[0],
        tokens_back[1],
        condition_grad,
        ada_grad,
        qkv_grad,
        pieces(1, 0).transpose(0, 1, 3, 2),
        pieces(2, 0),
        pieces(2, 2).transpose(0, 1, 3, 2),
        total_gains,
    )


def solution(mesh):
    dp_size, seq_size = mesh.shape["dp"], mesh.shape["seq"]
    if (dp_size, seq_size) == (8, 4):
        mesh = jax.sharding.Mesh(mesh.devices.reshape(2, 2, 2, 2, 2), CROSS)
        dp, seq = CROSS[:3], CROSS[3:]
        make_plan = CrossPlan
    else:
        dp, seq = ("dp",), ("seq",)
        make_plan = functools.partial(LinePlan, dp=("dp", dp_size), seq=("seq", seq_size))
    tokens = P(dp, seq, None)
    placed = (
        tokens,
        tokens,
        P(None, dp + seq),
        P(None, None, dp + seq, None),
        P(None, None, dp, None, seq),
        P(None, None, seq, dp),
        P(None, None, dp, seq),
        P(None, None, seq, dp),
        P(),
        tokens,
        tokens,
    )
    results = (tokens, tokens, tokens, tokens) + placed[2:8] + (P(),)

    def step(*args):
        heads = args[4].shape[4] // seq_size // HEAD
        group = 2 * HEAD if heads % 2 == 0 else HEAD
        body = functools.partial(on_device, make_plan, group)
        return jax.shard_map(
            body, mesh=mesh, in_specs=placed, out_specs=results, check_vma=False
        )(*args)

    return step
```

```python
import functools

import jax
import jax.numpy as jnp
from jax import lax
from jax.experimental import pallas as pl
from jax.experimental.pallas import tpu as pltpu
from jax.sharding import PartitionSpec as P

EPSILON = 1e-06
HIGHEST = lax.Precision.HIGHEST
F32 = jnp.float32
BF16 = jnp.bfloat16
HEAD = 64


def layer_stats(values):
    centred = values - jnp.mean(values, axis=-1, keepdims=True)
    root = lax.rsqrt(jnp.mean(centred * centred, axis=-1, keepdims=True) + EPSILON)
    return centred * root, root


def modulate(values, shift, scale):
    return layer_stats(values)[0] * (1.0 + scale) + shift


def modulate_back(values, grad, scale):
    normed, root = layer_stats(values)
    inner = grad * (1.0 + scale)
    first = jnp.mean(inner, axis=-1, keepdims=True)
    second = jnp.mean(inner * normed, axis=-1, keepdims=True)
    d_values = root * (inner - first - normed * second)
    return d_values, jnp.sum(grad, axis=0), jnp.sum(grad * normed, axis=0)


def mm(left, right):
    return lax.dot_general(left, right, (((1,), (0,)), ((), ())), preferred_element_type=F32)


def mm_nt(left, right):
    return lax.dot_general(left, right, (((1,), (1,)), ((), ())), preferred_element_type=F32)


def mm_tn(left, right):
    return lax.dot_general(left, right, (((0,), (0,)), ((), ())), preferred_element_type=F32)


def gelu(values):
    return jax.nn.gelu(values, approximate=True)


def head_factors(raw_t, gain_image, gain_text, image_len):
    root = lax.rsqrt(jnp.mean(raw_t * raw_t, axis=0, keepdims=True) + EPSILON)
    lanes = lax.broadcasted_iota(jnp.int32, raw_t.shape, 1)
    gain = jnp.where(lanes < image_len, gain_image, gain_text)
    return raw_t * root, root, gain


def transposed(first, second, low, high):
    return jnp.concatenate(
        [first[:, low:high].astype(F32).T, second[:, low:high].astype(F32).T], axis=1
    )


def attention_forward_kernel(step, image_ref, text_ref, gain_ref, o_image, o_text, lse_ref, o_scr):
    image_len, text_len = image_ref.shape[0], text_ref.shape[0]
    total = image_len + text_len
    wide = image_ref.shape[1] // 3
    factor = HEAD ** (-0.5)
    raw_q = transposed(image_ref, text_ref, 0, wide)
    raw_k = transposed(image_ref, text_ref, wide, 2 * wide)
    values_t = transposed(image_ref, text_ref, 2 * wide, 3 * wide).astype(BF16)
    for head in range(wide // HEAD):
        rows = slice(head * HEAD, (head + 1) * HEAD)
        q_hat, _, q_gain = head_factors(raw_q[rows], gain_ref[:, 0:1], gain_ref[:, 1:2], image_len)
        k_hat, _, k_gain = head_factors(raw_k[rows], gain_ref[:, 2:3], gain_ref[:, 3:4], image_len)
        q_t = ((q_hat * q_gain).astype(BF16).astype(F32) * factor).astype(BF16)
        keys = (k_hat * k_gain).T.astype(BF16)
        v_t = values_t[rows]
        for start in range(0, total, step):
            part = slice(start, start + step)
            scores = mm(keys, q_t[:, part])
            largest = jnp.max(scores, axis=0, keepdims=True)
            weights = jnp.exp(scores - largest)
            total_w = jnp.sum(weights, axis=0, keepdims=True)
            out = mm(v_t, weights.astype(BF16)) * (1.0 / total_w)
            o_scr[rows, part] = out
            lse_ref[head, :, part] = largest + jnp.log(total_w)
    o_image[...] = o_scr[:, :image_len].T.astype(BF16)
    o_text[...] = o_scr[:, image_len:].T.astype(BF16)


def attention_backward_kernel(
    step,
    image_ref,
    text_ref,
    gain_ref,
    o_image,
    o_text,
    do_image,
    do_text,
    lse_ref,
    d_image,
    d_text,
    gain_grad,
    dq_scr,
    dk_scr,
    dv_scr,
):
    image_len, text_len = image_ref.shape[0], text_ref.shape[0]
    total = image_len + text_len
    wide = image_ref.shape[1] // 3
    factor = HEAD ** (-0.5)
    raw_q = transposed(image_ref, text_ref, 0, wide)
    raw_k = transposed(image_ref, text_ref, wide, 2 * wide)
    o_t = transposed(o_image, o_text, 0, wide)
    do_t = transposed(do_image, do_text, 0, wide)
    lane_row = lax.broadcasted_iota(jnp.int32, (HEAD, 128), 1)
    gains_total = jnp.zeros((HEAD, 128), F32)
    for head in range(wide // HEAD):
        rows = slice(head * HEAD, (head + 1) * HEAD)
        low, high = 2 * wide + head * HEAD, 2 * wide + (head + 1) * HEAD
        q_hat, q_root, q_gain = head_factors(
            raw_q[rows], gain_ref[:, 0:1], gain_ref[:, 1:2], image_len
        )
        k_hat, k_root, k_gain = head_factors(
            raw_k[rows], gain_ref[:, 2:3], gain_ref[:, 3:4], image_len
        )
        q_full = (q_hat * q_gain).astype(BF16).astype(F32) * factor
        q_t = q_full.astype(BF16)
        queries = q_full.T.astype(BF16)
        k_t = (k_hat * k_gain).astype(BF16)
        keys = (k_hat * k_gain).T.astype(BF16)
        values = jnp.concatenate([image_ref[:, low:high], text_ref[:, low:high]], axis=0)
        d_out = jnp.concatenate([do_image[:, rows], do_text[:, rows]], axis=0)
        delta = jnp.sum(do_t[rows] * o_t[rows], axis=0, keepdims=True)
        d_out_t = do_t[rows].astype(BF16)
        d_keys = jnp.zeros((total, HEAD), F32)
        d_values = jnp.zeros((total, HEAD), F32)
        for start in range(0, total, step):
            part = slice(start, start + step)
            weights = jnp.exp(mm(keys, q_t[:, part]) - lse_ref[head, :, part])
            d_weights = mm(values, d_out_t[:, part])
            d_scores = (weights * (d_weights - delta[:, part])).astype(BF16)
            d_values += mm(weights.astype(BF16), d_out[part])
            d_keys += mm(d_scores, queries[part])
            dq_scr[rows, part] = mm(k_t, d_scores) * factor
        dv_scr[:, rows] = d_values
        dq = dq_scr[rows, :]
        dk = d_keys.T
        for slot, (grad, hat) in enumerate(((dq, q_hat), (dk, k_hat))):
            product = grad * hat
            image_sum = jnp.sum(product[:, :image_len], axis=1, keepdims=True)
            text_sum = jnp.sum(product[:, image_len:], axis=1, keepdims=True)
            gains_total += jnp.where(lane_row == 2 * slot, image_sum, 0.0)
            gains_total += jnp.where(lane_row == 2 * slot + 1, text_sum, 0.0)
        scaled = dq * q_gain
        dq_scr[rows, :] = q_root * (
            scaled - q_hat * jnp.mean(scaled * q_hat, axis=0, keepdims=True)
        )
        scaled = dk * k_gain
        dk_scr[rows, :] = k_root * (
            scaled - k_hat * jnp.mean(scaled * k_hat, axis=0, keepdims=True)
        )
    d_image[:, :wide] = dq_scr[:, :image_len].T.astype(BF16)
    d_text[:, :wide] = dq_scr[:, image_len:].T.astype(BF16)
    d_image[:, wide : 2 * wide] = dk_scr[:, :image_len].T.astype(BF16)
    d_text[:, wide : 2 * wide] = dk_scr[:, image_len:].T.astype(BF16)
    d_image[:, 2 * wide :] = dv_scr[:image_len].astype(BF16)
    d_text[:, 2 * wide :] = dv_scr[image_len:].astype(BF16)
    gain_grad[0] = gains_total


def query_step(total):
    for count in (3, 4, 2, 6, 9, 1):
        if total % (count * 128) == 0:
            return total // count
    return total


def kernel_cost(tokens, heads, products):
    return pl.CostEstimate(
        flops=2 * products * heads * tokens * tokens * HEAD * 4,
        transcendentals=heads * tokens * tokens,
        bytes_accessed=tokens * heads * HEAD * 2 * 8,
    )


def attention_forward(raw_image, raw_text, gains):
    groups = raw_image.shape[1] // (3 * 128)
    image_len, text_len = raw_image.shape[0], raw_text.shape[0]
    total = image_len + text_len
    return pl.pallas_call(
        functools.partial(attention_forward_kernel, query_step(total)),
        grid=(groups,),
        out_shape=(
            jax.ShapeDtypeStruct((image_len, groups * 128), BF16),
            jax.ShapeDtypeStruct((text_len, groups * 128), BF16),
            jax.ShapeDtypeStruct((groups * 2, 1, total), F32),
        ),
        in_specs=[
            pl.BlockSpec((image_len, 384), lambda g: (0, g)),
            pl.BlockSpec((text_len, 384), lambda g: (0, g)),
            pl.BlockSpec((HEAD, 4), lambda g: (0, 0)),
        ],
        out_specs=(
            pl.BlockSpec((image_len, 128), lambda g: (0, g)),
            pl.BlockSpec((text_len, 128), lambda g: (0, g)),
            pl.BlockSpec((2, 1, total), lambda g: (g, 0, 0)),
        ),
        scratch_shapes=[pltpu.VMEM((128, total), F32)],
        cost_estimate=kernel_cost(total, groups * 2, 2),
        name="attend_forward",
    )(raw_image, raw_text, gains)


def attention_backward(raw_image, raw_text, gains, o_image, o_text, do_image, do_text, lse):
    groups = raw_image.shape[1] // (3 * 128)
    image_len, text_len = raw_image.shape[0], raw_text.shape[0]
    total = image_len + text_len
    wide_image = pl.BlockSpec((image_len, 384), lambda g: (0, g))
    wide_text = pl.BlockSpec((text_len, 384), lambda g: (0, g))
    slim_image = pl.BlockSpec((image_len, 128), lambda g: (0, g))
    slim_text = pl.BlockSpec((text_len, 128), lambda g: (0, g))
    d_image, d_text, gain_grad = pl.pallas_call(
        functools.partial(attention_backward_kernel, query_step(total)),
        grid=(groups,),
        out_shape=(
            jax.ShapeDtypeStruct(raw_image.shape, BF16),
            jax.ShapeDtypeStruct(raw_text.shape, BF16),
            jax.ShapeDtypeStruct((groups, HEAD, 128), F32),
        ),
        in_specs=[
            wide_image,
            wide_text,
            pl.BlockSpec((HEAD, 4), lambda g: (0, 0)),
            slim_image,
            slim_text,
            slim_image,
            slim_text,
            pl.BlockSpec((2, 1, total), lambda g: (g, 0, 0)),
        ],
        out_specs=(wide_image, wide_text, pl.BlockSpec((1, HEAD, 128), lambda g: (g, 0, 0))),
        scratch_shapes=[
            pltpu.VMEM((128, total), F32),
            pltpu.VMEM((128, total), F32),
            pltpu.VMEM((total, 128), F32),
        ],
        cost_estimate=kernel_cost(total, groups * 2, 5),
        name="attend_backward",
    )(raw_image, raw_text, gains, o_image, o_text, do_image, do_text, lse)
    return d_image, d_text, jnp.sum(gain_grad, axis=0)[:, :4].T


def plain_parts(raw_image, raw_text, gains):
    raw = jnp.concatenate([raw_image, raw_text], axis=0).astype(F32)
    raw = raw.reshape(raw.shape[0], -1, 3, HEAD)
    is_image = (jnp.arange(raw.shape[0]) < raw_image.shape[0])[:, None, None]
    hats, roots, scales, rounded = [], [], [], []
    for slot in range(2):
        part = raw[:, :, slot]
        root = lax.rsqrt(jnp.mean(part * part, axis=-1, keepdims=True) + EPSILON)
        scale = jnp.where(is_image, gains[:, 2 * slot], gains[:, 2 * slot + 1])
        hats.append(part * root)
        roots.append(root)
        scales.append(scale)
        rounded.append((part * root * scale).astype(BF16))
    return hats, roots, scales, rounded, raw[:, :, 2].astype(BF16)


def plain_forward(raw_image, raw_text, gains):
    _, _, _, (queries, keys), values = plain_parts(raw_image, raw_text, gains)
    scores = jnp.einsum("qhd,khd->hqk", queries, keys, preferred_element_type=F32)
    scores = scores * HEAD ** (-0.5)
    largest = jnp.max(scores, axis=-1, keepdims=True)
    lse = largest + jnp.log(jnp.sum(jnp.exp(scores - largest), axis=-1, keepdims=True))
    weights = jnp.exp(scores - lse).astype(BF16)
    out = jnp.einsum("hqk,khd->qhd", weights, values, preferred_element_type=F32)
    out = out.astype(BF16).reshape(out.shape[0], -1)
    return out[: raw_image.shape[0]], out[raw_image.shape[0] :], lse


def plain_backward(raw_image, raw_text, gains, o_image, o_text, do_image, do_text, lse):
    hats, roots, scales, (queries, keys), values = plain_parts(raw_image, raw_text, gains)
    factor = HEAD ** (-0.5)
    image_len = raw_image.shape[0]
    d_out = jnp.concatenate([do_image, do_text], axis=0).reshape(queries.shape)
    scores = jnp.einsum("qhd,khd->hqk", queries, keys, preferred_element_type=F32) * factor
    weights = jnp.exp(scores - lse)
    d_weights = jnp.einsum("qhd,khd->hqk", d_out, values, preferred_element_type=F32)
    inner = jnp.sum(weights * d_weights, axis=-1, keepdims=True)
    d_scores = (weights * (d_weights - inner)).astype(BF16)
    dq = jnp.einsum("hqk,khd->qhd", d_scores, keys, preferred_element_type=F32) * factor
    dk = jnp.einsum("hqk,qhd->khd", d_scores, queries, preferred_element_type=F32) * factor
    dv = jnp.einsum("hqk,qhd->khd", weights.astype(BF16), d_out, preferred_element_type=F32)
    gain_rows, parts = [], []
    for grad, hat, root, scale in zip((dq, dk), hats, roots, scales):
        product = grad * hat
        gain_rows += [jnp.sum(product[:image_len], (0, 1)), jnp.sum(product[image_len:], (0, 1))]
        scaled = grad * scale
        parts.append(root * (scaled - hat * jnp.mean(scaled * hat, axis=-1, keepdims=True)))
    joined = jnp.stack(parts + [dv], axis=2).astype(BF16).reshape(d_out.shape[0], -1)
    return joined[:image_len], joined[image_len:], jnp.stack(gain_rows)


def tie(*groups):
    return lax.optimization_barrier(groups)


class Side:
    def __init__(self, state=(), steps=(), finish=None):
        self.state, self.steps, self.finish = state, list(steps), finish
        self.running = False

    def open(self, token):
        if self.steps:
            token, self.state = tie(token, self.state)
            self.state = self.steps.pop(0)(self.state)
            self.running = True
        return token

    def close(self, token):
        if self.running:
            token, self.state = tie(token, self.state)
            self.running = False
        return token

    def result(self):
        while self.steps:
            self.state = self.steps.pop(0)(self.state)
        return self.finish(self.state)


def join_kernel(size, cut, me_ref, own, *refs):
    after, before = refs[: size - 1], refs[size - 1 : 2 * size - 2]
    image, text, sems = refs[2 * size - 2 :]
    tail = own.shape[0] - cut

    def copies(source, k):
        return (
            pltpu.make_async_copy(
                source.at[pl.ds(0, cut)], image.at[pl.ds(k * cut, cut)], sems.at[k, 0]
            ),
            pltpu.make_async_copy(
                source.at[pl.ds(cut, tail)], text.at[pl.ds(k * tail, tail)], sems.at[k, 1]
            ),
        )

    def start(source, k):
        for copy in copies(source, k):
            copy.start()

    start(own, 0)
    for k in range(1, size):
        from_after = me_ref[0] + k < size
        pl.when(from_after)(functools.partial(start, after[k - 1], k))
        pl.when(jnp.logical_not(from_after))(functools.partial(start, before[size - k - 1], k))
    for k in range(size):
        for copy in copies(own, k):
            copy.wait()


def join_tokens(own, after, before, me, cut):
    size, (rows, width) = len(after) + 1, own.shape
    return pl.pallas_call(
        functools.partial(join_kernel, size, cut),
        out_shape=(
            jax.ShapeDtypeStruct((size * cut, width), own.dtype),
            jax.ShapeDtypeStruct((size * (rows - cut), width), own.dtype),
        ),
        in_specs=[pl.BlockSpec(memory_space=pltpu.SMEM)]
        + [pl.BlockSpec(memory_space=pl.ANY)] * (2 * size - 1),
        out_specs=(
            pl.BlockSpec(memory_space=pltpu.VMEM),
            pl.BlockSpec(memory_space=pltpu.VMEM),
        ),
        scratch_shapes=[pltpu.SemaphoreType.DMA((size, 2))],
        compiler_params=pltpu.CompilerParams(vmem_limit_bytes=16 * 2**20),
        cost_estimate=pl.CostEstimate(
            flops=0, transcendentals=0, bytes_accessed=4 * size * own.size
        ),
        name="join_tokens",
    )(me.astype(jnp.int32)[None], own, *after, *before)


class Streams:
    def __init__(self, image_len, text_len, axis, size):
        self.lengths = (image_len, text_len)
        self.axis, self.size = axis, size

    def gather_side(self, pair):
        size = self.size

        def step(state):
            own, after, before = state
            down, up = (after[-1], before[-1]) if after else (own, own)
            down = lax.ppermute(down, self.axis, [(i, i - 1) for i in range(1, size)])
            up = lax.ppermute(up, self.axis, [(i, i + 1) for i in range(size - 1)])
            return own, after + (down,), before + (up,)

        def finish(state):
            return join_tokens(*state, lax.axis_index(self.axis), self.lengths[0])

        return Side((jnp.concatenate(pair, axis=0), (), ()), [step] * (size - 1), finish)

    def scatter_side(self, pair):
        size, cut = self.size, self.lengths[0]
        low = [part.astype(BF16) for part in pair]
        blocks = tuple(
            jnp.concatenate(
                [low[s][k * n : (k + 1) * n] for s, n in enumerate(self.lengths)], axis=0
            )
            for k in range(size)
        )

        def step(index, state):
            blocks, sums = state
            k = size - 1 - index
            send_up, send_down = blocks[k], blocks[size - k]
            if sums:
                send_up, send_down = (
                    (send.astype(F32) + value.astype(F32)).astype(BF16)
                    for send, value in zip((send_up, send_down), sums)
                )
            up = lax.ppermute(send_up, self.axis, [(i, i + 1) for i in range(index + 1)])
            down = lax.ppermute(send_down, self.axis, [(i, i - 1) for i in range(k, size)])
            return blocks, (up, down)

        def finish(state):
            blocks, (up, down) = state
            total = blocks[0].astype(F32) + up.astype(F32) + down.astype(F32)
            return total[:cut], total[cut:]

        steps = [functools.partial(step, index) for index in range(size - 1)]
        return Side((blocks, ()), steps, finish)

    def gather(self, pair):
        return self.gather_side(pair).result()

    def scatter(self, pair):
        return self.scatter_side(pair).result()


def bit_order(size):
    bits = [b for b in range(size.bit_length() - 1)]
    masks = [0]
    for b in bits:
        masks += [m | (1 << b) for m in masks]
    return bits, masks


def swap_bit(value, axis, size, bit):
    return lax.ppermute(value, axis, [(i, i ^ (1 << bit)) for i in range(size)])


def bit_gather(own, axis, size):
    blocks = own[None]
    for b in bit_order(size)[0]:
        blocks = jnp.concatenate([blocks, swap_bit(blocks, axis, size, b)], axis=0)
    return blocks


def bit_scatter(parts, axis, size):
    me = lax.axis_index(axis)
    for b in reversed(bit_order(size)[0]):
        half = parts.shape[0] // 2
        upper = ((me >> b) & 1) == 1
        keep = jnp.where(upper, parts[half:], parts[:half])
        send = jnp.where(upper, parts[:half], parts[half:])
        parts = keep + swap_bit(send, axis, size, b)
    return parts[0]


def bit_sum(value, axis, size):
    for b in bit_order(size)[0]:
        value = value + swap_bit(value, axis, size, b)
    return value


def forward_layer(streams, x, mods, weights, gains, attend, plain, side, last):
    qkv, out_t, up, down_t = weights
    if plain is not None:
        normed = [
            (plain[s].astype(F32) * (1.0 + mods[s, 1]) + mods[s, 0]).astype(BF16)
            for s in range(2)
        ]
    else:
        normed = streams.gather(
            [modulate(x[s], mods[s, 0], mods[s, 1]).astype(BF16) for s in range(2)]
        )
    raw = side.open([mm(normed[s], qkv[s]).astype(BF16) for s in range(2)])
    o_image, o_text, lse = attend(raw[0], raw[1], gains)
    mixed = side.close((o_image, o_text))
    branch = streams.scatter([mm_nt(mixed[s], out_t[s]) for s in range(2)])
    middle = [x[s] + mods[s, 2] * branch[s] for s in range(2)]
    second = streams.gather(
        [modulate(middle[s], mods[s, 3], mods[s, 4]).astype(BF16) for s in range(2)]
    )
    second = side.open(second)
    hidden = [mm(second[s], up[s]) for s in range(2)]
    active = side.close([gelu(hidden[s]).astype(BF16) for s in range(2)])
    hidden = [hidden[s].astype(BF16) for s in range(2)]
    result = streams.scatter_side([mm_nt(active[s], down_t[s]) for s in range(2)])
    saved = (x, normed, raw, mixed, lse, branch, middle, second, hidden, active)
    if last:
        return None, saved, result
    result = result.result()
    return [middle[s] + mods[s, 5] * result[s] for s in range(2)], saved, result


def backward_layer(streams, gy, dm, saved, mods, weights, gains, calls, side, last):
    qkv, out_t, up, down_t = weights
    x, normed, raw, mixed, lse, branch, middle, second, hidden, active = saved
    if dm is None:
        dm = streams.gather([(mods[s, 5] * gy[s]).astype(BF16) for s in range(2)])
    dm = side.open(dm)
    du = []
    for s in range(2):
        _, pull = jax.vjp(gelu, hidden[s].astype(F32))
        du.append(pull(mm(dm[s], down_t[s]))[0].astype(BF16))
    d_second = side.close([mm_nt(du[s], up[s]).astype(BF16) for s in range(2)])
    d_second = streams.scatter(d_second)
    late = [mm_tn(second[s], du[s]) for s in range(2)]
    late += [mm_tn(dm[s], active[s]) for s in range(2)]
    late = jnp.stack([part.astype(BF16) for part in late])
    reduced_mlp = calls.reduce_grad(late, True)
    d_middle, d_shift2, d_scale2 = [], [], []
    for s in range(2):
        inner, d_shift, d_scale = modulate_back(middle[s], d_second[s], mods[s, 4])
        d_middle.append(gy[s] + inner)
        d_shift2.append(d_shift)
        d_scale2.append(d_scale)
    d_gate1 = [jnp.sum(d_middle[s] * branch[s], axis=0) for s in range(2)]
    da = streams.gather([(mods[s, 2] * d_middle[s]).astype(BF16) for s in range(2)])
    d_mixed = side.open([mm(da[s], out_t[s]).astype(BF16) for s in range(2)])
    late = jnp.stack([mm_tn(da[s], mixed[s]).astype(BF16) for s in range(2)])
    reduced_out = calls.reduce_grad(late, True)
    d_image, d_text, gain_rows = calls.attend_back(
        raw[0], raw[1], gains, mixed[0], mixed[1], d_mixed[0], d_mixed[1], lse
    )
    d_raw = side.close((d_image, d_text))
    late = jnp.stack([mm_tn(normed[s], d_raw[s]).astype(BF16) for s in range(2)])
    if last:
        d_raw, late = tie(d_raw, late)
    d_first = streams.scatter([mm_nt(d_raw[s], qkv[s]) for s in range(2)])
    reduced_qkv = calls.reduce_grad(late, not last)
    d_gains = gain_rows.reshape(2, 2, HEAD).transpose(1, 0, 2)
    early = (d_gate1, d_shift2, d_scale2), d_gains
    if last:
        d_first = calls.before_end(early, d_first)
        d_first, reduced_out[0] = tie(d_first, reduced_out[0])
    gx, late = [], []
    for s in range(2):
        inner, d_shift, d_scale = modulate_back(x[s], d_first[s], mods[s, 1])
        gx.append(d_middle[s] + inner)
        late += [d_shift, d_scale]
    return gx, early, late, (reduced_qkv, reduced_out, reduced_mlp)


class Calls:
    def __init__(self, attend_back, dp_axis):
        self.attend_back, self.axis, self.previous = attend_back, dp_axis, None
        self.before_end = None

    def reduce_grad(self, grad, in_order):
        if in_order and self.previous is not None:
            grad, self.previous[0] = tie(grad, self.previous[0])
        box = [lax.psum_scatter(grad, self.axis, scatter_dimension=1, tiled=True)]
        if in_order:
            self.previous = box
        return box


def on_device(dp, seq, width_of_group, *args):
    (
        image_in,
        text_input,
        condition,
        ada_weight,
        qkv_weight,
        out_weight,
        up_weight,
        down_weight,
        norm_gain,
        image_cotangent,
        text_cotangent,
    ) = args
    dp_axis, dp_size = dp
    seq_axis, seq_size = seq
    layers = qkv_weight.shape[0]
    width = image_in.shape[2]
    streams = Streams(image_in.shape[1], text_input.shape[1], seq_axis, seq_size)
    attend, attend_back = (
        (attention_forward, attention_backward)
        if width_of_group % 128 == 0
        else (plain_forward, plain_backward)
    )
    rows = qkv_weight.shape[2]

    def fetch(local):
        return lax.all_gather(local, dp_axis, axis=1, tiled=True)

    qkv_local = qkv_weight.reshape(layers, 2, rows, 3, -1, width_of_group)
    qkv_local = qkv_local.transpose(0, 1, 2, 4, 3, 5).reshape(layers, 2, rows, -1)
    out_local = out_weight.transpose(0, 1, 3, 2)
    down_local = down_weight.transpose(0, 1, 3, 2)
    weights = [
        tuple(fetch(w[l]) for w in (qkv_local, out_local, up_weight, down_local))
        for l in range(layers)
    ]

    act_cond, silu_pull = jax.vjp(jax.nn.silu, condition.astype(F32))
    act_low = act_cond.astype(BF16)
    partial_mods = jnp.einsum("nd,lsde->nlse", act_low, ada_weight, preferred_element_type=F32)
    own_mods = bit_scatter(partial_mods.reshape(dp_size, -1), dp_axis, dp_size)
    x = [image_in[0].astype(F32), text_input[0].astype(F32)]
    plain = streams.gather([layer_stats(part)[0].astype(BF16) for part in x])
    own_mods, plain = tie(own_mods, plain)
    own_mods = bit_sum(own_mods, seq_axis, seq_size).reshape(layers, 2, 6, width)
    gains_all = norm_gain.astype(F32)
    gain_columns = [gains_all[l].transpose(1, 0, 2).reshape(4, HEAD).T for l in range(layers)]

    gy = [image_cotangent[0].astype(F32), text_cotangent[0].astype(F32)]
    side = streams.gather_side(
        [(own_mods[layers - 1, s, 5] * gy[s]).astype(BF16) for s in range(2)]
    )
    saved_list, results = [], []
    for l in range(layers):
        x, saved, result = forward_layer(
            streams,
            x,
            own_mods[l],
            weights[l],
            gain_columns[l],
            attend,
            None if l else plain,
            side,
            l == layers - 1,
        )
        saved_list.append(saved)
        results.append(result)
    dm, side = side.result(), results[-1]

    def share(values):
        return bit_gather(bit_sum(values, seq_axis, seq_size), dp_axis, dp_size)

    gys, early_all, late_all = [None] * layers, [None] * layers, [None] * layers
    grads, ends = [None] * layers, {}

    def before_end(early, token):
        early_all[0] = early
        results[-1] = side.result()
        parts = []
        for l in range(layers):
            d_gate2 = [jnp.sum(gys[l][s] * results[l][s], axis=0) for s in range(2)]
            d_gate1, d_shift2, d_scale2 = early_all[l][0]
            for s in range(2):
                parts += late_all[l][2 * s : 2 * s + 2] if l else []
                parts += [d_gate1[s], d_shift2[s], d_scale2[s], d_gate2[s]]
        gain_parts = [early_all[l][1].reshape(-1) for l in range(layers)]
        shared = share(jnp.concatenate(parts + gain_parts))
        ends["early"], token = tie(shared, token)
        return token

    calls = Calls(attend_back, dp_axis)
    calls.before_end = before_end
    for l in reversed(range(layers)):
        gys[l] = gy
        gy, early_all[l], late_all[l], grads[l] = backward_layer(
            streams,
            gy,
            dm,
            saved_list[l],
            own_mods[l],
            weights[l],
            gain_columns[l],
            calls,
            side,
            l == 0,
        )
        dm = None
    last_middle = saved_list[-1][6]
    outputs = [
        (last_middle[s] + own_mods[layers - 1, s, 5] * results[-1][s]).astype(BF16)[None]
        for s in range(2)
    ]

    there = jnp.array(bit_order(dp_size)[1], jnp.int32) ^ lax.axis_index(dp_axis)
    rest = share(jnp.concatenate(late_all[0])).reshape(dp_size, 2, 2 * width)
    early, total_mods, place = ends["early"], [], 0
    for l in range(layers):
        size = (6 if l else 4) * width
        part = early[:, place : place + 2 * size].reshape(dp_size, 2, size)
        place += 2 * size
        total_mods.append(part if l else jnp.concatenate([rest, part], axis=2))
    total_mods = jnp.stack(total_mods, axis=1)
    total_gains = jnp.sum(early[:, place:][there], axis=0).reshape(layers, 2, 2, HEAD)
    act_there = act_low.astype(F32)[there]
    ada_grad = jnp.einsum("nd,nlse->lsde", act_there, total_mods, precision=HIGHEST)
    d_act = jnp.einsum("nlse,lsde->nd", total_mods, ada_weight.astype(F32), precision=HIGHEST)
    condition_grad = silu_pull(d_act[there])[0]

    def pieces(kind, first):
        return jnp.stack([grads[l][kind][0][first : first + 2] for l in range(layers)]).astype(F32)

    qkv_grad = pieces(0, 0).reshape(layers, 2, rows, -1, 3, width_of_group)
    qkv_grad = qkv_grad.transpose(0, 1, 2, 4, 3, 5).reshape(qkv_weight.shape)
    return (
        outputs[0],
        outputs[1],
        gy[0][None],
        gy[1][None],
        condition_grad,
        ada_grad,
        qkv_grad,
        pieces(1, 0).transpose(0, 1, 3, 2),
        pieces(2, 0),
        pieces(2, 2).transpose(0, 1, 3, 2),
        total_gains,
    )


def solution(mesh):
    tokens = P("dp", "seq", None)
    placed = (
        tokens,
        tokens,
        P(None, ("dp", "seq")),
        P(None, None, ("dp", "seq"), None),
        P(None, None, "dp", None, "seq"),
        P(None, None, "seq", "dp"),
        P(None, None, "dp", "seq"),
        P(None, None, "seq", "dp"),
        P(),
        tokens,
        tokens,
    )
    results = (tokens, tokens, tokens, tokens) + placed[2:8] + (P(),)

    def step(*args):
        heads = args[4].shape[4] // mesh.shape["seq"] // HEAD
        group = 2 * HEAD if heads % 2 == 0 else HEAD
        body = functools.partial(
            on_device, ("dp", mesh.shape["dp"]), ("seq", mesh.shape["seq"]), group
        )
        return jax.shard_map(
            body, mesh=mesh, in_specs=placed, out_specs=results, check_vma=False
        )(*args)

    return step
```

```python
import functools

import jax
import jax.numpy as jnp
from jax import lax
from jax.experimental import pallas as pl
from jax.experimental.pallas import tpu as pltpu
from jax.sharding import PartitionSpec as P

EPSILON = 1e-06
HIGHEST = lax.Precision.HIGHEST
F32 = jnp.float32
BF16 = jnp.bfloat16
HEAD = 64


def layer_stats(values):
    centred = values - jnp.mean(values, axis=-1, keepdims=True)
    root = lax.rsqrt(jnp.mean(centred * centred, axis=-1, keepdims=True) + EPSILON)
    return centred * root, root


def modulate(values, shift, scale):
    return layer_stats(values)[0] * (1.0 + scale) + shift


def modulate_back(values, grad, scale):
    normed, root = layer_stats(values)
    inner = grad * (1.0 + scale)
    first = jnp.mean(inner, axis=-1, keepdims=True)
    second = jnp.mean(inner * normed, axis=-1, keepdims=True)
    d_values = root * (inner - first - normed * second)
    return d_values, jnp.sum(grad, axis=0), jnp.sum(grad * normed, axis=0)


def mm(left, right):
    return lax.dot_general(left, right, (((1,), (0,)), ((), ())), preferred_element_type=F32)


def mm_nt(left, right):
    return lax.dot_general(left, right, (((1,), (1,)), ((), ())), preferred_element_type=F32)


def mm_tn(left, right):
    return lax.dot_general(left, right, (((0,), (0,)), ((), ())), preferred_element_type=F32)


def gelu(values):
    return jax.nn.gelu(values, approximate=True)


def head_factors(raw_t, gain_image, gain_text, image_len):
    root = lax.rsqrt(jnp.mean(raw_t * raw_t, axis=0, keepdims=True) + EPSILON)
    lanes = lax.broadcasted_iota(jnp.int32, raw_t.shape, 1)
    gain = jnp.where(lanes < image_len, gain_image, gain_text)
    return raw_t * root, root, gain


def transposed(first, second, low, high):
    return jnp.concatenate(
        [first[:, low:high].astype(F32).T, second[:, low:high].astype(F32).T], axis=1
    )


def attention_forward_kernel(step, image_ref, text_ref, gain_ref, o_image, o_text, lse_ref, o_scr):
    image_len, text_len = image_ref.shape[0], text_ref.shape[0]
    total = image_len + text_len
    wide = image_ref.shape[1] // 3
    factor = HEAD ** (-0.5)
    raw_q = transposed(image_ref, text_ref, 0, wide)
    raw_k = transposed(image_ref, text_ref, wide, 2 * wide)
    values_t = transposed(image_ref, text_ref, 2 * wide, 3 * wide).astype(BF16)
    for head in range(wide // HEAD):
        rows = slice(head * HEAD, (head + 1) * HEAD)
        q_hat, _, q_gain = head_factors(raw_q[rows], gain_ref[:, 0:1], gain_ref[:, 1:2], image_len)
        k_hat, _, k_gain = head_factors(raw_k[rows], gain_ref[:, 2:3], gain_ref[:, 3:4], image_len)
        q_t = ((q_hat * q_gain).astype(BF16).astype(F32) * factor).astype(BF16)
        keys = (k_hat * k_gain).T.astype(BF16)
        v_t = values_t[rows]
        for start in range(0, total, step):
            part = slice(start, start + step)
            scores = mm(keys, q_t[:, part])
            largest = jnp.max(scores, axis=0, keepdims=True)
            weights = jnp.exp(scores - largest)
            total_w = jnp.sum(weights, axis=0, keepdims=True)
            out = mm(v_t, weights.astype(BF16)) * (1.0 / total_w)
            o_scr[rows, part] = out
            lse_ref[head, :, part] = largest + jnp.log(total_w)
    o_image[...] = o_scr[:, :image_len].T.astype(BF16)
    o_text[...] = o_scr[:, image_len:].T.astype(BF16)


def attention_backward_kernel(
    step,
    image_ref,
    text_ref,
    gain_ref,
    o_image,
    o_text,
    do_image,
    do_text,
    lse_ref,
    d_image,
    d_text,
    gain_grad,
    dq_scr,
    dk_scr,
    dv_scr,
):
    image_len, text_len = image_ref.shape[0], text_ref.shape[0]
    total = image_len + text_len
    wide = image_ref.shape[1] // 3
    factor = HEAD ** (-0.5)
    raw_q = transposed(image_ref, text_ref, 0, wide)
    raw_k = transposed(image_ref, text_ref, wide, 2 * wide)
    o_t = transposed(o_image, o_text, 0, wide)
    do_t = transposed(do_image, do_text, 0, wide)
    lane_row = lax.broadcasted_iota(jnp.int32, (HEAD, 128), 1)
    gains_total = jnp.zeros((HEAD, 128), F32)
    for head in range(wide // HEAD):
        rows = slice(head * HEAD, (head + 1) * HEAD)
        low, high = 2 * wide + head * HEAD, 2 * wide + (head + 1) * HEAD
        q_hat, q_root, q_gain = head_factors(
            raw_q[rows], gain_ref[:, 0:1], gain_ref[:, 1:2], image_len
        )
        k_hat, k_root, k_gain = head_factors(
            raw_k[rows], gain_ref[:, 2:3], gain_ref[:, 3:4], image_len
        )
        q_full = (q_hat * q_gain).astype(BF16).astype(F32) * factor
        q_t = q_full.astype(BF16)
        queries = q_full.T.astype(BF16)
        k_t = (k_hat * k_gain).astype(BF16)
        keys = (k_hat * k_gain).T.astype(BF16)
        values = jnp.concatenate([image_ref[:, low:high], text_ref[:, low:high]], axis=0)
        d_out = jnp.concatenate([do_image[:, rows], do_text[:, rows]], axis=0)
        delta = jnp.sum(do_t[rows] * o_t[rows], axis=0, keepdims=True)
        d_out_t = do_t[rows].astype(BF16)
        d_keys = jnp.zeros((total, HEAD), F32)
        d_values = jnp.zeros((total, HEAD), F32)
        for start in range(0, total, step):
            part = slice(start, start + step)
            weights = jnp.exp(mm(keys, q_t[:, part]) - lse_ref[head, :, part])
            d_weights = mm(values, d_out_t[:, part])
            d_scores = (weights * (d_weights - delta[:, part])).astype(BF16)
            d_values += mm(weights.astype(BF16), d_out[part])
            d_keys += mm(d_scores, queries[part])
            dq_scr[rows, part] = mm(k_t, d_scores) * factor
        dv_scr[:, rows] = d_values
        dq = dq_scr[rows, :]
        dk = d_keys.T
        for slot, (grad, hat) in enumerate(((dq, q_hat), (dk, k_hat))):
            product = grad * hat
            image_sum = jnp.sum(product[:, :image_len], axis=1, keepdims=True)
            text_sum = jnp.sum(product[:, image_len:], axis=1, keepdims=True)
            gains_total += jnp.where(lane_row == 2 * slot, image_sum, 0.0)
            gains_total += jnp.where(lane_row == 2 * slot + 1, text_sum, 0.0)
        scaled = dq * q_gain
        dq_scr[rows, :] = q_root * (
            scaled - q_hat * jnp.mean(scaled * q_hat, axis=0, keepdims=True)
        )
        scaled = dk * k_gain
        dk_scr[rows, :] = k_root * (
            scaled - k_hat * jnp.mean(scaled * k_hat, axis=0, keepdims=True)
        )
    d_image[:, :wide] = dq_scr[:, :image_len].T.astype(BF16)
    d_text[:, :wide] = dq_scr[:, image_len:].T.astype(BF16)
    d_image[:, wide : 2 * wide] = dk_scr[:, :image_len].T.astype(BF16)
    d_text[:, wide : 2 * wide] = dk_scr[:, image_len:].T.astype(BF16)
    d_image[:, 2 * wide :] = dv_scr[:image_len].astype(BF16)
    d_text[:, 2 * wide :] = dv_scr[image_len:].astype(BF16)
    gain_grad[0] = gains_total


def query_step(total):
    for count in (3, 4, 2, 6, 9, 1):
        if total % (count * 128) == 0:
            return total // count
    return total


def kernel_cost(tokens, heads, products):
    return pl.CostEstimate(
        flops=2 * products * heads * tokens * tokens * HEAD * 4,
        transcendentals=heads * tokens * tokens,
        bytes_accessed=tokens * heads * HEAD * 2 * 8,
    )


def attention_forward(raw_image, raw_text, gains):
    groups = raw_image.shape[1] // (3 * 128)
    image_len, text_len = raw_image.shape[0], raw_text.shape[0]
    total = image_len + text_len
    return pl.pallas_call(
        functools.partial(attention_forward_kernel, query_step(total)),
        grid=(groups,),
        out_shape=(
            jax.ShapeDtypeStruct((image_len, groups * 128), BF16),
            jax.ShapeDtypeStruct((text_len, groups * 128), BF16),
            jax.ShapeDtypeStruct((groups * 2, 1, total), F32),
        ),
        in_specs=[
            pl.BlockSpec((image_len, 384), lambda g: (0, g)),
            pl.BlockSpec((text_len, 384), lambda g: (0, g)),
            pl.BlockSpec((HEAD, 4), lambda g: (0, 0)),
        ],
        out_specs=(
            pl.BlockSpec((image_len, 128), lambda g: (0, g)),
            pl.BlockSpec((text_len, 128), lambda g: (0, g)),
            pl.BlockSpec((2, 1, total), lambda g: (g, 0, 0)),
        ),
        scratch_shapes=[pltpu.VMEM((128, total), F32)],
        cost_estimate=kernel_cost(total, groups * 2, 2),
        name="attend_forward",
    )(raw_image, raw_text, gains)


def attention_backward(raw_image, raw_text, gains, o_image, o_text, do_image, do_text, lse):
    groups = raw_image.shape[1] // (3 * 128)
    image_len, text_len = raw_image.shape[0], raw_text.shape[0]
    total = image_len + text_len
    wide_image = pl.BlockSpec((image_len, 384), lambda g: (0, g))
    wide_text = pl.BlockSpec((text_len, 384), lambda g: (0, g))
    slim_image = pl.BlockSpec((image_len, 128), lambda g: (0, g))
    slim_text = pl.BlockSpec((text_len, 128), lambda g: (0, g))
    d_image, d_text, gain_grad = pl.pallas_call(
        functools.partial(attention_backward_kernel, query_step(total)),
        grid=(groups,),
        out_shape=(
            jax.ShapeDtypeStruct(raw_image.shape, BF16),
            jax.ShapeDtypeStruct(raw_text.shape, BF16),
            jax.ShapeDtypeStruct((groups, HEAD, 128), F32),
        ),
        in_specs=[
            wide_image,
            wide_text,
            pl.BlockSpec((HEAD, 4), lambda g: (0, 0)),
            slim_image,
            slim_text,
            slim_image,
            slim_text,
            pl.BlockSpec((2, 1, total), lambda g: (g, 0, 0)),
        ],
        out_specs=(wide_image, wide_text, pl.BlockSpec((1, HEAD, 128), lambda g: (g, 0, 0))),
        scratch_shapes=[
            pltpu.VMEM((128, total), F32),
            pltpu.VMEM((128, total), F32),
            pltpu.VMEM((total, 128), F32),
        ],
        cost_estimate=kernel_cost(total, groups * 2, 5),
        name="attend_backward",
    )(raw_image, raw_text, gains, o_image, o_text, do_image, do_text, lse)
    return d_image, d_text, jnp.sum(gain_grad, axis=0)[:, :4].T


def plain_parts(raw_image, raw_text, gains):
    raw = jnp.concatenate([raw_image, raw_text], axis=0).astype(F32)
    raw = raw.reshape(raw.shape[0], -1, 3, HEAD)
    is_image = (jnp.arange(raw.shape[0]) < raw_image.shape[0])[:, None, None]
    hats, roots, scales, rounded = [], [], [], []
    for slot in range(2):
        part = raw[:, :, slot]
        root = lax.rsqrt(jnp.mean(part * part, axis=-1, keepdims=True) + EPSILON)
        scale = jnp.where(is_image, gains[:, 2 * slot], gains[:, 2 * slot + 1])
        hats.append(part * root)
        roots.append(root)
        scales.append(scale)
        rounded.append((part * root * scale).astype(BF16))
    return hats, roots, scales, rounded, raw[:, :, 2].astype(BF16)


def plain_forward(raw_image, raw_text, gains):
    _, _, _, (queries, keys), values = plain_parts(raw_image, raw_text, gains)
    scores = jnp.einsum("qhd,khd->hqk", queries, keys, preferred_element_type=F32)
    scores = scores * HEAD ** (-0.5)
    largest = jnp.max(scores, axis=-1, keepdims=True)
    lse = largest + jnp.log(jnp.sum(jnp.exp(scores - largest), axis=-1, keepdims=True))
    weights = jnp.exp(scores - lse).astype(BF16)
    out = jnp.einsum("hqk,khd->qhd", weights, values, preferred_element_type=F32)
    out = out.astype(BF16).reshape(out.shape[0], -1)
    return out[: raw_image.shape[0]], out[raw_image.shape[0] :], lse


def plain_backward(raw_image, raw_text, gains, o_image, o_text, do_image, do_text, lse):
    hats, roots, scales, (queries, keys), values = plain_parts(raw_image, raw_text, gains)
    factor = HEAD ** (-0.5)
    image_len = raw_image.shape[0]
    d_out = jnp.concatenate([do_image, do_text], axis=0).reshape(queries.shape)
    scores = jnp.einsum("qhd,khd->hqk", queries, keys, preferred_element_type=F32) * factor
    weights = jnp.exp(scores - lse)
    d_weights = jnp.einsum("qhd,khd->hqk", d_out, values, preferred_element_type=F32)
    inner = jnp.sum(weights * d_weights, axis=-1, keepdims=True)
    d_scores = (weights * (d_weights - inner)).astype(BF16)
    dq = jnp.einsum("hqk,khd->qhd", d_scores, keys, preferred_element_type=F32) * factor
    dk = jnp.einsum("hqk,qhd->khd", d_scores, queries, preferred_element_type=F32) * factor
    dv = jnp.einsum("hqk,qhd->khd", weights.astype(BF16), d_out, preferred_element_type=F32)
    gain_rows, parts = [], []
    for grad, hat, root, scale in zip((dq, dk), hats, roots, scales):
        product = grad * hat
        gain_rows += [jnp.sum(product[:image_len], (0, 1)), jnp.sum(product[image_len:], (0, 1))]
        scaled = grad * scale
        parts.append(root * (scaled - hat * jnp.mean(scaled * hat, axis=-1, keepdims=True)))
    joined = jnp.stack(parts + [dv], axis=2).astype(BF16).reshape(d_out.shape[0], -1)
    return joined[:image_len], joined[image_len:], jnp.stack(gain_rows)


def tie(*groups):
    return lax.optimization_barrier(groups)


class Side:
    def __init__(self, state=(), steps=(), finish=None):
        self.state, self.steps, self.finish = state, list(steps), finish
        self.running = False

    def open(self, token):
        if self.steps:
            token, self.state = tie(token, self.state)
            self.state = self.steps.pop(0)(self.state)
            self.running = True
        return token

    def close(self, token):
        if self.running:
            token, self.state = tie(token, self.state)
            self.running = False
        return token

    def result(self):
        while self.steps:
            self.state = self.steps.pop(0)(self.state)
        return self.finish(self.state)


def join_kernel(size, cut, me_ref, own, *refs):
    after, before = refs[: size - 1], refs[size - 1 : 2 * size - 2]
    image, text, sems = refs[2 * size - 2 :]
    tail = own.shape[0] - cut

    def copies(source, k):
        return (
            pltpu.make_async_copy(
                source.at[pl.ds(0, cut)], image.at[pl.ds(k * cut, cut)], sems.at[k, 0]
            ),
            pltpu.make_async_copy(
                source.at[pl.ds(cut, tail)], text.at[pl.ds(k * tail, tail)], sems.at[k, 1]
            ),
        )

    def start(source, k):
        for copy in copies(source, k):
            copy.start()

    start(own, 0)
    for k in range(1, size):
        from_after = me_ref[0] + k < size
        pl.when(from_after)(functools.partial(start, after[k - 1], k))
        pl.when(jnp.logical_not(from_after))(functools.partial(start, before[size - k - 1], k))
    for k in range(size):
        for copy in copies(own, k):
            copy.wait()


def join_tokens(own, after, before, me, cut):
    size, (rows, width) = len(after) + 1, own.shape
    return pl.pallas_call(
        functools.partial(join_kernel, size, cut),
        out_shape=(
            jax.ShapeDtypeStruct((size * cut, width), own.dtype),
            jax.ShapeDtypeStruct((size * (rows - cut), width), own.dtype),
        ),
        in_specs=[pl.BlockSpec(memory_space=pltpu.SMEM)]
        + [pl.BlockSpec(memory_space=pl.ANY)] * (2 * size - 1),
        out_specs=(
            pl.BlockSpec(memory_space=pltpu.VMEM),
            pl.BlockSpec(memory_space=pltpu.VMEM),
        ),
        scratch_shapes=[pltpu.SemaphoreType.DMA((size, 2))],
        compiler_params=pltpu.CompilerParams(vmem_limit_bytes=16 * 2**20),
        cost_estimate=pl.CostEstimate(
            flops=0, transcendentals=0, bytes_accessed=4 * size * own.size
        ),
        name="join_tokens",
    )(me.astype(jnp.int32)[None], own, *after, *before)


class Streams:
    def __init__(self, image_len, text_len, axis, size):
        self.lengths = (image_len, text_len)
        self.axis, self.size = axis, size

    def gather_side(self, pair):
        size = self.size

        def step(state):
            own, after, before = state
            down, up = (after[-1], before[-1]) if after else (own, own)
            down = lax.ppermute(down, self.axis, [(i, i - 1) for i in range(1, size)])
            up = lax.ppermute(up, self.axis, [(i, i + 1) for i in range(size - 1)])
            return own, after + (down,), before + (up,)

        def finish(state):
            return join_tokens(*state, lax.axis_index(self.axis), self.lengths[0])

        return Side((jnp.concatenate(pair, axis=0), (), ()), [step] * (size - 1), finish)

    def scatter_side(self, pair):
        size, cut = self.size, self.lengths[0]
        low = [part.astype(BF16) for part in pair]
        blocks = tuple(
            jnp.concatenate(
                [low[s][k * n : (k + 1) * n] for s, n in enumerate(self.lengths)], axis=0
            )
            for k in range(size)
        )

        def step(index, state):
            blocks, sums = state
            k = size - 1 - index
            send_up, send_down = blocks[k], blocks[size - k]
            if sums:
                send_up, send_down = (
                    (send.astype(F32) + value.astype(F32)).astype(BF16)
                    for send, value in zip((send_up, send_down), sums)
                )
            up = lax.ppermute(send_up, self.axis, [(i, i + 1) for i in range(index + 1)])
            down = lax.ppermute(send_down, self.axis, [(i, i - 1) for i in range(k, size)])
            return blocks, (up, down)

        def finish(state):
            blocks, (up, down) = state
            total = blocks[0].astype(F32) + up.astype(F32) + down.astype(F32)
            return total[:cut], total[cut:]

        steps = [functools.partial(step, index) for index in range(size - 1)]
        return Side((blocks, ()), steps, finish)

    def gather(self, pair):
        return self.gather_side(pair).result()

    def scatter(self, pair):
        return self.scatter_side(pair).result()


def bit_order(size):
    bits = [b for b in range(size.bit_length() - 1)]
    masks = [0]
    for b in bits:
        masks += [m | (1 << b) for m in masks]
    return bits, masks


def swap_bit(value, axis, size, bit):
    return lax.ppermute(value, axis, [(i, i ^ (1 << bit)) for i in range(size)])


def bit_gather(own, axis, size):
    blocks = own[None]
    for b in bit_order(size)[0]:
        blocks = jnp.concatenate([blocks, swap_bit(blocks, axis, size, b)], axis=0)
    return blocks


def bit_scatter(parts, axis, size):
    me = lax.axis_index(axis)
    for b in reversed(bit_order(size)[0]):
        half = parts.shape[0] // 2
        upper = ((me >> b) & 1) == 1
        keep = jnp.where(upper, parts[half:], parts[:half])
        send = jnp.where(upper, parts[:half], parts[half:])
        parts = keep + swap_bit(send, axis, size, b)
    return parts[0]


def bit_sum(value, axis, size):
    for b in bit_order(size)[0]:
        value = value + swap_bit(value, axis, size, b)
    return value


def forward_layer(streams, x, mods, weights, gains, attend, plain, side, last):
    qkv, out_t, up, down_t = weights
    if plain is not None:
        normed = [
            (plain[s].astype(F32) * (1.0 + mods[s, 1]) + mods[s, 0]).astype(BF16)
            for s in range(2)
        ]
    else:
        normed = streams.gather(
            [modulate(x[s], mods[s, 0], mods[s, 1]).astype(BF16) for s in range(2)]
        )
    raw = side.open([mm(normed[s], qkv[s]).astype(BF16) for s in range(2)])
    o_image, o_text, lse = attend(raw[0], raw[1], gains)
    mixed = side.close((o_image, o_text))
    branch = streams.scatter([mm_nt(mixed[s], out_t[s]) for s in range(2)])
    middle = [x[s] + mods[s, 2] * branch[s] for s in range(2)]
    second = streams.gather(
        [modulate(middle[s], mods[s, 3], mods[s, 4]).astype(BF16) for s in range(2)]
    )
    second = side.open(second)
    hidden = [mm(second[s], up[s]) for s in range(2)]
    active = side.close([gelu(hidden[s]).astype(BF16) for s in range(2)])
    hidden = [hidden[s].astype(BF16) for s in range(2)]
    result = streams.scatter_side([mm_nt(active[s], down_t[s]) for s in range(2)])
    saved = (x, normed, raw, mixed, lse, branch, middle, second, hidden, active)
    if last:
        return None, saved, result
    result = result.result()
    return [middle[s] + mods[s, 5] * result[s] for s in range(2)], saved, result


def backward_layer(streams, gy, dm, saved, mods, weights, gains, calls, side, last):
    qkv, out_t, up, down_t = weights
    x, normed, raw, mixed, lse, branch, middle, second, hidden, active = saved
    if dm is None:
        dm = streams.gather([(mods[s, 5] * gy[s]).astype(BF16) for s in range(2)])
    dm = side.open(dm)
    du = []
    for s in range(2):
        _, pull = jax.vjp(gelu, hidden[s].astype(F32))
        du.append(pull(mm(dm[s], down_t[s]))[0].astype(BF16))
    d_second = side.close([mm_nt(du[s], up[s]).astype(BF16) for s in range(2)])
    d_second = streams.scatter_side(d_second)
    du = d_second.close(d_second.open(du))
    late = [mm_tn(second[s], du[s]) for s in range(2)]
    late += [mm_tn(dm[s], active[s]) for s in range(2)]
    reduced_mlp = calls.reduce_grad(jnp.stack([part.astype(BF16) for part in late]))
    d_second = calls.settle(d_second.result())
    d_middle, d_shift2, d_scale2 = [], [], []
    for s in range(2):
        inner, d_shift, d_scale = modulate_back(middle[s], d_second[s], mods[s, 4])
        d_middle.append(gy[s] + inner)
        d_shift2.append(d_shift)
        d_scale2.append(d_scale)
    d_gate1 = [jnp.sum(d_middle[s] * branch[s], axis=0) for s in range(2)]
    da = streams.gather([(mods[s, 2] * d_middle[s]).astype(BF16) for s in range(2)])
    d_mixed = side.open([mm(da[s], out_t[s]).astype(BF16) for s in range(2)])
    late = jnp.stack([mm_tn(da[s], mixed[s]).astype(BF16) for s in range(2)])
    reduced_out = calls.reduce_grad(late)
    d_image, d_text, gain_rows = calls.attend_back(
        raw[0], raw[1], gains, mixed[0], mixed[1], d_mixed[0], d_mixed[1], lse
    )
    d_raw = side.close((d_image, d_text))
    if last:
        late = jnp.stack([mm_tn(normed[s], d_raw[s]).astype(BF16) for s in range(2)])
        d_raw, late = tie(d_raw, late)
        d_first = [mm_nt(d_raw[s], qkv[s]).astype(BF16) for s in range(2)]
        d_first, reduced_mlp[0] = tie(d_first, reduced_mlp[0])
        d_first = streams.scatter_side(d_first)
    else:
        d_first = streams.scatter_side([mm_nt(d_raw[s], qkv[s]) for s in range(2)])
        d_raw = d_first.close(d_first.open(d_raw))
        late = jnp.stack([mm_tn(normed[s], d_raw[s]).astype(BF16) for s in range(2)])
    reduced_qkv = calls.reduce_grad(late)
    d_first = d_first.result()
    if not last:
        d_first, reduced_mlp[0] = tie(d_first, reduced_mlp[0])
        calls.pending = [reduced_qkv, reduced_out]
    d_gains = gain_rows.reshape(2, 2, HEAD).transpose(1, 0, 2)
    early = (d_gate1, d_shift2, d_scale2), d_gains
    if last:
        d_first = calls.before_end(early, d_first)
    gx, late = [], []
    for s in range(2):
        inner, d_shift, d_scale = modulate_back(x[s], d_first[s], mods[s, 1])
        gx.append(d_middle[s] + inner)
        late += [d_shift, d_scale]
    return gx, early, late, (reduced_qkv, reduced_out, reduced_mlp)


class Calls:
    def __init__(self, attend_back, dp_axis):
        self.attend_back, self.axis, self.pending = attend_back, dp_axis, []
        self.before_end = None

    def reduce_grad(self, grad):
        return [lax.psum_scatter(grad, self.axis, scatter_dimension=1, tiled=True)]

    def settle(self, token):
        for box in self.pending:
            token, box[0] = tie(token, box[0])
        self.pending = []
        return token


def on_device(dp, seq, width_of_group, *args):
    (
        image_in,
        text_input,
        condition,
        ada_weight,
        qkv_weight,
        out_weight,
        up_weight,
        down_weight,
        norm_gain,
        image_cotangent,
        text_cotangent,
    ) = args
    dp_axis, dp_size = dp
    seq_axis, seq_size = seq
    layers = qkv_weight.shape[0]
    width = image_in.shape[2]
    streams = Streams(image_in.shape[1], text_input.shape[1], seq_axis, seq_size)
    attend, attend_back = (
        (attention_forward, attention_backward)
        if width_of_group % 128 == 0
        else (plain_forward, plain_backward)
    )
    rows = qkv_weight.shape[2]

    def fetch(local):
        return lax.all_gather(local, dp_axis, axis=1, tiled=True)

    qkv_local = qkv_weight.reshape(layers, 2, rows, 3, -1, width_of_group)
    qkv_local = qkv_local.transpose(0, 1, 2, 4, 3, 5).reshape(layers, 2, rows, -1)
    out_local = out_weight.transpose(0, 1, 3, 2)
    down_local = down_weight.transpose(0, 1, 3, 2)
    weights = [
        tuple(fetch(w[l]) for w in (qkv_local, out_local, up_weight, down_local))
        for l in range(layers)
    ]

    act_cond, silu_pull = jax.vjp(jax.nn.silu, condition.astype(F32))
    act_low = act_cond.astype(BF16)
    partial_mods = jnp.einsum("nd,lsde->nlse", act_low, ada_weight, preferred_element_type=F32)
    own_mods = bit_scatter(partial_mods.reshape(dp_size, -1), dp_axis, dp_size)
    x = [image_in[0].astype(F32), text_input[0].astype(F32)]
    plain = streams.gather([layer_stats(part)[0].astype(BF16) for part in x])
    own_mods, plain = tie(own_mods, plain)
    own_mods = bit_sum(own_mods, seq_axis, seq_size).reshape(layers, 2, 6, width)
    gains_all = norm_gain.astype(F32)
    gain_columns = [gains_all[l].transpose(1, 0, 2).reshape(4, HEAD).T for l in range(layers)]

    gy = [image_cotangent[0].astype(F32), text_cotangent[0].astype(F32)]
    side = streams.gather_side(
        [(own_mods[layers - 1, s, 5] * gy[s]).astype(BF16) for s in range(2)]
    )
    saved_list, results = [], []
    for l in range(layers):
        x, saved, result = forward_layer(
            streams,
            x,
            own_mods[l],
            weights[l],
            gain_columns[l],
            attend,
            None if l else plain,
            side,
            l == layers - 1,
        )
        saved_list.append(saved)
        results.append(result)
    dm, side = side.result(), results[-1]

    def share(values):
        return bit_gather(bit_sum(values, seq_axis, seq_size), dp_axis, dp_size)

    gys, early_all, late_all = [None] * layers, [None] * layers, [None] * layers
    grads, ends = [None] * layers, {}

    def before_end(early, token):
        early_all[0] = early
        results[-1] = side.result()
        parts = []
        for l in range(layers):
            d_gate2 = [jnp.sum(gys[l][s] * results[l][s], axis=0) for s in range(2)]
            d_gate1, d_shift2, d_scale2 = early_all[l][0]
            for s in range(2):
                parts += late_all[l][2 * s : 2 * s + 2] if l else []
                parts += [d_gate1[s], d_shift2[s], d_scale2[s], d_gate2[s]]
        gain_parts = [early_all[l][1].reshape(-1) for l in range(layers)]
        shared = share(jnp.concatenate(parts + gain_parts))
        ends["early"], token = tie(shared, token)
        return token

    calls = Calls(attend_back, dp_axis)
    calls.before_end = before_end
    for l in reversed(range(layers)):
        gys[l] = gy
        gy, early_all[l], late_all[l], grads[l] = backward_layer(
            streams,
            gy,
            dm,
            saved_list[l],
            own_mods[l],
            weights[l],
            gain_columns[l],
            calls,
            side,
            l == 0,
        )
        dm = None
    last_middle = saved_list[-1][6]
    outputs = [
        (last_middle[s] + own_mods[layers - 1, s, 5] * results[-1][s]).astype(BF16)[None]
        for s in range(2)
    ]

    there = jnp.array(bit_order(dp_size)[1], jnp.int32) ^ lax.axis_index(dp_axis)
    late_all[0], grads[0] = tie(late_all[0], grads[0])
    rest = share(jnp.concatenate(late_all[0])).reshape(dp_size, 2, 2 * width)
    early, total_mods, place = ends["early"], [], 0
    for l in range(layers):
        size = (6 if l else 4) * width
        part = early[:, place : place + 2 * size].reshape(dp_size, 2, size)
        place += 2 * size
        total_mods.append(part if l else jnp.concatenate([rest, part], axis=2))
    total_mods = jnp.stack(total_mods, axis=1)
    total_gains = jnp.sum(early[:, place:][there], axis=0).reshape(layers, 2, 2, HEAD)
    act_there = act_low.astype(F32)[there]
    ada_grad = jnp.einsum("nd,nlse->lsde", act_there, total_mods, precision=HIGHEST)
    d_act = jnp.einsum("nlse,lsde->nd", total_mods, ada_weight.astype(F32), precision=HIGHEST)
    condition_grad = silu_pull(d_act[there])[0]

    def pieces(kind, first):
        return jnp.stack([grads[l][kind][0][first : first + 2] for l in range(layers)]).astype(F32)

    qkv_grad = pieces(0, 0).reshape(layers, 2, rows, -1, 3, width_of_group)
    qkv_grad = qkv_grad.transpose(0, 1, 2, 4, 3, 5).reshape(qkv_weight.shape)
    return (
        outputs[0],
        outputs[1],
        gy[0][None],
        gy[1][None],
        condition_grad,
        ada_grad,
        qkv_grad,
        pieces(1, 0).transpose(0, 1, 3, 2),
        pieces(2, 0),
        pieces(2, 2).transpose(0, 1, 3, 2),
        total_gains,
    )


def solution(mesh):
    tokens = P("dp", "seq", None)
    placed = (
        tokens,
        tokens,
        P(None, ("dp", "seq")),
        P(None, None, ("dp", "seq"), None),
        P(None, None, "dp", None, "seq"),
        P(None, None, "seq", "dp"),
        P(None, None, "dp", "seq"),
        P(None, None, "seq", "dp"),
        P(),
        tokens,
        tokens,
    )
    results = (tokens, tokens, tokens, tokens) + placed[2:8] + (P(),)

    def step(*args):
        heads = args[4].shape[4] // mesh.shape["seq"] // HEAD
        group = 2 * HEAD if heads % 2 == 0 else HEAD
        body = functools.partial(
            on_device, ("dp", mesh.shape["dp"]), ("seq", mesh.shape["seq"]), group
        )
        return jax.shard_map(
            body, mesh=mesh, in_specs=placed, out_specs=results, check_vma=False
        )(*args)

    return step
```

```python
import functools

import jax
import jax.numpy as jnp
from jax import lax
from jax.experimental import pallas as pl
from jax.experimental.pallas import tpu as pltpu
from jax.sharding import PartitionSpec as P

EPSILON = 1e-06
HIGHEST = lax.Precision.HIGHEST
F32 = jnp.float32
BF16 = jnp.bfloat16
HEAD = 64


def layer_stats(values):
    centred = values - jnp.mean(values, axis=-1, keepdims=True)
    root = lax.rsqrt(jnp.mean(centred * centred, axis=-1, keepdims=True) + EPSILON)
    return centred * root, root


def modulate(values, shift, scale):
    return layer_stats(values)[0] * (1.0 + scale) + shift


def modulate_back(values, grad, scale):
    normed, root = layer_stats(values)
    inner = grad * (1.0 + scale)
    first = jnp.mean(inner, axis=-1, keepdims=True)
    second = jnp.mean(inner * normed, axis=-1, keepdims=True)
    d_values = root * (inner - first - normed * second)
    return d_values, jnp.sum(grad, axis=0), jnp.sum(grad * normed, axis=0)


def mm(left, right):
    return lax.dot_general(left, right, (((1,), (0,)), ((), ())), preferred_element_type=F32)


def mm_nt(left, right):
    return lax.dot_general(left, right, (((1,), (1,)), ((), ())), preferred_element_type=F32)


def mm_tn(left, right):
    return lax.dot_general(left, right, (((0,), (0,)), ((), ())), preferred_element_type=F32)


def gelu(values):
    return jax.nn.gelu(values, approximate=True)


def head_factors(raw_t, gain_image, gain_text, image_len):
    root = lax.rsqrt(jnp.mean(raw_t * raw_t, axis=0, keepdims=True) + EPSILON)
    lanes = lax.broadcasted_iota(jnp.int32, raw_t.shape, 1)
    gain = jnp.where(lanes < image_len, gain_image, gain_text)
    return raw_t * root, root, gain


def transposed(first, second, low, high):
    return jnp.concatenate(
        [first[:, low:high].astype(F32).T, second[:, low:high].astype(F32).T], axis=1
    )


def attention_forward_kernel(step, image_ref, text_ref, gain_ref, o_image, o_text, lse_ref, o_scr):
    image_len, text_len = image_ref.shape[0], text_ref.shape[0]
    total = image_len + text_len
    wide = image_ref.shape[1] // 3
    factor = HEAD ** (-0.5)
    raw_q = transposed(image_ref, text_ref, 0, wide)
    raw_k = transposed(image_ref, text_ref, wide, 2 * wide)
    values_t = transposed(image_ref, text_ref, 2 * wide, 3 * wide).astype(BF16)
    for head in range(wide // HEAD):
        rows = slice(head * HEAD, (head + 1) * HEAD)
        q_hat, _, q_gain = head_factors(raw_q[rows], gain_ref[:, 0:1], gain_ref[:, 1:2], image_len)
        k_hat, _, k_gain = head_factors(raw_k[rows], gain_ref[:, 2:3], gain_ref[:, 3:4], image_len)
        q_t = ((q_hat * q_gain).astype(BF16).astype(F32) * factor).astype(BF16)
        keys = (k_hat * k_gain).T.astype(BF16)
        v_t = values_t[rows]
        for start in range(0, total, step):
            part = slice(start, start + step)
            scores = mm(keys, q_t[:, part])
            largest = jnp.max(scores, axis=0, keepdims=True)
            weights = jnp.exp(scores - largest)
            total_w = jnp.sum(weights, axis=0, keepdims=True)
            out = mm(v_t, weights.astype(BF16)) * (1.0 / total_w)
            o_scr[rows, part] = out
            lse_ref[head, :, part] = largest + jnp.log(total_w)
    o_image[...] = o_scr[:, :image_len].T.astype(BF16)
    o_text[...] = o_scr[:, image_len:].T.astype(BF16)


def attention_backward_kernel(
    step,
    image_ref,
    text_ref,
    gain_ref,
    o_image,
    o_text,
    do_image,
    do_text,
    lse_ref,
    d_image,
    d_text,
    gain_grad,
    dq_scr,
    dk_scr,
    dv_scr,
):
    image_len, text_len = image_ref.shape[0], text_ref.shape[0]
    total = image_len + text_len
    wide = image_ref.shape[1] // 3
    factor = HEAD ** (-0.5)
    raw_q = transposed(image_ref, text_ref, 0, wide)
    raw_k = transposed(image_ref, text_ref, wide, 2 * wide)
    o_t = transposed(o_image, o_text, 0, wide)
    do_t = transposed(do_image, do_text, 0, wide)
    lane_row = lax.broadcasted_iota(jnp.int32, (HEAD, 128), 1)
    gains_total = jnp.zeros((HEAD, 128), F32)
    for head in range(wide // HEAD):
        rows = slice(head * HEAD, (head + 1) * HEAD)
        low, high = 2 * wide + head * HEAD, 2 * wide + (head + 1) * HEAD
        q_hat, q_root, q_gain = head_factors(
            raw_q[rows], gain_ref[:, 0:1], gain_ref[:, 1:2], image_len
        )
        k_hat, k_root, k_gain = head_factors(
            raw_k[rows], gain_ref[:, 2:3], gain_ref[:, 3:4], image_len
        )
        q_full = (q_hat * q_gain).astype(BF16).astype(F32) * factor
        q_t = q_full.astype(BF16)
        queries = q_full.T.astype(BF16)
        k_t = (k_hat * k_gain).astype(BF16)
        keys = (k_hat * k_gain).T.astype(BF16)
        values = jnp.concatenate([image_ref[:, low:high], text_ref[:, low:high]], axis=0)
        d_out = jnp.concatenate([do_image[:, rows], do_text[:, rows]], axis=0)
        delta = jnp.sum(do_t[rows] * o_t[rows], axis=0, keepdims=True)
        d_out_t = do_t[rows].astype(BF16)
        d_keys = jnp.zeros((total, HEAD), F32)
        d_values = jnp.zeros((total, HEAD), F32)
        for start in range(0, total, step):
            part = slice(start, start + step)
            weights = jnp.exp(mm(keys, q_t[:, part]) - lse_ref[head, :, part])
            d_weights = mm(values, d_out_t[:, part])
            d_scores = (weights * (d_weights - delta[:, part])).astype(BF16)
            d_values += mm(weights.astype(BF16), d_out[part])
            d_keys += mm(d_scores, queries[part])
            dq_scr[rows, part] = mm(k_t, d_scores) * factor
        dv_scr[:, rows] = d_values
        dq = dq_scr[rows, :]
        dk = d_keys.T
        for slot, (grad, hat) in enumerate(((dq, q_hat), (dk, k_hat))):
            product = grad * hat
            image_sum = jnp.sum(product[:, :image_len], axis=1, keepdims=True)
            text_sum = jnp.sum(product[:, image_len:], axis=1, keepdims=True)
            gains_total += jnp.where(lane_row == 2 * slot, image_sum, 0.0)
            gains_total += jnp.where(lane_row == 2 * slot + 1, text_sum, 0.0)
        scaled = dq * q_gain
        dq_scr[rows, :] = q_root * (
            scaled - q_hat * jnp.mean(scaled * q_hat, axis=0, keepdims=True)
        )
        scaled = dk * k_gain
        dk_scr[rows, :] = k_root * (
            scaled - k_hat * jnp.mean(scaled * k_hat, axis=0, keepdims=True)
        )
    d_image[:, :wide] = dq_scr[:, :image_len].T.astype(BF16)
    d_text[:, :wide] = dq_scr[:, image_len:].T.astype(BF16)
    d_image[:, wide : 2 * wide] = dk_scr[:, :image_len].T.astype(BF16)
    d_text[:, wide : 2 * wide] = dk_scr[:, image_len:].T.astype(BF16)
    d_image[:, 2 * wide :] = dv_scr[:image_len].astype(BF16)
    d_text[:, 2 * wide :] = dv_scr[image_len:].astype(BF16)
    gain_grad[0] = gains_total


def query_step(total):
    for count in (3, 4, 2, 6, 9, 1):
        if total % (count * 128) == 0:
            return total // count
    return total


def kernel_cost(tokens, heads, products):
    return pl.CostEstimate(
        flops=2 * products * heads * tokens * tokens * HEAD * 4,
        transcendentals=heads * tokens * tokens,
        bytes_accessed=tokens * heads * HEAD * 2 * 8,
    )


def attention_forward(raw_image, raw_text, gains):
    groups = raw_image.shape[1] // (3 * 128)
    image_len, text_len = raw_image.shape[0], raw_text.shape[0]
    total = image_len + text_len
    return pl.pallas_call(
        functools.partial(attention_forward_kernel, query_step(total)),
        grid=(groups,),
        out_shape=(
            jax.ShapeDtypeStruct((image_len, groups * 128), BF16),
            jax.ShapeDtypeStruct((text_len, groups * 128), BF16),
            jax.ShapeDtypeStruct((groups * 2, 1, total), F32),
        ),
        in_specs=[
            pl.BlockSpec((image_len, 384), lambda g: (0, g)),
            pl.BlockSpec((text_len, 384), lambda g: (0, g)),
            pl.BlockSpec((HEAD, 4), lambda g: (0, 0)),
        ],
        out_specs=(
            pl.BlockSpec((image_len, 128), lambda g: (0, g)),
            pl.BlockSpec((text_len, 128), lambda g: (0, g)),
            pl.BlockSpec((2, 1, total), lambda g: (g, 0, 0)),
        ),
        scratch_shapes=[pltpu.VMEM((128, total), F32)],
        cost_estimate=kernel_cost(total, groups * 2, 2),
        name="attend_forward",
    )(raw_image, raw_text, gains)


def attention_backward(raw_image, raw_text, gains, o_image, o_text, do_image, do_text, lse):
    groups = raw_image.shape[1] // (3 * 128)
    image_len, text_len = raw_image.shape[0], raw_text.shape[0]
    total = image_len + text_len
    wide_image = pl.BlockSpec((image_len, 384), lambda g: (0, g))
    wide_text = pl.BlockSpec((text_len, 384), lambda g: (0, g))
    slim_image = pl.BlockSpec((image_len, 128), lambda g: (0, g))
    slim_text = pl.BlockSpec((text_len, 128), lambda g: (0, g))
    d_image, d_text, gain_grad = pl.pallas_call(
        functools.partial(attention_backward_kernel, query_step(total)),
        grid=(groups,),
        out_shape=(
            jax.ShapeDtypeStruct(raw_image.shape, BF16),
            jax.ShapeDtypeStruct(raw_text.shape, BF16),
            jax.ShapeDtypeStruct((groups, HEAD, 128), F32),
        ),
        in_specs=[
            wide_image,
            wide_text,
            pl.BlockSpec((HEAD, 4), lambda g: (0, 0)),
            slim_image,
            slim_text,
            slim_image,
            slim_text,
            pl.BlockSpec((2, 1, total), lambda g: (g, 0, 0)),
        ],
        out_specs=(wide_image, wide_text, pl.BlockSpec((1, HEAD, 128), lambda g: (g, 0, 0))),
        scratch_shapes=[
            pltpu.VMEM((128, total), F32),
            pltpu.VMEM((128, total), F32),
            pltpu.VMEM((total, 128), F32),
        ],
        cost_estimate=kernel_cost(total, groups * 2, 5),
        name="attend_backward",
    )(raw_image, raw_text, gains, o_image, o_text, do_image, do_text, lse)
    return d_image, d_text, jnp.sum(gain_grad, axis=0)[:, :4].T


def plain_parts(raw_image, raw_text, gains):
    raw = jnp.concatenate([raw_image, raw_text], axis=0).astype(F32)
    raw = raw.reshape(raw.shape[0], -1, 3, HEAD)
    is_image = (jnp.arange(raw.shape[0]) < raw_image.shape[0])[:, None, None]
    hats, roots, scales, rounded = [], [], [], []
    for slot in range(2):
        part = raw[:, :, slot]
        root = lax.rsqrt(jnp.mean(part * part, axis=-1, keepdims=True) + EPSILON)
        scale = jnp.where(is_image, gains[:, 2 * slot], gains[:, 2 * slot + 1])
        hats.append(part * root)
        roots.append(root)
        scales.append(scale)
        rounded.append((part * root * scale).astype(BF16))
    return hats, roots, scales, rounded, raw[:, :, 2].astype(BF16)


def plain_forward(raw_image, raw_text, gains):
    _, _, _, (queries, keys), values = plain_parts(raw_image, raw_text, gains)
    scores = jnp.einsum("qhd,khd->hqk", queries, keys, preferred_element_type=F32)
    scores = scores * HEAD ** (-0.5)
    largest = jnp.max(scores, axis=-1, keepdims=True)
    lse = largest + jnp.log(jnp.sum(jnp.exp(scores - largest), axis=-1, keepdims=True))
    weights = jnp.exp(scores - lse).astype(BF16)
    out = jnp.einsum("hqk,khd->qhd", weights, values, preferred_element_type=F32)
    out = out.astype(BF16).reshape(out.shape[0], -1)
    return out[: raw_image.shape[0]], out[raw_image.shape[0] :], lse


def plain_backward(raw_image, raw_text, gains, o_image, o_text, do_image, do_text, lse):
    hats, roots, scales, (queries, keys), values = plain_parts(raw_image, raw_text, gains)
    factor = HEAD ** (-0.5)
    image_len = raw_image.shape[0]
    d_out = jnp.concatenate([do_image, do_text], axis=0).reshape(queries.shape)
    scores = jnp.einsum("qhd,khd->hqk", queries, keys, preferred_element_type=F32) * factor
    weights = jnp.exp(scores - lse)
    d_weights = jnp.einsum("qhd,khd->hqk", d_out, values, preferred_element_type=F32)
    inner = jnp.sum(weights * d_weights, axis=-1, keepdims=True)
    d_scores = (weights * (d_weights - inner)).astype(BF16)
    dq = jnp.einsum("hqk,khd->qhd", d_scores, keys, preferred_element_type=F32) * factor
    dk = jnp.einsum("hqk,qhd->khd", d_scores, queries, preferred_element_type=F32) * factor
    dv = jnp.einsum("hqk,qhd->khd", weights.astype(BF16), d_out, preferred_element_type=F32)
    gain_rows, parts = [], []
    for grad, hat, root, scale in zip((dq, dk), hats, roots, scales):
        product = grad * hat
        gain_rows += [jnp.sum(product[:image_len], (0, 1)), jnp.sum(product[image_len:], (0, 1))]
        scaled = grad * scale
        parts.append(root * (scaled - hat * jnp.mean(scaled * hat, axis=-1, keepdims=True)))
    joined = jnp.stack(parts + [dv], axis=2).astype(BF16).reshape(d_out.shape[0], -1)
    return joined[:image_len], joined[image_len:], jnp.stack(gain_rows)


def tie(*groups):
    return lax.optimization_barrier(groups)


class Side:
    def __init__(self, state=(), steps=(), finish=None):
        self.state, self.steps, self.finish = state, list(steps), finish
        self.running = False

    def open(self, token):
        if self.steps:
            token, self.state = tie(token, self.state)
            self.state = self.steps.pop(0)(self.state)
            self.running = True
        return token

    def close(self, token):
        if self.running:
            token, self.state = tie(token, self.state)
            self.running = False
        return token

    def result(self):
        while self.steps:
            self.state = self.steps.pop(0)(self.state)
        return self.finish(self.state)


def join_kernel(size, cut, me_ref, own, *refs):
    after, before = refs[: size - 1], refs[size - 1 : 2 * size - 2]
    image, text, sems = refs[2 * size - 2 :]
    tail = own.shape[0] - cut

    def copies(source, k):
        return (
            pltpu.make_async_copy(
                source.at[pl.ds(0, cut)], image.at[pl.ds(k * cut, cut)], sems.at[k, 0]
            ),
            pltpu.make_async_copy(
                source.at[pl.ds(cut, tail)], text.at[pl.ds(k * tail, tail)], sems.at[k, 1]
            ),
        )

    def start(source, k):
        for copy in copies(source, k):
            copy.start()

    start(own, 0)
    for k in range(1, size):
        from_after = me_ref[0] + k < size
        pl.when(from_after)(functools.partial(start, after[k - 1], k))
        pl.when(jnp.logical_not(from_after))(functools.partial(start, before[size - k - 1], k))
    for k in range(size):
        for copy in copies(own, k):
            copy.wait()


def join_tokens(own, after, before, me, cut):
    size, (rows, width) = len(after) + 1, own.shape
    return pl.pallas_call(
        functools.partial(join_kernel, size, cut),
        out_shape=(
            jax.ShapeDtypeStruct((size * cut, width), own.dtype),
            jax.ShapeDtypeStruct((size * (rows - cut), width), own.dtype),
        ),
        in_specs=[pl.BlockSpec(memory_space=pltpu.SMEM)]
        + [pl.BlockSpec(memory_space=pl.ANY)] * (2 * size - 1),
        out_specs=(
            pl.BlockSpec(memory_space=pltpu.VMEM),
            pl.BlockSpec(memory_space=pltpu.VMEM),
        ),
        scratch_shapes=[pltpu.SemaphoreType.DMA((size, 2))],
        compiler_params=pltpu.CompilerParams(vmem_limit_bytes=16 * 2**20),
        cost_estimate=pl.CostEstimate(
            flops=0, transcendentals=0, bytes_accessed=4 * size * own.size
        ),
        name="join_tokens",
    )(me.astype(jnp.int32)[None], own, *after, *before)


class Streams:
    def __init__(self, image_len, text_len, axis, size):
        self.lengths = (image_len, text_len)
        self.axis, self.size = axis, size

    def gather_side(self, pair):
        size = self.size

        def step(state):
            own, after, before = state
            down, up = (after[-1], before[-1]) if after else (own, own)
            down = lax.ppermute(down, self.axis, [(i, i - 1) for i in range(1, size)])
            up = lax.ppermute(up, self.axis, [(i, i + 1) for i in range(size - 1)])
            return own, after + (down,), before + (up,)

        def finish(state):
            return join_tokens(*state, lax.axis_index(self.axis), self.lengths[0])

        return Side((jnp.concatenate(pair, axis=0), (), ()), [step] * (size - 1), finish)

    def scatter_side(self, pair):
        size, (image_len, text_len) = self.size, self.lengths
        image, text = (part.astype(BF16) for part in pair)
        cut = (image_len + text_len) // 32 * 16
        firsts = tuple(image[k * image_len : k * image_len + cut] for k in range(size))
        seconds = tuple(
            jnp.concatenate(
                [
                    image[k * image_len + cut : (k + 1) * image_len],
                    text[k * text_len : (k + 1) * text_len],
                ],
                axis=0,
            )
            for k in range(size)
        )

        def step(index, state):
            return tuple(half_step(index, *half) for half in state)

        def half_step(index, blocks, sums):
            k = size - 1 - index
            send_up, send_down = blocks[k], blocks[size - k]
            if sums:
                send_up, send_down = (
                    (send.astype(F32) + value.astype(F32)).astype(BF16)
                    for send, value in zip((send_up, send_down), sums)
                )
            up = lax.ppermute(send_up, self.axis, [(i, i + 1) for i in range(index + 1)])
            down = lax.ppermute(send_down, self.axis, [(i, i - 1) for i in range(k, size)])
            return blocks, (up, down)

        def finish(state):
            first, second = (
                blocks[0].astype(F32) + up.astype(F32) + down.astype(F32)
                for blocks, (up, down) in state
            )
            return (
                jnp.concatenate([first, second[: image_len - cut]], axis=0),
                second[image_len - cut :],
            )

        steps = [functools.partial(step, index) for index in range(size - 1)]
        return Side(((firsts, ()), (seconds, ())), steps, finish)

    def gather(self, pair):
        return self.gather_side(pair).result()

    def scatter(self, pair):
        return self.scatter_side(pair).result()


def bit_order(size):
    bits = [b for b in range(size.bit_length() - 1)]
    masks = [0]
    for b in bits:
        masks += [m | (1 << b) for m in masks]
    return bits, masks


def swap_bit(value, axis, size, bit):
    return lax.ppermute(value, axis, [(i, i ^ (1 << bit)) for i in range(size)])


def bit_gather(own, axis, size):
    blocks = own[None]
    for b in bit_order(size)[0]:
        blocks = jnp.concatenate([blocks, swap_bit(blocks, axis, size, b)], axis=0)
    return blocks


def bit_scatter(parts, axis, size):
    me = lax.axis_index(axis)
    for b in reversed(bit_order(size)[0]):
        half = parts.shape[0] // 2
        upper = ((me >> b) & 1) == 1
        keep = jnp.where(upper, parts[half:], parts[:half])
        send = jnp.where(upper, parts[:half], parts[half:])
        parts = keep + swap_bit(send, axis, size, b)
    return parts[0]


def bit_sum(value, axis, size):
    for b in bit_order(size)[0]:
        value = value + swap_bit(value, axis, size, b)
    return value


def pack_rows(rows):
    place = lax.broadcasted_iota(jnp.int32, (-(-len(rows) // 8) * 8, rows[0].shape[0]), 0)
    packed = jnp.zeros(place.shape, F32)
    for k, row in enumerate(rows):
        packed = jnp.where(place == k, row[None], packed)
    return packed


def forward_layer(streams, x, mods, weights, gains, attend, plain, side, last):
    qkv, out_t, up, down_t = weights
    if plain is not None:
        normed = [
            (plain[s].astype(F32) * (1.0 + mods[s, 1]) + mods[s, 0]).astype(BF16)
            for s in range(2)
        ]
    else:
        normed = streams.gather(
            [modulate(x[s], mods[s, 0], mods[s, 1]).astype(BF16) for s in range(2)]
        )
    raw = side.open([mm(normed[s], qkv[s]).astype(BF16) for s in range(2)])
    o_image, o_text, lse = attend(raw[0], raw[1], gains)
    mixed = side.close((o_image, o_text))
    branch = streams.scatter([mm_nt(mixed[s], out_t[s]) for s in range(2)])
    middle = [x[s] + mods[s, 2] * branch[s] for s in range(2)]
    second = streams.gather(
        [modulate(middle[s], mods[s, 3], mods[s, 4]).astype(BF16) for s in range(2)]
    )
    second = side.open(second)
    hidden = [mm(second[s], up[s]) for s in range(2)]
    active = side.close([gelu(hidden[s]).astype(BF16) for s in range(2)])
    hidden = [hidden[s].astype(BF16) for s in range(2)]
    result = streams.scatter_side([mm_nt(active[s], down_t[s]) for s in range(2)])
    saved = (x, normed, raw, mixed, lse, branch, middle, second, hidden, active)
    if last:
        return None, saved, result
    result = result.result()
    return [middle[s] + mods[s, 5] * result[s] for s in range(2)], saved, result


def backward_layer(streams, gy, dm, saved, mods, weights, gains, calls, side, last):
    qkv, out_t, up, down_t = weights
    x, normed, raw, mixed, lse, branch, middle, second, hidden, active = saved
    if dm is None:
        dm = streams.gather([(mods[s, 5] * gy[s]).astype(BF16) for s in range(2)])
    dm = side.open(dm)
    du = []
    for s in range(2):
        _, pull = jax.vjp(gelu, hidden[s].astype(F32))
        du.append(pull(mm(dm[s], down_t[s]))[0].astype(BF16))
    d_second = side.close([mm_nt(du[s], up[s]).astype(BF16) for s in range(2)])
    d_second = streams.scatter_side(d_second)
    du = d_second.close(d_second.open(du))
    late = [mm_tn(second[s], du[s]) for s in range(2)]
    late += [mm_tn(dm[s], active[s]) for s in range(2)]
    reduced_mlp = calls.reduce_grad(jnp.stack([part.astype(BF16) for part in late]))
    d_second = calls.settle(d_second.result())
    d_middle, d_shift2, d_scale2 = [], [], []
    for s in range(2):
        inner, d_shift, d_scale = modulate_back(middle[s], d_second[s], mods[s, 4])
        d_middle.append(gy[s] + inner)
        d_shift2.append(d_shift)
        d_scale2.append(d_scale)
    d_gate1 = [jnp.sum(d_middle[s] * branch[s], axis=0) for s in range(2)]
    da = streams.gather([(mods[s, 2] * d_middle[s]).astype(BF16) for s in range(2)])
    d_mixed = side.open([mm(da[s], out_t[s]).astype(BF16) for s in range(2)])
    late = jnp.stack([mm_tn(da[s], mixed[s]).astype(BF16) for s in range(2)])
    reduced_out = calls.reduce_grad(late)
    d_image, d_text, gain_rows = calls.attend_back(
        raw[0], raw[1], gains, mixed[0], mixed[1], d_mixed[0], d_mixed[1], lse
    )
    d_raw = side.close((d_image, d_text))
    if last:
        late = jnp.stack([mm_tn(normed[s], d_raw[s]).astype(BF16) for s in range(2)])
        d_raw, late = tie(d_raw, late)
        d_first = [mm_nt(d_raw[s], qkv[s]).astype(BF16) for s in range(2)]
        d_first, reduced_mlp[0] = tie(d_first, reduced_mlp[0])
        d_first = streams.scatter_side(d_first)
    else:
        d_first = streams.scatter_side([mm_nt(d_raw[s], qkv[s]) for s in range(2)])
        d_raw = d_first.close(d_first.open(d_raw))
        late = jnp.stack([mm_tn(normed[s], d_raw[s]).astype(BF16) for s in range(2)])
    reduced_qkv = calls.reduce_grad(late)
    d_first = d_first.result()
    if not last:
        d_first, reduced_mlp[0] = tie(d_first, reduced_mlp[0])
        calls.pending = [reduced_qkv, reduced_out]
    d_gains = gain_rows.reshape(2, 2, HEAD).transpose(1, 0, 2)
    early = (d_gate1, d_shift2, d_scale2), d_gains
    if last:
        d_first = calls.before_end(early, d_first)
    gx, late = [], []
    for s in range(2):
        inner, d_shift, d_scale = modulate_back(x[s], d_first[s], mods[s, 1])
        gx.append(d_middle[s] + inner)
        late += [d_shift, d_scale]
    return gx, early, late, (reduced_qkv, reduced_out, reduced_mlp)


class Calls:
    def __init__(self, attend_back, dp_axis):
        self.attend_back, self.axis, self.pending = attend_back, dp_axis, []
        self.before_end = None

    def reduce_grad(self, grad):
        return [lax.psum_scatter(grad, self.axis, scatter_dimension=1, tiled=True)]

    def settle(self, token):
        for box in self.pending:
            token, box[0] = tie(token, box[0])
        self.pending = []
        return token


def on_device(dp, seq, width_of_group, *args):
    (
        image_in,
        text_input,
        condition,
        ada_weight,
        qkv_weight,
        out_weight,
        up_weight,
        down_weight,
        norm_gain,
        image_cotangent,
        text_cotangent,
    ) = args
    dp_axis, dp_size = dp
    seq_axis, seq_size = seq
    layers = qkv_weight.shape[0]
    width = image_in.shape[2]
    streams = Streams(image_in.shape[1], text_input.shape[1], seq_axis, seq_size)
    attend, attend_back = (
        (attention_forward, attention_backward)
        if width_of_group % 128 == 0
        else (plain_forward, plain_backward)
    )
    rows = qkv_weight.shape[2]

    x = [image_in[0].astype(F32), text_input[0].astype(F32)]
    plain = streams.gather_side([layer_stats(part)[0].astype(BF16) for part in x])
    given = (qkv_weight, out_weight, up_weight, down_weight)
    plain.state, given = tie(plain.state, given)
    qkv_weight, out_weight, up_weight, down_weight = given
    plain = plain.result()

    def fetch(local):
        return lax.all_gather(local, dp_axis, axis=1, tiled=True)

    qkv_local = qkv_weight.reshape(layers, 2, rows, 3, -1, width_of_group)
    qkv_local = qkv_local.transpose(0, 1, 2, 4, 3, 5).reshape(layers, 2, rows, -1)
    out_local = out_weight.transpose(0, 1, 3, 2)
    down_local = down_weight.transpose(0, 1, 3, 2)
    weights = [
        tuple(fetch(w[l]) for w in (qkv_local, out_local, up_weight, down_local))
        for l in range(layers)
    ]

    act_cond, silu_pull = jax.vjp(jax.nn.silu, condition.astype(F32))
    act_low = act_cond.astype(BF16)
    partial_mods = jnp.einsum("nd,lsde->nlse", act_low, ada_weight, preferred_element_type=F32)
    own_mods = bit_scatter(partial_mods.reshape(dp_size, -1), dp_axis, dp_size)
    own_mods, plain = tie(own_mods, plain)
    own_mods = bit_sum(own_mods, seq_axis, seq_size).reshape(layers, 2, 6, width)
    gains_all = norm_gain.astype(F32)
    gain_columns = [gains_all[l].transpose(1, 0, 2).reshape(4, HEAD).T for l in range(layers)]

    gy = [image_cotangent[0].astype(F32), text_cotangent[0].astype(F32)]
    side = streams.gather_side(
        [(own_mods[layers - 1, s, 5] * gy[s]).astype(BF16) for s in range(2)]
    )
    saved_list, results = [], []
    for l in range(layers):
        x, saved, result = forward_layer(
            streams,
            x,
            own_mods[l],
            weights[l],
            gain_columns[l],
            attend,
            None if l else plain,
            side,
            l == layers - 1,
        )
        saved_list.append(saved)
        results.append(result)
    dm, side = side.result(), results[-1]

    def share(values):
        return bit_gather(bit_sum(values, seq_axis, seq_size), dp_axis, dp_size)

    gys, early_all, late_all = [None] * layers, [None] * layers, [None] * layers
    grads, ends = [None] * layers, {}

    def before_end(early, token):
        early_all[0] = early
        results[-1] = side.result()
        parts = []
        for l in range(layers):
            d_gate2 = [jnp.sum(gys[l][s] * results[l][s], axis=0) for s in range(2)]
            d_gate1, d_shift2, d_scale2 = early_all[l][0]
            for s in range(2):
                parts += late_all[l][2 * s : 2 * s + 2] if l else []
                parts += [d_gate1[s], d_shift2[s], d_scale2[s], d_gate2[s]]
        for l in range(layers):
            gain_row = early_all[l][1].reshape(-1)
            parts.append(jnp.pad(gain_row, (0, width - gain_row.shape[0])))
        shared = share(pack_rows(parts))
        ends["early"], token = tie(shared, token)
        return token

    calls = Calls(attend_back, dp_axis)
    calls.before_end = before_end
    for l in reversed(range(layers)):
        gys[l] = gy
        gy, early_all[l], late_all[l], grads[l] = backward_layer(
            streams,
            gy,
            dm,
            saved_list[l],
            own_mods[l],
            weights[l],
            gain_columns[l],
            calls,
            side,
            l == 0,
        )
        dm = None
    last_middle = saved_list[-1][6]
    outputs = [
        (last_middle[s] + own_mods[layers - 1, s, 5] * results[-1][s]).astype(BF16)[None]
        for s in range(2)
    ]

    there = jnp.array(bit_order(dp_size)[1], jnp.int32) ^ lax.axis_index(dp_axis)
    late_all[0], grads[0] = tie(late_all[0], grads[0])
    rest = share(pack_rows(late_all[0]))[:, :4].reshape(dp_size, 2, 2 * width)
    early, total_mods, place = ends["early"], [], 0
    for l in range(layers):
        count = 12 if l else 8
        part = early[:, place : place + count].reshape(dp_size, 2, count // 2 * width)
        place += count
        total_mods.append(part if l else jnp.concatenate([rest, part], axis=2))
    total_mods = jnp.stack(total_mods, axis=1)
    total_gains = jnp.sum(early[there, place : place + layers, : 4 * HEAD], axis=0)
    total_gains = total_gains.reshape(layers, 2, 2, HEAD)
    act_there = act_low.astype(F32)[there]
    ada_grad = jnp.einsum("nd,nlse->lsde", act_there, total_mods, precision=HIGHEST)
    d_act = jnp.einsum("nlse,lsde->nd", total_mods, ada_weight.astype(F32), precision=HIGHEST)
    condition_grad = silu_pull(d_act[there])[0]

    def pieces(kind, first):
        return jnp.stack([grads[l][kind][0][first : first + 2] for l in range(layers)]).astype(F32)

    qkv_grad = pieces(0, 0).reshape(layers, 2, rows, -1, 3, width_of_group)
    qkv_grad = qkv_grad.transpose(0, 1, 2, 4, 3, 5).reshape(qkv_weight.shape)
    return (
        outputs[0],
        outputs[1],
        gy[0][None],
        gy[1][None],
        condition_grad,
        ada_grad,
        qkv_grad,
        pieces(1, 0).transpose(0, 1, 3, 2),
        pieces(2, 0),
        pieces(2, 2).transpose(0, 1, 3, 2),
        total_gains,
    )


def solution(mesh):
    tokens = P("dp", "seq", None)
    placed = (
        tokens,
        tokens,
        P(None, ("dp", "seq")),
        P(None, None, ("dp", "seq"), None),
        P(None, None, "dp", None, "seq"),
        P(None, None, "seq", "dp"),
        P(None, None, "dp", "seq"),
        P(None, None, "seq", "dp"),
        P(),
        tokens,
        tokens,
    )
    results = (tokens, tokens, tokens, tokens) + placed[2:8] + (P(),)

    def step(*args):
        heads = args[4].shape[4] // mesh.shape["seq"] // HEAD
        group = 2 * HEAD if heads % 2 == 0 else HEAD
        body = functools.partial(
            on_device, ("dp", mesh.shape["dp"]), ("seq", mesh.shape["seq"]), group
        )
        return jax.shard_map(
            body, mesh=mesh, in_specs=placed, out_specs=results, check_vma=False
        )(*args)

    return step
```

```python
import functools

import jax
import jax.numpy as jnp
from jax import lax
from jax.experimental import pallas as pl
from jax.experimental.pallas import tpu as pltpu
from jax.sharding import PartitionSpec as P

EPSILON = 1e-06
HIGHEST = lax.Precision.HIGHEST
F32 = jnp.float32
BF16 = jnp.bfloat16
HEAD = 64


def layer_stats(values):
    centred = values - jnp.mean(values, axis=-1, keepdims=True)
    root = lax.rsqrt(jnp.mean(centred * centred, axis=-1, keepdims=True) + EPSILON)
    return centred * root, root


def modulate(values, shift, scale):
    return layer_stats(values)[0] * (1.0 + scale) + shift


def modulate_back(values, grad, scale):
    normed, root = layer_stats(values)
    inner = grad * (1.0 + scale)
    first = jnp.mean(inner, axis=-1, keepdims=True)
    second = jnp.mean(inner * normed, axis=-1, keepdims=True)
    d_values = root * (inner - first - normed * second)
    return d_values, jnp.sum(grad, axis=0), jnp.sum(grad * normed, axis=0)


def mm(left, right):
    return lax.dot_general(left, right, (((1,), (0,)), ((), ())), preferred_element_type=F32)


def mm_nt(left, right):
    return lax.dot_general(left, right, (((1,), (1,)), ((), ())), preferred_element_type=F32)


def mm_tn(left, right):
    return lax.dot_general(left, right, (((0,), (0,)), ((), ())), preferred_element_type=F32)


def gelu(values):
    return jax.nn.gelu(values, approximate=True)


def head_factors(raw_t, gain_image, gain_text, image_len):
    root = lax.rsqrt(jnp.mean(raw_t * raw_t, axis=0, keepdims=True) + EPSILON)
    lanes = lax.broadcasted_iota(jnp.int32, raw_t.shape, 1)
    gain = jnp.where(lanes < image_len, gain_image, gain_text)
    return raw_t * root, root, gain


def transposed(first, second, low, high):
    return jnp.concatenate(
        [first[:, low:high].astype(F32).T, second[:, low:high].astype(F32).T], axis=1
    )


def attention_forward_kernel(step, image_ref, text_ref, gain_ref, o_image, o_text, lse_ref, o_scr):
    image_len, text_len = image_ref.shape[0], text_ref.shape[0]
    total = image_len + text_len
    wide = image_ref.shape[1] // 3
    factor = HEAD ** (-0.5)
    raw_q = transposed(image_ref, text_ref, 0, wide)
    raw_k = transposed(image_ref, text_ref, wide, 2 * wide)
    values_t = transposed(image_ref, text_ref, 2 * wide, 3 * wide).astype(BF16)
    for head in range(wide // HEAD):
        rows = slice(head * HEAD, (head + 1) * HEAD)
        q_hat, _, q_gain = head_factors(raw_q[rows], gain_ref[:, 0:1], gain_ref[:, 1:2], image_len)
        k_hat, _, k_gain = head_factors(raw_k[rows], gain_ref[:, 2:3], gain_ref[:, 3:4], image_len)
        q_t = ((q_hat * q_gain).astype(BF16).astype(F32) * factor).astype(BF16)
        keys = (k_hat * k_gain).T.astype(BF16)
        v_t = values_t[rows]
        for start in range(0, total, step):
            part = slice(start, start + step)
            scores = mm(keys, q_t[:, part])
            largest = jnp.max(scores, axis=0, keepdims=True)
            weights = jnp.exp(scores - largest)
            total_w = jnp.sum(weights, axis=0, keepdims=True)
            out = mm(v_t, weights.astype(BF16)) * (1.0 / total_w)
            o_scr[rows, part] = out
            lse_ref[head, :, part] = largest + jnp.log(total_w)
    o_image[...] = o_scr[:, :image_len].T.astype(BF16)
    o_text[...] = o_scr[:, image_len:].T.astype(BF16)


def attention_backward_kernel(
    step,
    image_ref,
    text_ref,
    gain_ref,
    o_image,
    o_text,
    do_image,
    do_text,
    lse_ref,
    d_image,
    d_text,
    gain_grad,
    dq_scr,
    dk_scr,
    dv_scr,
):
    image_len, text_len = image_ref.shape[0], text_ref.shape[0]
    total = image_len + text_len
    wide = image_ref.shape[1] // 3
    factor = HEAD ** (-0.5)
    raw_q = transposed(image_ref, text_ref, 0, wide)
    raw_k = transposed(image_ref, text_ref, wide, 2 * wide)
    o_t = transposed(o_image, o_text, 0, wide)
    do_t = transposed(do_image, do_text, 0, wide)
    lane_row = lax.broadcasted_iota(jnp.int32, (HEAD, 128), 1)
    gains_total = jnp.zeros((HEAD, 128), F32)
    for head in range(wide // HEAD):
        rows = slice(head * HEAD, (head + 1) * HEAD)
        low, high = 2 * wide + head * HEAD, 2 * wide + (head + 1) * HEAD
        q_hat, q_root, q_gain = head_factors(
            raw_q[rows], gain_ref[:, 0:1], gain_ref[:, 1:2], image_len
        )
        k_hat, k_root, k_gain = head_factors(
            raw_k[rows], gain_ref[:, 2:3], gain_ref[:, 3:4], image_len
        )
        q_full = (q_hat * q_gain).astype(BF16).astype(F32) * factor
        q_t = q_full.astype(BF16)
        queries = q_full.T.astype(BF16)
        k_t = (k_hat * k_gain).astype(BF16)
        keys = (k_hat * k_gain).T.astype(BF16)
        values = jnp.concatenate([image_ref[:, low:high], text_ref[:, low:high]], axis=0)
        d_out = jnp.concatenate([do_image[:, rows], do_text[:, rows]], axis=0)
        delta = jnp.sum(do_t[rows] * o_t[rows], axis=0, keepdims=True)
        d_out_t = do_t[rows].astype(BF16)
        d_keys = jnp.zeros((total, HEAD), F32)
        d_values = jnp.zeros((total, HEAD), F32)
        for start in range(0, total, step):
            part = slice(start, start + step)
            weights = jnp.exp(mm(keys, q_t[:, part]) - lse_ref[head, :, part])
            d_weights = mm(values, d_out_t[:, part])
            d_scores = (weights * (d_weights - delta[:, part])).astype(BF16)
            d_values += mm(weights.astype(BF16), d_out[part])
            d_keys += mm(d_scores, queries[part])
            dq_scr[rows, part] = mm(k_t, d_scores) * factor
        dv_scr[:, rows] = d_values
        dq = dq_scr[rows, :]
        dk = d_keys.T
        for slot, (grad, hat) in enumerate(((dq, q_hat), (dk, k_hat))):
            product = grad * hat
            image_sum = jnp.sum(product[:, :image_len], axis=1, keepdims=True)
            text_sum = jnp.sum(product[:, image_len:], axis=1, keepdims=True)
            gains_total += jnp.where(lane_row == 2 * slot, image_sum, 0.0)
            gains_total += jnp.where(lane_row == 2 * slot + 1, text_sum, 0.0)
        scaled = dq * q_gain
        dq_scr[rows, :] = q_root * (
            scaled - q_hat * jnp.mean(scaled * q_hat, axis=0, keepdims=True)
        )
        scaled = dk * k_gain
        dk_scr[rows, :] = k_root * (
            scaled - k_hat * jnp.mean(scaled * k_hat, axis=0, keepdims=True)
        )
    d_image[:, :wide] = dq_scr[:, :image_len].T.astype(BF16)
    d_text[:, :wide] = dq_scr[:, image_len:].T.astype(BF16)
    d_image[:, wide : 2 * wide] = dk_scr[:, :image_len].T.astype(BF16)
    d_text[:, wide : 2 * wide] = dk_scr[:, image_len:].T.astype(BF16)
    d_image[:, 2 * wide :] = dv_scr[:image_len].astype(BF16)
    d_text[:, 2 * wide :] = dv_scr[image_len:].astype(BF16)
    gain_grad[0] = gains_total


def query_step(total):
    for count in (3, 4, 2, 6, 9, 1):
        if total % (count * 128) == 0:
            return total // count
    return total


def kernel_cost(tokens, heads, products):
    return pl.CostEstimate(
        flops=2 * products * heads * tokens * tokens * HEAD * 4,
        transcendentals=heads * tokens * tokens,
        bytes_accessed=tokens * heads * HEAD * 2 * 8,
    )


def attention_forward(raw_image, raw_text, gains):
    groups = raw_image.shape[1] // (3 * 128)
    image_len, text_len = raw_image.shape[0], raw_text.shape[0]
    total = image_len + text_len
    return pl.pallas_call(
        functools.partial(attention_forward_kernel, query_step(total)),
        grid=(groups,),
        out_shape=(
            jax.ShapeDtypeStruct((image_len, groups * 128), BF16),
            jax.ShapeDtypeStruct((text_len, groups * 128), BF16),
            jax.ShapeDtypeStruct((groups * 2, 1, total), F32),
        ),
        in_specs=[
            pl.BlockSpec((image_len, 384), lambda g: (0, g)),
            pl.BlockSpec((text_len, 384), lambda g: (0, g)),
            pl.BlockSpec((HEAD, 4), lambda g: (0, 0)),
        ],
        out_specs=(
            pl.BlockSpec((image_len, 128), lambda g: (0, g)),
            pl.BlockSpec((text_len, 128), lambda g: (0, g)),
            pl.BlockSpec((2, 1, total), lambda g: (g, 0, 0)),
        ),
        scratch_shapes=[pltpu.VMEM((128, total), F32)],
        cost_estimate=kernel_cost(total, groups * 2, 2),
        name="attend_forward",
    )(raw_image, raw_text, gains)


def attention_backward(raw_image, raw_text, gains, o_image, o_text, do_image, do_text, lse):
    groups = raw_image.shape[1] // (3 * 128)
    image_len, text_len = raw_image.shape[0], raw_text.shape[0]
    total = image_len + text_len
    wide_image = pl.BlockSpec((image_len, 384), lambda g: (0, g))
    wide_text = pl.BlockSpec((text_len, 384), lambda g: (0, g))
    slim_image = pl.BlockSpec((image_len, 128), lambda g: (0, g))
    slim_text = pl.BlockSpec((text_len, 128), lambda g: (0, g))
    d_image, d_text, gain_grad = pl.pallas_call(
        functools.partial(attention_backward_kernel, query_step(total)),
        grid=(groups,),
        out_shape=(
            jax.ShapeDtypeStruct(raw_image.shape, BF16),
            jax.ShapeDtypeStruct(raw_text.shape, BF16),
            jax.ShapeDtypeStruct((groups, HEAD, 128), F32),
        ),
        in_specs=[
            wide_image,
            wide_text,
            pl.BlockSpec((HEAD, 4), lambda g: (0, 0)),
            slim_image,
            slim_text,
            slim_image,
            slim_text,
            pl.BlockSpec((2, 1, total), lambda g: (g, 0, 0)),
        ],
        out_specs=(wide_image, wide_text, pl.BlockSpec((1, HEAD, 128), lambda g: (g, 0, 0))),
        scratch_shapes=[
            pltpu.VMEM((128, total), F32),
            pltpu.VMEM((128, total), F32),
            pltpu.VMEM((total, 128), F32),
        ],
        cost_estimate=kernel_cost(total, groups * 2, 5),
        name="attend_backward",
    )(raw_image, raw_text, gains, o_image, o_text, do_image, do_text, lse)
    return d_image, d_text, jnp.sum(gain_grad, axis=0)


def plain_parts(raw_image, raw_text, gains):
    raw = jnp.concatenate([raw_image, raw_text], axis=0).astype(F32)
    raw = raw.reshape(raw.shape[0], -1, 3, HEAD)
    is_image = (jnp.arange(raw.shape[0]) < raw_image.shape[0])[:, None, None]
    hats, roots, scales, rounded = [], [], [], []
    for slot in range(2):
        part = raw[:, :, slot]
        root = lax.rsqrt(jnp.mean(part * part, axis=-1, keepdims=True) + EPSILON)
        scale = jnp.where(is_image, gains[:, 2 * slot], gains[:, 2 * slot + 1])
        hats.append(part * root)
        roots.append(root)
        scales.append(scale)
        rounded.append((part * root * scale).astype(BF16))
    return hats, roots, scales, rounded, raw[:, :, 2].astype(BF16)


def plain_forward(raw_image, raw_text, gains):
    _, _, _, (queries, keys), values = plain_parts(raw_image, raw_text, gains)
    scores = jnp.einsum("qhd,khd->hqk", queries, keys, preferred_element_type=F32)
    scores = scores * HEAD ** (-0.5)
    largest = jnp.max(scores, axis=-1, keepdims=True)
    lse = largest + jnp.log(jnp.sum(jnp.exp(scores - largest), axis=-1, keepdims=True))
    weights = jnp.exp(scores - lse).astype(BF16)
    out = jnp.einsum("hqk,khd->qhd", weights, values, preferred_element_type=F32)
    out = out.astype(BF16).reshape(out.shape[0], -1)
    return out[: raw_image.shape[0]], out[raw_image.shape[0] :], lse


def plain_backward(raw_image, raw_text, gains, o_image, o_text, do_image, do_text, lse):
    hats, roots, scales, (queries, keys), values = plain_parts(raw_image, raw_text, gains)
    factor = HEAD ** (-0.5)
    image_len = raw_image.shape[0]
    d_out = jnp.concatenate([do_image, do_text], axis=0).reshape(queries.shape)
    scores = jnp.einsum("qhd,khd->hqk", queries, keys, preferred_element_type=F32) * factor
    weights = jnp.exp(scores - lse)
    d_weights = jnp.einsum("qhd,khd->hqk", d_out, values, preferred_element_type=F32)
    inner = jnp.sum(weights * d_weights, axis=-1, keepdims=True)
    d_scores = (weights * (d_weights - inner)).astype(BF16)
    dq = jnp.einsum("hqk,khd->qhd", d_scores, keys, preferred_element_type=F32) * factor
    dk = jnp.einsum("hqk,qhd->khd", d_scores, queries, preferred_element_type=F32) * factor
    dv = jnp.einsum("hqk,qhd->khd", weights.astype(BF16), d_out, preferred_element_type=F32)
    gain_rows, parts = [], []
    for grad, hat, root, scale in zip((dq, dk), hats, roots, scales):
        product = grad * hat
        gain_rows += [jnp.sum(product[:image_len], (0, 1)), jnp.sum(product[image_len:], (0, 1))]
        scaled = grad * scale
        parts.append(root * (scaled - hat * jnp.mean(scaled * hat, axis=-1, keepdims=True)))
    joined = jnp.stack(parts + [dv], axis=2).astype(BF16).reshape(d_out.shape[0], -1)
    return joined[:image_len], joined[image_len:], jnp.stack(gain_rows, axis=1)


def tie(*groups):
    return lax.optimization_barrier(groups)


class Side:
    def __init__(self, state=(), steps=(), finish=None):
        self.state, self.steps, self.finish = state, list(steps), finish
        self.running = False

    def open(self, token):
        if self.steps:
            token, self.state = tie(token, self.state)
            self.state = self.steps.pop(0)(self.state)
            self.running = True
        return token

    def close(self, token):
        if self.running:
            token, self.state = tie(token, self.state)
            self.running = False
        return token

    def result(self):
        while self.steps:
            self.state = self.steps.pop(0)(self.state)
        return self.finish(self.state)


def join_kernel(size, cut, me_ref, own, *refs):
    after, before = refs[: size - 1], refs[size - 1 : 2 * size - 2]
    image, text, sems = refs[2 * size - 2 :]
    tail = own.shape[0] - cut

    def copies(source, k):
        return (
            pltpu.make_async_copy(
                source.at[pl.ds(0, cut)], image.at[pl.ds(k * cut, cut)], sems.at[k, 0]
            ),
            pltpu.make_async_copy(
                source.at[pl.ds(cut, tail)], text.at[pl.ds(k * tail, tail)], sems.at[k, 1]
            ),
        )

    def start(source, k):
        for copy in copies(source, k):
            copy.start()

    start(own, 0)
    for k in range(1, size):
        from_after = me_ref[0] + k < size
        pl.when(from_after)(functools.partial(start, after[k - 1], k))
        pl.when(jnp.logical_not(from_after))(functools.partial(start, before[size - k - 1], k))
    for k in range(size):
        for copy in copies(own, k):
            copy.wait()


def join_tokens(own, after, before, me, cut):
    size, (rows, width) = len(after) + 1, own.shape
    return pl.pallas_call(
        functools.partial(join_kernel, size, cut),
        out_shape=(
            jax.ShapeDtypeStruct((size * cut, width), own.dtype),
            jax.ShapeDtypeStruct((size * (rows - cut), width), own.dtype),
        ),
        in_specs=[pl.BlockSpec(memory_space=pltpu.SMEM)]
        + [pl.BlockSpec(memory_space=pl.ANY)] * (2 * size - 1),
        out_specs=(
            pl.BlockSpec(memory_space=pltpu.VMEM),
            pl.BlockSpec(memory_space=pltpu.VMEM),
        ),
        scratch_shapes=[pltpu.SemaphoreType.DMA((size, 2))],
        compiler_params=pltpu.CompilerParams(vmem_limit_bytes=16 * 2**20),
        cost_estimate=pl.CostEstimate(
            flops=0, transcendentals=0, bytes_accessed=4 * size * own.size
        ),
        name="join_tokens",
    )(me.astype(jnp.int32)[None], own, *after, *before)


class Streams:
    def __init__(self, image_len, text_len, axis, size):
        self.lengths = (image_len, text_len)
        self.axis, self.size = axis, size

    def gather_side(self, pair):
        size = self.size

        def step(state):
            own, after, before = state
            down, up = (after[-1], before[-1]) if after else (own, own)
            down = lax.ppermute(down, self.axis, [(i, i - 1) for i in range(1, size)])
            up = lax.ppermute(up, self.axis, [(i, i + 1) for i in range(size - 1)])
            return own, after + (down,), before + (up,)

        def finish(state):
            return join_tokens(*state, lax.axis_index(self.axis), self.lengths[0])

        return Side((jnp.concatenate(pair, axis=0), (), ()), [step] * (size - 1), finish)

    def scatter_side(self, pair):
        size, (image_len, text_len) = self.size, self.lengths
        image, text = (part.astype(BF16) for part in pair)
        cut = (image_len + text_len) // 32 * 16
        firsts = tuple(image[k * image_len : k * image_len + cut] for k in range(size))
        seconds = tuple(
            jnp.concatenate(
                [
                    image[k * image_len + cut : (k + 1) * image_len],
                    text[k * text_len : (k + 1) * text_len],
                ],
                axis=0,
            )
            for k in range(size)
        )

        def step(index, state):
            return tuple(half_step(index, *half) for half in state)

        def half_step(index, blocks, sums):
            k = size - 1 - index
            send_up, send_down = blocks[k], blocks[size - k]
            if sums:
                send_up, send_down = (
                    (send.astype(F32) + value.astype(F32)).astype(BF16)
                    for send, value in zip((send_up, send_down), sums)
                )
            up = lax.ppermute(send_up, self.axis, [(i, i + 1) for i in range(index + 1)])
            down = lax.ppermute(send_down, self.axis, [(i, i - 1) for i in range(k, size)])
            return blocks, (up, down)

        def finish(state):
            first, second = (
                blocks[0].astype(F32) + up.astype(F32) + down.astype(F32)
                for blocks, (up, down) in state
            )
            return (
                jnp.concatenate([first, second[: image_len - cut]], axis=0),
                second[image_len - cut :],
            )

        steps = [functools.partial(step, index) for index in range(size - 1)]
        return Side(((firsts, ()), (seconds, ())), steps, finish)

    def gather(self, pair):
        return self.gather_side(pair).result()

    def scatter(self, pair):
        return self.scatter_side(pair).result()


def bit_order(size):
    bits = [b for b in range(size.bit_length() - 1)]
    masks = [0]
    for b in bits:
        masks += [m | (1 << b) for m in masks]
    return bits, masks


def swap_bit(value, axis, size, bit):
    return lax.ppermute(value, axis, [(i, i ^ (1 << bit)) for i in range(size)])


def bit_gather(own, axis, size):
    blocks = own[None]
    for b in bit_order(size)[0]:
        blocks = jnp.concatenate([blocks, swap_bit(blocks, axis, size, b)], axis=0)
    return blocks


def bit_scatter(parts, axis, size):
    me = lax.axis_index(axis)
    for b in reversed(bit_order(size)[0]):
        half = parts.shape[0] // 2
        upper = ((me >> b) & 1) == 1
        keep = jnp.where(upper, parts[half:], parts[:half])
        send = jnp.where(upper, parts[:half], parts[half:])
        parts = keep + swap_bit(send, axis, size, b)
    return parts[0]


def bit_sum(value, axis, size):
    for b in bit_order(size)[0]:
        value = value + swap_bit(value, axis, size, b)
    return value


def forward_layer(streams, x, mods, weights, gains, attend, plain, side, last):
    qkv, out_t, up, down_t = weights
    if plain is not None:
        normed = [
            (plain[s].astype(F32) * (1.0 + mods[s, 1]) + mods[s, 0]).astype(BF16)
            for s in range(2)
        ]
    else:
        normed = streams.gather(
            [modulate(x[s], mods[s, 0], mods[s, 1]).astype(BF16) for s in range(2)]
        )
    raw = side.open([mm(normed[s], qkv[s]).astype(BF16) for s in range(2)])
    o_image, o_text, lse = attend(raw[0], raw[1], gains)
    mixed = side.close((o_image, o_text))
    branch = streams.scatter([mm_nt(mixed[s], out_t[s]) for s in range(2)])
    middle = [x[s] + mods[s, 2] * branch[s] for s in range(2)]
    second = streams.gather(
        [modulate(middle[s], mods[s, 3], mods[s, 4]).astype(BF16) for s in range(2)]
    )
    second = side.open(second)
    hidden = [mm(second[s], up[s]) for s in range(2)]
    active = side.close([gelu(hidden[s]).astype(BF16) for s in range(2)])
    hidden = [hidden[s].astype(BF16) for s in range(2)]
    result = streams.scatter_side([mm_nt(active[s], down_t[s]) for s in range(2)])
    saved = (x, normed, raw, mixed, lse, branch, middle, second, hidden, active)
    if last:
        return None, saved, result
    result = result.result()
    return [middle[s] + mods[s, 5] * result[s] for s in range(2)], saved, result


def backward_layer(streams, gy, dm, saved, mods, weights, gains, calls, side, last):
    qkv, out_t, up, down_t = weights
    x, normed, raw, mixed, lse, branch, middle, second, hidden, active = saved
    if dm is None:
        dm = streams.gather([(mods[s, 5] * gy[s]).astype(BF16) for s in range(2)])
    dm = side.open(dm)
    du = []
    for s in range(2):
        _, pull = jax.vjp(gelu, hidden[s].astype(F32))
        du.append(pull(mm(dm[s], down_t[s]))[0].astype(BF16))
    d_second = side.close([mm_nt(du[s], up[s]).astype(BF16) for s in range(2)])
    d_second = streams.scatter_side(d_second)
    du = d_second.close(d_second.open(du))
    late = [mm_tn(second[s], du[s]) for s in range(2)]
    late += [mm_tn(dm[s], active[s]) for s in range(2)]
    reduced_mlp = calls.reduce_grad(jnp.stack([part.astype(BF16) for part in late]))
    d_second = calls.settle(d_second.result())
    d_middle, d_shift2, d_scale2 = [], [], []
    for s in range(2):
        inner, d_shift, d_scale = modulate_back(middle[s], d_second[s], mods[s, 4])
        d_middle.append(gy[s] + inner)
        d_shift2.append(d_shift)
        d_scale2.append(d_scale)
    d_gate1 = [jnp.sum(d_middle[s] * branch[s], axis=0) for s in range(2)]
    da = streams.gather([(mods[s, 2] * d_middle[s]).astype(BF16) for s in range(2)])
    d_mixed = side.open([mm(da[s], out_t[s]).astype(BF16) for s in range(2)])
    late = jnp.stack([mm_tn(da[s], mixed[s]).astype(BF16) for s in range(2)])
    reduced_out = calls.reduce_grad(late)
    d_image, d_text, gain_rows = calls.attend_back(
        raw[0], raw[1], gains, mixed[0], mixed[1], d_mixed[0], d_mixed[1], lse
    )
    d_raw = side.close((d_image, d_text))
    if last:
        late = jnp.stack([mm_tn(normed[s], d_raw[s]).astype(BF16) for s in range(2)])
        d_raw, late = tie(d_raw, late)
        d_first = [mm_nt(d_raw[s], qkv[s]).astype(BF16) for s in range(2)]
        d_first, reduced_mlp[0] = tie(d_first, reduced_mlp[0])
        d_first = streams.scatter_side(d_first)
    else:
        d_first = streams.scatter_side([mm_nt(d_raw[s], qkv[s]) for s in range(2)])
        d_raw = d_first.close(d_first.open(d_raw))
        late = jnp.stack([mm_tn(normed[s], d_raw[s]).astype(BF16) for s in range(2)])
    reduced_qkv = calls.reduce_grad(late)
    early = (d_gate1, d_shift2, d_scale2), gain_rows
    if last:
        d_first = calls.before_end(early, d_first)
    else:
        d_first = d_first.result()
    if not last:
        d_first, reduced_mlp[0] = tie(d_first, reduced_mlp[0])
        calls.pending = [reduced_qkv, reduced_out]
    gx, late = [], []
    for s in range(2):
        inner, d_shift, d_scale = modulate_back(x[s], d_first[s], mods[s, 1])
        gx.append(d_middle[s] + inner)
        late += [d_shift, d_scale]
    return gx, early, late, (reduced_qkv, reduced_out, reduced_mlp)


class Calls:
    def __init__(self, attend_back, dp_axis):
        self.attend_back, self.axis, self.pending = attend_back, dp_axis, []
        self.before_end = None

    def reduce_grad(self, grad):
        return [lax.psum_scatter(grad, self.axis, scatter_dimension=1, tiled=True)]

    def settle(self, token):
        for box in self.pending:
            token, box[0] = tie(token, box[0])
        self.pending = []
        return token


def on_device(dp, seq, width_of_group, *args):
    (
        image_in,
        text_input,
        condition,
        ada_weight,
        qkv_weight,
        out_weight,
        up_weight,
        down_weight,
        norm_gain,
        image_cotangent,
        text_cotangent,
    ) = args
    dp_axis, dp_size = dp
    seq_axis, seq_size = seq
    layers = qkv_weight.shape[0]
    width = image_in.shape[2]
    streams = Streams(image_in.shape[1], text_input.shape[1], seq_axis, seq_size)
    attend, attend_back = (
        (attention_forward, attention_backward)
        if width_of_group % 128 == 0
        else (plain_forward, plain_backward)
    )
    rows = qkv_weight.shape[2]

    def fetch(local):
        return lax.all_gather(local, dp_axis, axis=1, tiled=True)

    qkv_local = qkv_weight.reshape(layers, 2, rows, 3, -1, width_of_group)
    qkv_local = qkv_local.transpose(0, 1, 2, 4, 3, 5).reshape(layers, 2, rows, -1)
    out_local = out_weight.transpose(0, 1, 3, 2)
    down_local = down_weight.transpose(0, 1, 3, 2)
    weights = [
        tuple(fetch(w[l]) for w in (qkv_local, out_local, up_weight, down_local))
        for l in range(layers)
    ]

    act_cond, silu_pull = jax.vjp(jax.nn.silu, condition.astype(F32))
    act_low = act_cond.astype(BF16)
    partial_mods = jnp.einsum("nd,lsde->nlse", act_low, ada_weight, preferred_element_type=F32)
    own_mods = bit_scatter(partial_mods.reshape(dp_size, -1), dp_axis, dp_size)
    x = [image_in[0].astype(F32), text_input[0].astype(F32)]
    plain = streams.gather([layer_stats(part)[0].astype(BF16) for part in x])
    own_mods, plain = tie(own_mods, plain)
    own_mods = bit_sum(own_mods, seq_axis, seq_size).reshape(layers, 2, 6, width)
    gains_all = norm_gain.astype(F32)
    gain_columns = [gains_all[l].transpose(1, 0, 2).reshape(4, HEAD).T for l in range(layers)]

    gy = [image_cotangent[0].astype(F32), text_cotangent[0].astype(F32)]
    side = streams.gather_side(
        [(own_mods[layers - 1, s, 5] * gy[s]).astype(BF16) for s in range(2)]
    )
    saved_list, results = [], []
    for l in range(layers):
        x, saved, result = forward_layer(
            streams,
            x,
            own_mods[l],
            weights[l],
            gain_columns[l],
            attend,
            None if l else plain,
            side,
            l == layers - 1,
        )
        saved_list.append(saved)
        results.append(result)
    dm, side = side.result(), results[-1]

    def share(values):
        return bit_gather(bit_sum(values, seq_axis, seq_size), dp_axis, dp_size)

    gys, early_all, late_all = [None] * layers, [None] * layers, [None] * layers
    grads, ends = [None] * layers, {}

    def before_end(early, scatter):
        early_all[0] = early
        results[-1] = side.result()
        layer_rows = []
        for l in range(layers):
            d_gate2 = [jnp.sum(gys[l][s] * results[l][s], axis=0) for s in range(2)]
            d_gate1, d_shift2, d_scale2 = early_all[l][0]
            first = late_all[l] if l else [jnp.zeros_like(d_gate2[0])] * 4
            layer_rows.append(
                [
                    first[2 * s : 2 * s + 2] + [d_gate1[s], d_shift2[s], d_scale2[s], d_gate2[s]]
                    for s in range(2)
                ]
            )
        small = layer_rows, [early_all[l][1] for l in range(layers)]
        for _ in range(2):
            small = scatter.close(scatter.open(small))
        layer_rows, gain_rows = small
        rows = jnp.stack([jnp.stack([jnp.stack(r) for r in both]) for both in layer_rows])
        ends["early"] = share(rows), share(jnp.stack(gain_rows))
        return scatter.result()

    calls = Calls(attend_back, dp_axis)
    calls.before_end = before_end
    for l in reversed(range(layers)):
        gys[l] = gy
        gy, early_all[l], late_all[l], grads[l] = backward_layer(
            streams,
            gy,
            dm,
            saved_list[l],
            own_mods[l],
            weights[l],
            gain_columns[l],
            calls,
            side,
            l == 0,
        )
        dm = None
    last_middle = saved_list[-1][6]
    outputs = [
        (last_middle[s] + own_mods[layers - 1, s, 5] * results[-1][s]).astype(BF16)[None]
        for s in range(2)
    ]

    there = jnp.array(bit_order(dp_size)[1], jnp.int32) ^ lax.axis_index(dp_axis)
    late_all[0], grads[0] = tie(late_all[0], grads[0])
    rest = share(jnp.stack([jnp.stack(late_all[0][:2]), jnp.stack(late_all[0][2:])]))
    total_mods, total_gains = ends["early"]
    first = jnp.concatenate([rest, total_mods[:, 0, :, 2:]], axis=2)
    total_mods = jnp.concatenate([first[:, None], total_mods[:, 1:]], axis=1)
    total_mods = total_mods.reshape(dp_size, layers, 2, 6 * width)
    total_gains = jnp.sum(total_gains[there], axis=0)[:, :, :4]
    total_gains = total_gains.reshape(layers, HEAD, 2, 2).transpose(0, 3, 2, 1)
    act_there = act_low.astype(F32)[there]
    ada_grad = jnp.einsum("nd,nlse->lsde", act_there, total_mods, precision=HIGHEST)
    d_act = jnp.einsum("nlse,lsde->nd", total_mods, ada_weight.astype(F32), precision=HIGHEST)
    condition_grad = silu_pull(d_act[there])[0]

    def pieces(kind, first):
        return jnp.stack([grads[l][kind][0][first : first + 2] for l in range(layers)]).astype(F32)

    qkv_grad = pieces(0, 0).reshape(layers, 2, rows, -1, 3, width_of_group)
    qkv_grad = qkv_grad.transpose(0, 1, 2, 4, 3, 5).reshape(qkv_weight.shape)
    return (
        outputs[0],
        outputs[1],
        gy[0][None],
        gy[1][None],
        condition_grad,
        ada_grad,
        qkv_grad,
        pieces(1, 0).transpose(0, 1, 3, 2),
        pieces(2, 0),
        pieces(2, 2).transpose(0, 1, 3, 2),
        total_gains,
    )


def solution(mesh):
    tokens = P("dp", "seq", None)
    placed = (
        tokens,
        tokens,
        P(None, ("dp", "seq")),
        P(None, None, ("dp", "seq"), None),
        P(None, None, "dp", None, "seq"),
        P(None, None, "seq", "dp"),
        P(None, None, "dp", "seq"),
        P(None, None, "seq", "dp"),
        P(),
        tokens,
        tokens,
    )
    results = (tokens, tokens, tokens, tokens) + placed[2:8] + (P(),)

    def step(*args):
        heads = args[4].shape[4] // mesh.shape["seq"] // HEAD
        group = 2 * HEAD if heads % 2 == 0 else HEAD
        body = functools.partial(
            on_device, ("dp", mesh.shape["dp"]), ("seq", mesh.shape["seq"]), group
        )
        return jax.shard_map(
            body, mesh=mesh, in_specs=placed, out_specs=results, check_vma=False
        )(*args)

    return step
```

```python
import functools

import jax
import jax.numpy as jnp
from jax import lax
from jax.experimental import pallas as pl
from jax.experimental.pallas import tpu as pltpu
from jax.sharding import PartitionSpec as P

EPSILON = 1e-06
HIGHEST = lax.Precision.HIGHEST
F32 = jnp.float32
BF16 = jnp.bfloat16
HEAD = 64


def layer_stats(values):
    centred = values - jnp.mean(values, axis=-1, keepdims=True)
    root = lax.rsqrt(jnp.mean(centred * centred, axis=-1, keepdims=True) + EPSILON)
    return centred * root, root


def modulate(values, shift, scale):
    return layer_stats(values)[0] * (1.0 + scale) + shift


def modulate_back(values, grad, scale):
    normed, root = layer_stats(values)
    inner = grad * (1.0 + scale)
    first = jnp.mean(inner, axis=-1, keepdims=True)
    second = jnp.mean(inner * normed, axis=-1, keepdims=True)
    d_values = root * (inner - first - normed * second)
    return d_values, jnp.sum(grad, axis=0), jnp.sum(grad * normed, axis=0)


def mm(left, right):
    return lax.dot_general(left, right, (((1,), (0,)), ((), ())), preferred_element_type=F32)


def mm_nt(left, right):
    return lax.dot_general(left, right, (((1,), (1,)), ((), ())), preferred_element_type=F32)


def mm_tn(left, right):
    return lax.dot_general(left, right, (((0,), (0,)), ((), ())), preferred_element_type=F32)


def gelu(values):
    return jax.nn.gelu(values, approximate=True)


def head_factors(raw_t, gain_image, gain_text, image_len):
    root = lax.rsqrt(jnp.mean(raw_t * raw_t, axis=0, keepdims=True) + EPSILON)
    lanes = lax.broadcasted_iota(jnp.int32, raw_t.shape, 1)
    gain = jnp.where(lanes < image_len, gain_image, gain_text)
    return raw_t * root, root, gain


def transposed(first, second, low, high):
    return jnp.concatenate(
        [first[:, low:high].astype(F32).T, second[:, low:high].astype(F32).T], axis=1
    )


def attention_forward_kernel(step, image_ref, text_ref, gain_ref, o_image, o_text, lse_ref, o_scr):
    image_len, text_len = image_ref.shape[0], text_ref.shape[0]
    total = image_len + text_len
    wide = image_ref.shape[1] // 3
    factor = HEAD ** (-0.5)
    raw_q = transposed(image_ref, text_ref, 0, wide)
    raw_k = transposed(image_ref, text_ref, wide, 2 * wide)
    values_t = transposed(image_ref, text_ref, 2 * wide, 3 * wide).astype(BF16)
    for head in range(wide // HEAD):
        rows = slice(head * HEAD, (head + 1) * HEAD)
        q_hat, _, q_gain = head_factors(raw_q[rows], gain_ref[:, 0:1], gain_ref[:, 1:2], image_len)
        k_hat, _, k_gain = head_factors(raw_k[rows], gain_ref[:, 2:3], gain_ref[:, 3:4], image_len)
        q_t = ((q_hat * q_gain).astype(BF16).astype(F32) * factor).astype(BF16)
        keys = (k_hat * k_gain).T.astype(BF16)
        v_t = values_t[rows]
        for start in range(0, total, step):
            part = slice(start, start + step)
            scores = mm(keys, q_t[:, part])
            largest = jnp.max(scores, axis=0, keepdims=True)
            weights = jnp.exp(scores - largest)
            total_w = jnp.sum(weights, axis=0, keepdims=True)
            out = mm(v_t, weights.astype(BF16)) * (1.0 / total_w)
            o_scr[rows, part] = out
            lse_ref[head, :, part] = largest + jnp.log(total_w)
    o_image[...] = o_scr[:, :image_len].T.astype(BF16)
    o_text[...] = o_scr[:, image_len:].T.astype(BF16)


def attention_backward_kernel(
    step,
    image_ref,
    text_ref,
    gain_ref,
    o_image,
    o_text,
    do_image,
    do_text,
    lse_ref,
    d_image,
    d_text,
    gain_grad,
    dq_scr,
    dk_scr,
    dv_scr,
):
    image_len, text_len = image_ref.shape[0], text_ref.shape[0]
    total = image_len + text_len
    wide = image_ref.shape[1] // 3
    factor = HEAD ** (-0.5)
    raw_q = transposed(image_ref, text_ref, 0, wide)
    raw_k = transposed(image_ref, text_ref, wide, 2 * wide)
    o_t = transposed(o_image, o_text, 0, wide)
    do_t = transposed(do_image, do_text, 0, wide)
    lane_row = lax.broadcasted_iota(jnp.int32, (HEAD, 128), 1)
    gains_total = jnp.zeros((HEAD, 128), F32)
    for head in range(wide // HEAD):
        rows = slice(head * HEAD, (head + 1) * HEAD)
        low, high = 2 * wide + head * HEAD, 2 * wide + (head + 1) * HEAD
        q_hat, q_root, q_gain = head_factors(
            raw_q[rows], gain_ref[:, 0:1], gain_ref[:, 1:2], image_len
        )
        k_hat, k_root, k_gain = head_factors(
            raw_k[rows], gain_ref[:, 2:3], gain_ref[:, 3:4], image_len
        )
        q_full = (q_hat * q_gain).astype(BF16).astype(F32) * factor
        q_t = q_full.astype(BF16)
        queries = q_full.T.astype(BF16)
        k_t = (k_hat * k_gain).astype(BF16)
        keys = (k_hat * k_gain).T.astype(BF16)
        values = jnp.concatenate([image_ref[:, low:high], text_ref[:, low:high]], axis=0)
        d_out = jnp.concatenate([do_image[:, rows], do_text[:, rows]], axis=0)
        delta = jnp.sum(do_t[rows] * o_t[rows], axis=0, keepdims=True)
        d_out_t = do_t[rows].astype(BF16)
        d_keys = jnp.zeros((total, HEAD), F32)
        d_values = jnp.zeros((total, HEAD), F32)
        for start in range(0, total, step):
            part = slice(start, start + step)
            weights = jnp.exp(mm(keys, q_t[:, part]) - lse_ref[head, :, part])
            d_weights = mm(values, d_out_t[:, part])
            d_scores = (weights * (d_weights - delta[:, part])).astype(BF16)
            d_values += mm(weights.astype(BF16), d_out[part])
            d_keys += mm(d_scores, queries[part])
            dq_scr[rows, part] = mm(k_t, d_scores) * factor
        dv_scr[:, rows] = d_values
        dq = dq_scr[rows, :]
        dk = d_keys.T
        for slot, (grad, hat) in enumerate(((dq, q_hat), (dk, k_hat))):
            product = grad * hat
            image_sum = jnp.sum(product[:, :image_len], axis=1, keepdims=True)
            text_sum = jnp.sum(product[:, image_len:], axis=1, keepdims=True)
            gains_total += jnp.where(lane_row == 2 * slot, image_sum, 0.0)
            gains_total += jnp.where(lane_row == 2 * slot + 1, text_sum, 0.0)
        scaled = dq * q_gain
        dq_scr[rows, :] = q_root * (
            scaled - q_hat * jnp.mean(scaled * q_hat, axis=0, keepdims=True)
        )
        scaled = dk * k_gain
        dk_scr[rows, :] = k_root * (
            scaled - k_hat * jnp.mean(scaled * k_hat, axis=0, keepdims=True)
        )
    d_image[:, :wide] = dq_scr[:, :image_len].T.astype(BF16)
    d_text[:, :wide] = dq_scr[:, image_len:].T.astype(BF16)
    d_image[:, wide : 2 * wide] = dk_scr[:, :image_len].T.astype(BF16)
    d_text[:, wide : 2 * wide] = dk_scr[:, image_len:].T.astype(BF16)
    d_image[:, 2 * wide :] = dv_scr[:image_len].astype(BF16)
    d_text[:, 2 * wide :] = dv_scr[image_len:].astype(BF16)
    gain_grad[0] = gains_total


def query_step(total):
    for count in (3, 4, 2, 6, 9, 1):
        if total % (count * 128) == 0:
            return total // count
    return total


def kernel_cost(tokens, heads, products):
    return pl.CostEstimate(
        flops=2 * products * heads * tokens * tokens * HEAD * 4,
        transcendentals=heads * tokens * tokens,
        bytes_accessed=tokens * heads * HEAD * 2 * 8,
    )


def attention_forward(raw_image, raw_text, gains):
    groups = raw_image.shape[1] // (3 * 128)
    image_len, text_len = raw_image.shape[0], raw_text.shape[0]
    total = image_len + text_len
    return pl.pallas_call(
        functools.partial(attention_forward_kernel, query_step(total)),
        grid=(groups,),
        out_shape=(
            jax.ShapeDtypeStruct((image_len, groups * 128), BF16),
            jax.ShapeDtypeStruct((text_len, groups * 128), BF16),
            jax.ShapeDtypeStruct((groups * 2, 1, total), F32),
        ),
        in_specs=[
            pl.BlockSpec((image_len, 384), lambda g: (0, g)),
            pl.BlockSpec((text_len, 384), lambda g: (0, g)),
            pl.BlockSpec((HEAD, 4), lambda g: (0, 0)),
        ],
        out_specs=(
            pl.BlockSpec((image_len, 128), lambda g: (0, g)),
            pl.BlockSpec((text_len, 128), lambda g: (0, g)),
            pl.BlockSpec((2, 1, total), lambda g: (g, 0, 0)),
        ),
        scratch_shapes=[pltpu.VMEM((128, total), F32)],
        cost_estimate=kernel_cost(total, groups * 2, 2),
        name="attend_forward",
    )(raw_image, raw_text, gains)


def attention_backward(raw_image, raw_text, gains, o_image, o_text, do_image, do_text, lse):
    groups = raw_image.shape[1] // (3 * 128)
    image_len, text_len = raw_image.shape[0], raw_text.shape[0]
    total = image_len + text_len
    wide_image = pl.BlockSpec((image_len, 384), lambda g: (0, g))
    wide_text = pl.BlockSpec((text_len, 384), lambda g: (0, g))
    slim_image = pl.BlockSpec((image_len, 128), lambda g: (0, g))
    slim_text = pl.BlockSpec((text_len, 128), lambda g: (0, g))
    d_image, d_text, gain_grad = pl.pallas_call(
        functools.partial(attention_backward_kernel, query_step(total)),
        grid=(groups,),
        out_shape=(
            jax.ShapeDtypeStruct(raw_image.shape, BF16),
            jax.ShapeDtypeStruct(raw_text.shape, BF16),
            jax.ShapeDtypeStruct((groups, HEAD, 128), F32),
        ),
        in_specs=[
            wide_image,
            wide_text,
            pl.BlockSpec((HEAD, 4), lambda g: (0, 0)),
            slim_image,
            slim_text,
            slim_image,
            slim_text,
            pl.BlockSpec((2, 1, total), lambda g: (g, 0, 0)),
        ],
        out_specs=(wide_image, wide_text, pl.BlockSpec((1, HEAD, 128), lambda g: (g, 0, 0))),
        scratch_shapes=[
            pltpu.VMEM((128, total), F32),
            pltpu.VMEM((128, total), F32),
            pltpu.VMEM((total, 128), F32),
        ],
        cost_estimate=kernel_cost(total, groups * 2, 5),
        name="attend_backward",
    )(raw_image, raw_text, gains, o_image, o_text, do_image, do_text, lse)
    return d_image, d_text, jnp.sum(gain_grad, axis=0)


def plain_parts(raw_image, raw_text, gains):
    raw = jnp.concatenate([raw_image, raw_text], axis=0).astype(F32)
    raw = raw.reshape(raw.shape[0], -1, 3, HEAD)
    is_image = (jnp.arange(raw.shape[0]) < raw_image.shape[0])[:, None, None]
    hats, roots, scales, rounded = [], [], [], []
    for slot in range(2):
        part = raw[:, :, slot]
        root = lax.rsqrt(jnp.mean(part * part, axis=-1, keepdims=True) + EPSILON)
        scale = jnp.where(is_image, gains[:, 2 * slot], gains[:, 2 * slot + 1])
        hats.append(part * root)
        roots.append(root)
        scales.append(scale)
        rounded.append((part * root * scale).astype(BF16))
    return hats, roots, scales, rounded, raw[:, :, 2].astype(BF16)


def plain_forward(raw_image, raw_text, gains):
    _, _, _, (queries, keys), values = plain_parts(raw_image, raw_text, gains)
    scores = jnp.einsum("qhd,khd->hqk", queries, keys, preferred_element_type=F32)
    scores = scores * HEAD ** (-0.5)
    largest = jnp.max(scores, axis=-1, keepdims=True)
    lse = largest + jnp.log(jnp.sum(jnp.exp(scores - largest), axis=-1, keepdims=True))
    weights = jnp.exp(scores - lse).astype(BF16)
    out = jnp.einsum("hqk,khd->qhd", weights, values, preferred_element_type=F32)
    out = out.astype(BF16).reshape(out.shape[0], -1)
    return out[: raw_image.shape[0]], out[raw_image.shape[0] :], lse


def plain_backward(raw_image, raw_text, gains, o_image, o_text, do_image, do_text, lse):
    hats, roots, scales, (queries, keys), values = plain_parts(raw_image, raw_text, gains)
    factor = HEAD ** (-0.5)
    image_len = raw_image.shape[0]
    d_out = jnp.concatenate([do_image, do_text], axis=0).reshape(queries.shape)
    scores = jnp.einsum("qhd,khd->hqk", queries, keys, preferred_element_type=F32) * factor
    weights = jnp.exp(scores - lse)
    d_weights = jnp.einsum("qhd,khd->hqk", d_out, values, preferred_element_type=F32)
    inner = jnp.sum(weights * d_weights, axis=-1, keepdims=True)
    d_scores = (weights * (d_weights - inner)).astype(BF16)
    dq = jnp.einsum("hqk,khd->qhd", d_scores, keys, preferred_element_type=F32) * factor
    dk = jnp.einsum("hqk,qhd->khd", d_scores, queries, preferred_element_type=F32) * factor
    dv = jnp.einsum("hqk,qhd->khd", weights.astype(BF16), d_out, preferred_element_type=F32)
    gain_rows, parts = [], []
    for grad, hat, root, scale in zip((dq, dk), hats, roots, scales):
        product = grad * hat
        gain_rows += [jnp.sum(product[:image_len], (0, 1)), jnp.sum(product[image_len:], (0, 1))]
        scaled = grad * scale
        parts.append(root * (scaled - hat * jnp.mean(scaled * hat, axis=-1, keepdims=True)))
    joined = jnp.stack(parts + [dv], axis=2).astype(BF16).reshape(d_out.shape[0], -1)
    return joined[:image_len], joined[image_len:], jnp.stack(gain_rows, axis=1)


def tie(*groups):
    return lax.optimization_barrier(groups)


class Side:
    def __init__(self, state=(), steps=(), finish=None):
        self.state, self.steps, self.finish = state, list(steps), finish
        self.running = False

    def open(self, token):
        if self.steps:
            token, self.state = tie(token, self.state)
            self.state = self.steps.pop(0)(self.state)
            self.running = True
        return token

    def close(self, token):
        if self.running:
            token, self.state = tie(token, self.state)
            self.running = False
        return token

    def result(self):
        while self.steps:
            self.state = self.steps.pop(0)(self.state)
        return self.finish(self.state)


def join_kernel(size, cut, me_ref, own, *refs):
    after, before = refs[: size - 1], refs[size - 1 : 2 * size - 2]
    image, text, sems = refs[2 * size - 2 :]
    tail = own.shape[0] - cut

    def copies(source, k):
        return (
            pltpu.make_async_copy(
                source.at[pl.ds(0, cut)], image.at[pl.ds(k * cut, cut)], sems.at[k, 0]
            ),
            pltpu.make_async_copy(
                source.at[pl.ds(cut, tail)], text.at[pl.ds(k * tail, tail)], sems.at[k, 1]
            ),
        )

    def start(source, k):
        for copy in copies(source, k):
            copy.start()

    start(own, 0)
    for k in range(1, size):
        from_after = me_ref[0] + k < size
        pl.when(from_after)(functools.partial(start, after[k - 1], k))
        pl.when(jnp.logical_not(from_after))(functools.partial(start, before[size - k - 1], k))
    for k in range(size):
        for copy in copies(own, k):
            copy.wait()


def join_tokens(own, after, before, me, cut):
    size, (rows, width) = len(after) + 1, own.shape
    return pl.pallas_call(
        functools.partial(join_kernel, size, cut),
        out_shape=(
            jax.ShapeDtypeStruct((size * cut, width), own.dtype),
            jax.ShapeDtypeStruct((size * (rows - cut), width), own.dtype),
        ),
        in_specs=[pl.BlockSpec(memory_space=pltpu.SMEM)]
        + [pl.BlockSpec(memory_space=pl.ANY)] * (2 * size - 1),
        out_specs=(
            pl.BlockSpec(memory_space=pltpu.VMEM),
            pl.BlockSpec(memory_space=pltpu.VMEM),
        ),
        scratch_shapes=[pltpu.SemaphoreType.DMA((size, 2))],
        compiler_params=pltpu.CompilerParams(vmem_limit_bytes=16 * 2**20),
        cost_estimate=pl.CostEstimate(
            flops=0, transcendentals=0, bytes_accessed=4 * size * own.size
        ),
        name="join_tokens",
    )(me.astype(jnp.int32)[None], own, *after, *before)


class Streams:
    def __init__(self, image_len, text_len, axis, size):
        self.lengths = (image_len, text_len)
        self.axis, self.size = axis, size

    def gather_side(self, pair):
        size = self.size

        def step(state):
            own, after, before = state
            down, up = (after[-1], before[-1]) if after else (own, own)
            down = lax.ppermute(down, self.axis, [(i, i - 1) for i in range(1, size)])
            up = lax.ppermute(up, self.axis, [(i, i + 1) for i in range(size - 1)])
            return own, after + (down,), before + (up,)

        def finish(state):
            return join_tokens(*state, lax.axis_index(self.axis), self.lengths[0])

        return Side((jnp.concatenate(pair, axis=0), (), ()), [step] * (size - 1), finish)

    def scatter_side(self, pair):
        size, (image_len, text_len) = self.size, self.lengths
        image, text = (part.astype(BF16) for part in pair)
        cut = (image_len + text_len) // 32 * 16
        firsts = tuple(image[k * image_len : k * image_len + cut] for k in range(size))
        seconds = tuple(
            jnp.concatenate(
                [
                    image[k * image_len + cut : (k + 1) * image_len],
                    text[k * text_len : (k + 1) * text_len],
                ],
                axis=0,
            )
            for k in range(size)
        )

        def step(index, state):
            return tuple(half_step(index, *half) for half in state)

        def half_step(index, blocks, sums):
            k = size - 1 - index
            send_up, send_down = blocks[k], blocks[size - k]
            if sums:
                send_up, send_down = (
                    (send.astype(F32) + value.astype(F32)).astype(BF16)
                    for send, value in zip((send_up, send_down), sums)
                )
            up = lax.ppermute(send_up, self.axis, [(i, i + 1) for i in range(index + 1)])
            down = lax.ppermute(send_down, self.axis, [(i, i - 1) for i in range(k, size)])
            return blocks, (up, down)

        def finish(state):
            first, second = (
                blocks[0].astype(F32) + up.astype(F32) + down.astype(F32)
                for blocks, (up, down) in state
            )
            return (
                jnp.concatenate([first, second[: image_len - cut]], axis=0),
                second[image_len - cut :],
            )

        steps = [functools.partial(step, index) for index in range(size - 1)]
        return Side(((firsts, ()), (seconds, ())), steps, finish)

    def gather(self, pair):
        return self.gather_side(pair).result()

    def scatter(self, pair):
        return self.scatter_side(pair).result()


def bit_order(size):
    bits = [b for b in range(size.bit_length() - 1)]
    masks = [0]
    for b in bits:
        masks += [m | (1 << b) for m in masks]
    return bits, masks


def swap_bit(value, axis, size, bit):
    return lax.ppermute(value, axis, [(i, i ^ (1 << bit)) for i in range(size)])


def bit_gather(own, axis, size):
    blocks = own[None]
    for b in bit_order(size)[0]:
        blocks = jnp.concatenate([blocks, swap_bit(blocks, axis, size, b)], axis=0)
    return blocks


def bit_scatter(parts, axis, size, after_first):
    me = lax.axis_index(axis)
    for b in reversed(bit_order(size)[0]):
        half = parts.shape[0] // 2
        upper = ((me >> b) & 1) == 1
        keep = jnp.where(upper, parts[half:], parts[:half])
        send = jnp.where(upper, parts[:half], parts[half:])
        parts = keep + swap_bit(send, axis, size, b)
        if after_first is not None:
            parts, after_first = after_first(parts), None
    return parts[0]


def bit_sum(value, axis, size):
    for b in bit_order(size)[0]:
        value = value + swap_bit(value, axis, size, b)
    return value


def forward_layer(streams, x, mods, weights, gains, attend, plain, side, last):
    qkv, out_t, up, down_t = weights
    if plain is not None:
        normed = [
            (plain[s].astype(F32) * (1.0 + mods[s, 1]) + mods[s, 0]).astype(BF16)
            for s in range(2)
        ]
    else:
        normed = streams.gather(
            [modulate(x[s], mods[s, 0], mods[s, 1]).astype(BF16) for s in range(2)]
        )
    raw = side.open([mm(normed[s], qkv[s]).astype(BF16) for s in range(2)])
    o_image, o_text, lse = attend(raw[0], raw[1], gains)
    mixed = side.close((o_image, o_text))
    branch = streams.scatter([mm_nt(mixed[s], out_t[s]) for s in range(2)])
    middle = [x[s] + mods[s, 2] * branch[s] for s in range(2)]
    second = streams.gather(
        [modulate(middle[s], mods[s, 3], mods[s, 4]).astype(BF16) for s in range(2)]
    )
    second = side.open(second)
    hidden = [mm(second[s], up[s]) for s in range(2)]
    active = side.close([gelu(hidden[s]).astype(BF16) for s in range(2)])
    hidden = [hidden[s].astype(BF16) for s in range(2)]
    result = streams.scatter_side([mm_nt(active[s], down_t[s]) for s in range(2)])
    saved = (x, normed, raw, mixed, lse, branch, middle, second, hidden, active)
    if last:
        return None, saved, result
    result = result.result()
    return [middle[s] + mods[s, 5] * result[s] for s in range(2)], saved, result


def backward_layer(streams, gy, dm, saved, mods, weights, gains, calls, side, last):
    qkv, out_t, up, down_t = weights
    x, normed, raw, mixed, lse, branch, middle, second, hidden, active = saved
    if dm is None:
        dm = streams.gather([(mods[s, 5] * gy[s]).astype(BF16) for s in range(2)])
    dm = side.open(dm)
    du = []
    for s in range(2):
        _, pull = jax.vjp(gelu, hidden[s].astype(F32))
        du.append(pull(mm(dm[s], down_t[s]))[0].astype(BF16))
    d_second = side.close([mm_nt(du[s], up[s]).astype(BF16) for s in range(2)])
    d_second = streams.scatter_side(d_second)
    du = d_second.close(d_second.open(du))
    late = [mm_tn(second[s], du[s]) for s in range(2)]
    late += [mm_tn(dm[s], active[s]) for s in range(2)]
    reduced_mlp = calls.reduce_grad(jnp.stack([part.astype(BF16) for part in late]))
    d_second = calls.settle(d_second.result())
    d_middle, d_shift2, d_scale2 = [], [], []
    for s in range(2):
        inner, d_shift, d_scale = modulate_back(middle[s], d_second[s], mods[s, 4])
        d_middle.append(gy[s] + inner)
        d_shift2.append(d_shift)
        d_scale2.append(d_scale)
    d_gate1 = [jnp.sum(d_middle[s] * branch[s], axis=0) for s in range(2)]
    da = streams.gather_side([(mods[s, 2] * d_middle[s]).astype(BF16) for s in range(2)])
    early = d_gate1, d_shift2, d_scale2
    if last:
        da = calls.before_end(early, da)
    else:
        da = da.result()
    d_mixed = side.open([mm(da[s], out_t[s]).astype(BF16) for s in range(2)])
    late = jnp.stack([mm_tn(da[s], mixed[s]).astype(BF16) for s in range(2)])
    reduced_out = calls.reduce_grad(late)
    d_image, d_text, gain_rows = calls.attend_back(
        raw[0], raw[1], gains, mixed[0], mixed[1], d_mixed[0], d_mixed[1], lse
    )
    d_raw = side.close((d_image, d_text))
    if last:
        late = jnp.stack([mm_tn(normed[s], d_raw[s]).astype(BF16) for s in range(2)])
        d_raw, late = tie(d_raw, late)
        d_first = [mm_nt(d_raw[s], qkv[s]).astype(BF16) for s in range(2)]
        d_first, reduced_mlp[0] = tie(d_first, reduced_mlp[0])
        d_first = streams.scatter_side(d_first)
    else:
        d_first = streams.scatter_side([mm_nt(d_raw[s], qkv[s]) for s in range(2)])
        d_raw = d_first.close(d_first.open(d_raw))
        late = jnp.stack([mm_tn(normed[s], d_raw[s]).astype(BF16) for s in range(2)])
    reduced_qkv = calls.reduce_grad(late)
    if last:
        for _ in range(2):
            calls.shared = d_first.close(d_first.open(calls.shared))
    d_first = d_first.result()
    if not last:
        d_first, reduced_mlp[0] = tie(d_first, reduced_mlp[0])
        calls.pending = [reduced_qkv, reduced_out]
    gx, late = [], []
    for s in range(2):
        inner, d_shift, d_scale = modulate_back(x[s], d_first[s], mods[s, 1])
        gx.append(d_middle[s] + inner)
        late += [d_shift, d_scale]
    return gx, early, gain_rows, late, (reduced_qkv, reduced_out, reduced_mlp)


class Calls:
    def __init__(self, attend_back, dp_axis):
        self.attend_back, self.axis, self.pending = attend_back, dp_axis, []
        self.before_end = self.shared = None

    def reduce_grad(self, grad):
        return [lax.psum_scatter(grad, self.axis, scatter_dimension=1, tiled=True)]

    def settle(self, token):
        for box in self.pending:
            token, box[0] = tie(token, box[0])
        self.pending = []
        return token


def on_device(dp, seq, width_of_group, *args):
    (
        image_in,
        text_input,
        condition,
        ada_weight,
        qkv_weight,
        out_weight,
        up_weight,
        down_weight,
        norm_gain,
        image_cotangent,
        text_cotangent,
    ) = args
    dp_axis, dp_size = dp
    seq_axis, seq_size = seq
    layers = qkv_weight.shape[0]
    width = image_in.shape[2]
    streams = Streams(image_in.shape[1], text_input.shape[1], seq_axis, seq_size)
    attend, attend_back = (
        (attention_forward, attention_backward)
        if width_of_group % 128 == 0
        else (plain_forward, plain_backward)
    )
    rows = qkv_weight.shape[2]

    def fetch(local):
        return lax.all_gather(local, dp_axis, axis=1, tiled=True)

    qkv_local = qkv_weight.reshape(layers, 2, rows, 3, -1, width_of_group)
    qkv_local = qkv_local.transpose(0, 1, 2, 4, 3, 5).reshape(layers, 2, rows, -1)
    out_local = out_weight.transpose(0, 1, 3, 2)
    down_local = down_weight.transpose(0, 1, 3, 2)
    weights = [
        tuple(fetch(w[l]) for w in (qkv_local, out_local, up_weight, down_local))
        for l in range(layers)
    ]

    act_cond, silu_pull = jax.vjp(jax.nn.silu, condition.astype(F32))
    act_low = act_cond.astype(BF16)
    partial_mods = jnp.einsum("nd,lsde->nlse", act_low, ada_weight, preferred_element_type=F32)
    x = [image_in[0].astype(F32), text_input[0].astype(F32)]
    plain = streams.gather_side([layer_stats(part)[0].astype(BF16) for part in x])
    plain.state = plain.steps.pop(0)(plain.state)

    def beside_tokens(parts):
        parts, plain.state = tie(parts, plain.state)
        return parts

    own_mods = partial_mods.reshape(dp_size, -1)
    own_mods = bit_scatter(own_mods, dp_axis, dp_size, beside_tokens)
    plain = plain.result()
    own_mods, plain = tie(own_mods, plain)
    own_mods = bit_sum(own_mods, seq_axis, seq_size).reshape(layers, 2, 6, width)
    gains_all = norm_gain.astype(F32)
    gain_columns = [gains_all[l].transpose(1, 0, 2).reshape(4, HEAD).T for l in range(layers)]

    gy = [image_cotangent[0].astype(F32), text_cotangent[0].astype(F32)]
    side = streams.gather_side(
        [(own_mods[layers - 1, s, 5] * gy[s]).astype(BF16) for s in range(2)]
    )
    saved_list, results = [], []
    for l in range(layers):
        x, saved, result = forward_layer(
            streams,
            x,
            own_mods[l],
            weights[l],
            gain_columns[l],
            attend,
            None if l else plain,
            side,
            l == layers - 1,
        )
        saved_list.append(saved)
        results.append(result)
    dm, side = side.result(), results[-1]

    def share(values):
        return bit_gather(bit_sum(values, seq_axis, seq_size), dp_axis, dp_size)

    gys, early_all, late_all = [None] * layers, [None] * layers, [None] * layers
    grads, gain_all = [None] * layers, [None] * layers

    def before_end(early, gather):
        early_all[0] = early
        results[-1] = side.result()
        layer_rows = []
        for l in range(layers):
            d_gate2 = [jnp.sum(gys[l][s] * results[l][s], axis=0) for s in range(2)]
            d_gate1, d_shift2, d_scale2 = early_all[l]
            first = late_all[l] if l else [jnp.zeros_like(d_gate2[0])] * 4
            layer_rows.append(
                [
                    first[2 * s : 2 * s + 2] + [d_gate1[s], d_shift2[s], d_scale2[s], d_gate2[s]]
                    for s in range(2)
                ]
            )
        layer_rows = gather.close(gather.open(layer_rows))
        rows = jnp.stack([jnp.stack([jnp.stack(r) for r in both]) for both in layer_rows])
        token, calls.shared = tie(gather.result(), rows)
        return token

    calls = Calls(attend_back, dp_axis)
    calls.before_end = before_end
    for l in reversed(range(layers)):
        gys[l] = gy
        gy, early_all[l], gain_all[l], late_all[l], grads[l] = backward_layer(
            streams,
            gy,
            dm,
            saved_list[l],
            own_mods[l],
            weights[l],
            gain_columns[l],
            calls,
            side,
            l == 0,
        )
        dm = None
    last_middle = saved_list[-1][6]
    outputs = [
        (last_middle[s] + own_mods[layers - 1, s, 5] * results[-1][s]).astype(BF16)[None]
        for s in range(2)
    ]

    there = jnp.array(bit_order(dp_size)[1], jnp.int32) ^ lax.axis_index(dp_axis)
    late_all[0], grads[0], gain_all = tie(late_all[0], grads[0], gain_all)
    rest = share(jnp.stack([jnp.stack(late_all[0][:2]), jnp.stack(late_all[0][2:])]))
    total_mods, total_gains = share(calls.shared), share(jnp.stack(gain_all))
    first = jnp.concatenate([rest, total_mods[:, 0, :, 2:]], axis=2)
    total_mods = jnp.concatenate([first[:, None], total_mods[:, 1:]], axis=1)
    total_mods = total_mods.reshape(dp_size, layers, 2, 6 * width)
    total_gains = jnp.sum(total_gains[there], axis=0)[:, :, :4]
    total_gains = total_gains.reshape(layers, HEAD, 2, 2).transpose(0, 3, 2, 1)
    act_there = act_low.astype(F32)[there]
    ada_grad = jnp.einsum("nd,nlse->lsde", act_there, total_mods, precision=HIGHEST)
    d_act = jnp.einsum("nlse,lsde->nd", total_mods, ada_weight.astype(F32), precision=HIGHEST)
    condition_grad = silu_pull(d_act[there])[0]

    def pieces(kind, first):
        return jnp.stack([grads[l][kind][0][first : first + 2] for l in range(layers)]).astype(F32)

    qkv_grad = pieces(0, 0).reshape(layers, 2, rows, -1, 3, width_of_group)
    qkv_grad = qkv_grad.transpose(0, 1, 2, 4, 3, 5).reshape(qkv_weight.shape)
    return (
        outputs[0],
        outputs[1],
        gy[0][None],
        gy[1][None],
        condition_grad,
        ada_grad,
        qkv_grad,
        pieces(1, 0).transpose(0, 1, 3, 2),
        pieces(2, 0),
        pieces(2, 2).transpose(0, 1, 3, 2),
        total_gains,
    )


def solution(mesh):
    tokens = P("dp", "seq", None)
    placed = (
        tokens,
        tokens,
        P(None, ("dp", "seq")),
        P(None, None, ("dp", "seq"), None),
        P(None, None, "dp", None, "seq"),
        P(None, None, "seq", "dp"),
        P(None, None, "dp", "seq"),
        P(None, None, "seq", "dp"),
        P(),
        tokens,
        tokens,
    )
    results = (tokens, tokens, tokens, tokens) + placed[2:8] + (P(),)

    def step(*args):
        heads = args[4].shape[4] // mesh.shape["seq"] // HEAD
        group = 2 * HEAD if heads % 2 == 0 else HEAD
        body = functools.partial(
            on_device, ("dp", mesh.shape["dp"]), ("seq", mesh.shape["seq"]), group
        )
        return jax.shard_map(
            body, mesh=mesh, in_specs=placed, out_specs=results, check_vma=False
        )(*args)

    return step
```

```python
import functools

import jax
import jax.numpy as jnp
from jax import lax
from jax.experimental import pallas as pl
from jax.experimental.pallas import tpu as pltpu
from jax.sharding import PartitionSpec as P

EPSILON = 1e-06
HIGHEST = lax.Precision.HIGHEST
F32 = jnp.float32
BF16 = jnp.bfloat16
HEAD = 64


def layer_stats(values):
    centred = values - jnp.mean(values, axis=-1, keepdims=True)
    root = lax.rsqrt(jnp.mean(centred * centred, axis=-1, keepdims=True) + EPSILON)
    return centred * root, root


def modulate(values, shift, scale):
    return layer_stats(values)[0] * (1.0 + scale) + shift


def modulate_back(values, grad, scale):
    normed, root = layer_stats(values)
    inner = grad * (1.0 + scale)
    first = jnp.mean(inner, axis=-1, keepdims=True)
    second = jnp.mean(inner * normed, axis=-1, keepdims=True)
    d_values = root * (inner - first - normed * second)
    return d_values, jnp.sum(grad, axis=0), jnp.sum(grad * normed, axis=0)


def mm(left, right):
    return lax.dot_general(left, right, (((1,), (0,)), ((), ())), preferred_element_type=F32)


def mm_nt(left, right):
    return lax.dot_general(left, right, (((1,), (1,)), ((), ())), preferred_element_type=F32)


def mm_tn(left, right):
    return lax.dot_general(left, right, (((0,), (0,)), ((), ())), preferred_element_type=F32)


def gelu(values):
    return jax.nn.gelu(values, approximate=True)


def head_factors(raw_t, gain_image, gain_text, image_len):
    root = lax.rsqrt(jnp.mean(raw_t * raw_t, axis=0, keepdims=True) + EPSILON)
    lanes = lax.broadcasted_iota(jnp.int32, raw_t.shape, 1)
    gain = jnp.where(lanes < image_len, gain_image, gain_text)
    return raw_t * root, root, gain


def transposed(first, second, low, high):
    return jnp.concatenate(
        [first[:, low:high].astype(F32).T, second[:, low:high].astype(F32).T], axis=1
    )


def attention_forward_kernel(step, image_ref, text_ref, gain_ref, o_image, o_text, lse_ref, o_scr):
    image_len, text_len = image_ref.shape[0], text_ref.shape[0]
    total = image_len + text_len
    wide = image_ref.shape[1] // 3
    factor = HEAD ** (-0.5)
    raw_q = transposed(image_ref, text_ref, 0, wide)
    raw_k = transposed(image_ref, text_ref, wide, 2 * wide)
    values_t = transposed(image_ref, text_ref, 2 * wide, 3 * wide).astype(BF16)
    for head in range(wide // HEAD):
        rows = slice(head * HEAD, (head + 1) * HEAD)
        q_hat, _, q_gain = head_factors(raw_q[rows], gain_ref[:, 0:1], gain_ref[:, 1:2], image_len)
        k_hat, _, k_gain = head_factors(raw_k[rows], gain_ref[:, 2:3], gain_ref[:, 3:4], image_len)
        q_t = ((q_hat * q_gain).astype(BF16).astype(F32) * factor).astype(BF16)
        keys = (k_hat * k_gain).T.astype(BF16)
        v_t = values_t[rows]
        for start in range(0, total, step):
            part = slice(start, start + step)
            scores = mm(keys, q_t[:, part])
            largest = jnp.max(scores, axis=0, keepdims=True)
            weights = jnp.exp(scores - largest)
            total_w = jnp.sum(weights, axis=0, keepdims=True)
            out = mm(v_t, weights.astype(BF16)) * (1.0 / total_w)
            o_scr[rows, part] = out
            lse_ref[head, :, part] = largest + jnp.log(total_w)
    o_image[...] = o_scr[:, :image_len].T.astype(BF16)
    o_text[...] = o_scr[:, image_len:].T.astype(BF16)


def attention_backward_kernel(
    step,
    image_ref,
    text_ref,
    gain_ref,
    o_image,
    o_text,
    do_image,
    do_text,
    lse_ref,
    d_image,
    d_text,
    gain_grad,
    dq_scr,
    dk_scr,
    dv_scr,
):
    image_len, text_len = image_ref.shape[0], text_ref.shape[0]
    total = image_len + text_len
    wide = image_ref.shape[1] // 3
    factor = HEAD ** (-0.5)
    raw_q = transposed(image_ref, text_ref, 0, wide)
    raw_k = transposed(image_ref, text_ref, wide, 2 * wide)
    o_t = transposed(o_image, o_text, 0, wide)
    do_t = transposed(do_image, do_text, 0, wide)
    lane_row = lax.broadcasted_iota(jnp.int32, (HEAD, 128), 1)
    gains_total = jnp.zeros((HEAD, 128), F32)
    for head in range(wide // HEAD):
        rows = slice(head * HEAD, (head + 1) * HEAD)
        low, high = 2 * wide + head * HEAD, 2 * wide + (head + 1) * HEAD
        q_hat, q_root, q_gain = head_factors(
            raw_q[rows], gain_ref[:, 0:1], gain_ref[:, 1:2], image_len
        )
        k_hat, k_root, k_gain = head_factors(
            raw_k[rows], gain_ref[:, 2:3], gain_ref[:, 3:4], image_len
        )
        q_full = (q_hat * q_gain).astype(BF16).astype(F32) * factor
        q_t = q_full.astype(BF16)
        queries = q_full.T.astype(BF16)
        k_t = (k_hat * k_gain).astype(BF16)
        keys = (k_hat * k_gain).T.astype(BF16)
        values = jnp.concatenate([image_ref[:, low:high], text_ref[:, low:high]], axis=0)
        d_out = jnp.concatenate([do_image[:, rows], do_text[:, rows]], axis=0)
        delta = jnp.sum(do_t[rows] * o_t[rows], axis=0, keepdims=True)
        d_out_t = do_t[rows].astype(BF16)
        d_keys = jnp.zeros((total, HEAD), F32)
        d_values = jnp.zeros((total, HEAD), F32)
        for start in range(0, total, step):
            part = slice(start, start + step)
            weights = jnp.exp(mm(keys, q_t[:, part]) - lse_ref[head, :, part])
            d_weights = mm(values, d_out_t[:, part])
            d_scores = (weights * (d_weights - delta[:, part])).astype(BF16)
            d_values += mm(weights.astype(BF16), d_out[part])
            d_keys += mm(d_scores, queries[part])
            dq_scr[rows, part] = mm(k_t, d_scores) * factor
        dv_scr[:, rows] = d_values
        dq = dq_scr[rows, :]
        dk = d_keys.T
        for slot, (grad, hat) in enumerate(((dq, q_hat), (dk, k_hat))):
            product = grad * hat
            image_sum = jnp.sum(product[:, :image_len], axis=1, keepdims=True)
            text_sum = jnp.sum(product[:, image_len:], axis=1, keepdims=True)
            gains_total += jnp.where(lane_row == 2 * slot, image_sum, 0.0)
            gains_total += jnp.where(lane_row == 2 * slot + 1, text_sum, 0.0)
        scaled = dq * q_gain
        dq_scr[rows, :] = q_root * (
            scaled - q_hat * jnp.mean(scaled * q_hat, axis=0, keepdims=True)
        )
        scaled = dk * k_gain
        dk_scr[rows, :] = k_root * (
            scaled - k_hat * jnp.mean(scaled * k_hat, axis=0, keepdims=True)
        )
    d_image[:, :wide] = dq_scr[:, :image_len].T.astype(BF16)
    d_text[:, :wide] = dq_scr[:, image_len:].T.astype(BF16)
    d_image[:, wide : 2 * wide] = dk_scr[:, :image_len].T.astype(BF16)
    d_text[:, wide : 2 * wide] = dk_scr[:, image_len:].T.astype(BF16)
    d_image[:, 2 * wide :] = dv_scr[:image_len].astype(BF16)
    d_text[:, 2 * wide :] = dv_scr[image_len:].astype(BF16)
    gain_grad[0] = gains_total


def query_step(total):
    for count in (3, 4, 2, 6, 9, 1):
        if total % (count * 128) == 0:
            return total // count
    return total


def kernel_cost(tokens, heads, products):
    return pl.CostEstimate(
        flops=2 * products * heads * tokens * tokens * HEAD * 4,
        transcendentals=heads * tokens * tokens,
        bytes_accessed=tokens * heads * HEAD * 2 * 8,
    )


def attention_forward(raw_image, raw_text, gains):
    groups = raw_image.shape[1] // (3 * 128)
    image_len, text_len = raw_image.shape[0], raw_text.shape[0]
    total = image_len + text_len
    return pl.pallas_call(
        functools.partial(attention_forward_kernel, query_step(total)),
        grid=(groups,),
        out_shape=(
            jax.ShapeDtypeStruct((image_len, groups * 128), BF16),
            jax.ShapeDtypeStruct((text_len, groups * 128), BF16),
            jax.ShapeDtypeStruct((groups * 2, 1, total), F32),
        ),
        in_specs=[
            pl.BlockSpec((image_len, 384), lambda g: (0, g)),
            pl.BlockSpec((text_len, 384), lambda g: (0, g)),
            pl.BlockSpec((HEAD, 4), lambda g: (0, 0)),
        ],
        out_specs=(
            pl.BlockSpec((image_len, 128), lambda g: (0, g)),
            pl.BlockSpec((text_len, 128), lambda g: (0, g)),
            pl.BlockSpec((2, 1, total), lambda g: (g, 0, 0)),
        ),
        scratch_shapes=[pltpu.VMEM((128, total), F32)],
        cost_estimate=kernel_cost(total, groups * 2, 2),
        name="attend_forward",
    )(raw_image, raw_text, gains)


def attention_backward(raw_image, raw_text, gains, o_image, o_text, do_image, do_text, lse):
    groups = raw_image.shape[1] // (3 * 128)
    image_len, text_len = raw_image.shape[0], raw_text.shape[0]
    total = image_len + text_len
    wide_image = pl.BlockSpec((image_len, 384), lambda g: (0, g))
    wide_text = pl.BlockSpec((text_len, 384), lambda g: (0, g))
    slim_image = pl.BlockSpec((image_len, 128), lambda g: (0, g))
    slim_text = pl.BlockSpec((text_len, 128), lambda g: (0, g))
    d_image, d_text, gain_grad = pl.pallas_call(
        functools.partial(attention_backward_kernel, query_step(total)),
        grid=(groups,),
        out_shape=(
            jax.ShapeDtypeStruct(raw_image.shape, BF16),
            jax.ShapeDtypeStruct(raw_text.shape, BF16),
            jax.ShapeDtypeStruct((groups, HEAD, 128), F32),
        ),
        in_specs=[
            wide_image,
            wide_text,
            pl.BlockSpec((HEAD, 4), lambda g: (0, 0)),
            slim_image,
            slim_text,
            slim_image,
            slim_text,
            pl.BlockSpec((2, 1, total), lambda g: (g, 0, 0)),
        ],
        out_specs=(wide_image, wide_text, pl.BlockSpec((1, HEAD, 128), lambda g: (g, 0, 0))),
        scratch_shapes=[
            pltpu.VMEM((128, total), F32),
            pltpu.VMEM((128, total), F32),
            pltpu.VMEM((total, 128), F32),
        ],
        cost_estimate=kernel_cost(total, groups * 2, 5),
        name="attend_backward",
    )(raw_image, raw_text, gains, o_image, o_text, do_image, do_text, lse)
    return d_image, d_text, jnp.sum(gain_grad, axis=0)


def plain_parts(raw_image, raw_text, gains):
    raw = jnp.concatenate([raw_image, raw_text], axis=0).astype(F32)
    raw = raw.reshape(raw.shape[0], -1, 3, HEAD)
    is_image = (jnp.arange(raw.shape[0]) < raw_image.shape[0])[:, None, None]
    hats, roots, scales, rounded = [], [], [], []
    for slot in range(2):
        part = raw[:, :, slot]
        root = lax.rsqrt(jnp.mean(part * part, axis=-1, keepdims=True) + EPSILON)
        scale = jnp.where(is_image, gains[:, 2 * slot], gains[:, 2 * slot + 1])
        hats.append(part * root)
        roots.append(root)
        scales.append(scale)
        rounded.append((part * root * scale).astype(BF16))
    return hats, roots, scales, rounded, raw[:, :, 2].astype(BF16)


def plain_forward(raw_image, raw_text, gains):
    _, _, _, (queries, keys), values = plain_parts(raw_image, raw_text, gains)
    scores = jnp.einsum("qhd,khd->hqk", queries, keys, preferred_element_type=F32)
    scores = scores * HEAD ** (-0.5)
    largest = jnp.max(scores, axis=-1, keepdims=True)
    lse = largest + jnp.log(jnp.sum(jnp.exp(scores - largest), axis=-1, keepdims=True))
    weights = jnp.exp(scores - lse).astype(BF16)
    out = jnp.einsum("hqk,khd->qhd", weights, values, preferred_element_type=F32)
    out = out.astype(BF16).reshape(out.shape[0], -1)
    return out[: raw_image.shape[0]], out[raw_image.shape[0] :], lse


def plain_backward(raw_image, raw_text, gains, o_image, o_text, do_image, do_text, lse):
    hats, roots, scales, (queries, keys), values = plain_parts(raw_image, raw_text, gains)
    factor = HEAD ** (-0.5)
    image_len = raw_image.shape[0]
    d_out = jnp.concatenate([do_image, do_text], axis=0).reshape(queries.shape)
    scores = jnp.einsum("qhd,khd->hqk", queries, keys, preferred_element_type=F32) * factor
    weights = jnp.exp(scores - lse)
    d_weights = jnp.einsum("qhd,khd->hqk", d_out, values, preferred_element_type=F32)
    inner = jnp.sum(weights * d_weights, axis=-1, keepdims=True)
    d_scores = (weights * (d_weights - inner)).astype(BF16)
    dq = jnp.einsum("hqk,khd->qhd", d_scores, keys, preferred_element_type=F32) * factor
    dk = jnp.einsum("hqk,qhd->khd", d_scores, queries, preferred_element_type=F32) * factor
    dv = jnp.einsum("hqk,qhd->khd", weights.astype(BF16), d_out, preferred_element_type=F32)
    gain_rows, parts = [], []
    for grad, hat, root, scale in zip((dq, dk), hats, roots, scales):
        product = grad * hat
        gain_rows += [jnp.sum(product[:image_len], (0, 1)), jnp.sum(product[image_len:], (0, 1))]
        scaled = grad * scale
        parts.append(root * (scaled - hat * jnp.mean(scaled * hat, axis=-1, keepdims=True)))
    joined = jnp.stack(parts + [dv], axis=2).astype(BF16).reshape(d_out.shape[0], -1)
    return joined[:image_len], joined[image_len:], jnp.stack(gain_rows, axis=1)


def tie(*groups):
    return lax.optimization_barrier(groups)


class Side:
    def __init__(self, state=(), steps=(), finish=None):
        self.state, self.steps, self.finish = state, list(steps), finish
        self.running = False

    def open(self, token):
        if self.steps:
            token, self.state = tie(token, self.state)
            self.state = self.steps.pop(0)(self.state)
            self.running = True
        return token

    def close(self, token):
        if self.running:
            token, self.state = tie(token, self.state)
            self.running = False
        return token

    def result(self):
        while self.steps:
            self.state = self.steps.pop(0)(self.state)
        return self.finish(self.state)


def join_kernel(size, cut, me_ref, own, *refs):
    after, before = refs[: size - 1], refs[size - 1 : 2 * size - 2]
    image, text, sems = refs[2 * size - 2 :]
    tail = own.shape[0] - cut

    def copies(source, k):
        return (
            pltpu.make_async_copy(
                source.at[pl.ds(0, cut)], image.at[pl.ds(k * cut, cut)], sems.at[k, 0]
            ),
            pltpu.make_async_copy(
                source.at[pl.ds(cut, tail)], text.at[pl.ds(k * tail, tail)], sems.at[k, 1]
            ),
        )

    def start(source, k):
        for copy in copies(source, k):
            copy.start()

    start(own, 0)
    for k in range(1, size):
        from_after = me_ref[0] + k < size
        pl.when(from_after)(functools.partial(start, after[k - 1], k))
        pl.when(jnp.logical_not(from_after))(functools.partial(start, before[size - k - 1], k))
    for k in range(size):
        for copy in copies(own, k):
            copy.wait()


def join_tokens(own, after, before, me, cut):
    size, (rows, width) = len(after) + 1, own.shape
    return pl.pallas_call(
        functools.partial(join_kernel, size, cut),
        out_shape=(
            jax.ShapeDtypeStruct((size * cut, width), own.dtype),
            jax.ShapeDtypeStruct((size * (rows - cut), width), own.dtype),
        ),
        in_specs=[pl.BlockSpec(memory_space=pltpu.SMEM)]
        + [pl.BlockSpec(memory_space=pl.ANY)] * (2 * size - 1),
        out_specs=(
            pl.BlockSpec(memory_space=pltpu.VMEM),
            pl.BlockSpec(memory_space=pltpu.VMEM),
        ),
        scratch_shapes=[pltpu.SemaphoreType.DMA((size, 2))],
        compiler_params=pltpu.CompilerParams(vmem_limit_bytes=16 * 2**20),
        cost_estimate=pl.CostEstimate(
            flops=0, transcendentals=0, bytes_accessed=4 * size * own.size
        ),
        name="join_tokens",
    )(me.astype(jnp.int32)[None], own, *after, *before)


class Streams:
    def __init__(self, image_len, text_len, axis, size):
        self.lengths = (image_len, text_len)
        self.axis, self.size = axis, size

    def gather_side(self, pair):
        size = self.size

        def step(state):
            own, after, before = state
            down, up = (after[-1], before[-1]) if after else (own, own)
            down = lax.ppermute(down, self.axis, [(i, i - 1) for i in range(1, size)])
            up = lax.ppermute(up, self.axis, [(i, i + 1) for i in range(size - 1)])
            return own, after + (down,), before + (up,)

        def finish(state):
            return join_tokens(*state, lax.axis_index(self.axis), self.lengths[0])

        return Side((jnp.concatenate(pair, axis=0), (), ()), [step] * (size - 1), finish)

    def scatter_side(self, pair):
        size, (image_len, text_len) = self.size, self.lengths
        image, text = (part.astype(BF16) for part in pair)
        cut = (image_len + text_len) // 32 * 16
        firsts = tuple(image[k * image_len : k * image_len + cut] for k in range(size))
        seconds = tuple(
            jnp.concatenate(
                [
                    image[k * image_len + cut : (k + 1) * image_len],
                    text[k * text_len : (k + 1) * text_len],
                ],
                axis=0,
            )
            for k in range(size)
        )

        def step(index, state):
            return tuple(half_step(index, *half) for half in state)

        def half_step(index, blocks, sums):
            k = size - 1 - index
            send_up, send_down = blocks[k], blocks[size - k]
            if sums:
                send_up, send_down = (
                    (send.astype(F32) + value.astype(F32)).astype(BF16)
                    for send, value in zip((send_up, send_down), sums)
                )
            up = lax.ppermute(send_up, self.axis, [(i, i + 1) for i in range(index + 1)])
            down = lax.ppermute(send_down, self.axis, [(i, i - 1) for i in range(k, size)])
            return blocks, (up, down)

        def finish(state):
            first, second = (
                blocks[0].astype(F32) + up.astype(F32) + down.astype(F32)
                for blocks, (up, down) in state
            )
            return (
                jnp.concatenate([first, second[: image_len - cut]], axis=0),
                second[image_len - cut :],
            )

        steps = [functools.partial(step, index) for index in range(size - 1)]
        return Side(((firsts, ()), (seconds, ())), steps, finish)

    def gather(self, pair):
        return self.gather_side(pair).result()

    def scatter(self, pair):
        return self.scatter_side(pair).result()


def bit_order(size):
    bits = [b for b in range(size.bit_length() - 1)]
    masks = [0]
    for b in bits:
        masks += [m | (1 << b) for m in masks]
    return bits, masks


def swap_bit(value, axis, size, bit):
    return lax.ppermute(value, axis, [(i, i ^ (1 << bit)) for i in range(size)])


def bit_gather(own, axis, size):
    blocks = own[None]
    for b in bit_order(size)[0]:
        blocks = jnp.concatenate([blocks, swap_bit(blocks, axis, size, b)], axis=0)
    return blocks


def bit_scatter(parts, axis, size, after_first):
    me = lax.axis_index(axis)
    for b in reversed(bit_order(size)[0]):
        half = parts.shape[0] // 2
        upper = ((me >> b) & 1) == 1
        keep = jnp.where(upper, parts[half:], parts[:half])
        send = jnp.where(upper, parts[:half], parts[half:])
        parts = keep + swap_bit(send, axis, size, b)
        if after_first is not None:
            parts, after_first = after_first(parts), None
    return parts[0]


def bit_sum(value, axis, size):
    for b in bit_order(size)[0]:
        value = value + swap_bit(value, axis, size, b)
    return value


def forward_layer(streams, x, mods, weights, gains, attend, plain, side, last):
    qkv, out_t, up, down_t = weights
    if plain is not None:
        normed = [
            (plain[s].astype(F32) * (1.0 + mods[s, 1]) + mods[s, 0]).astype(BF16)
            for s in range(2)
        ]
    else:
        normed = streams.gather(
            [modulate(x[s], mods[s, 0], mods[s, 1]).astype(BF16) for s in range(2)]
        )
    raw = side.open([mm(normed[s], qkv[s]).astype(BF16) for s in range(2)])
    o_image, o_text, lse = attend(raw[0], raw[1], gains)
    mixed = side.close((o_image, o_text))
    branch = streams.scatter([mm_nt(mixed[s], out_t[s]) for s in range(2)])
    middle = [x[s] + mods[s, 2] * branch[s] for s in range(2)]
    second = streams.gather(
        [modulate(middle[s], mods[s, 3], mods[s, 4]).astype(BF16) for s in range(2)]
    )
    second = side.open(second)
    hidden = [mm(second[s], up[s]) for s in range(2)]
    active = side.close([gelu(hidden[s]).astype(BF16) for s in range(2)])
    hidden = [hidden[s].astype(BF16) for s in range(2)]
    result = streams.scatter_side([mm_nt(active[s], down_t[s]) for s in range(2)])
    saved = (x, normed, raw, mixed, lse, branch, middle, second, hidden, active)
    if last:
        return None, saved, result
    result = result.result()
    return [middle[s] + mods[s, 5] * result[s] for s in range(2)], saved, result


def backward_layer(streams, gy, dm, saved, mods, weights, gains, calls, side, last):
    qkv, out_t, up, down_t = weights
    x, normed, raw, mixed, lse, branch, middle, second, hidden, active = saved
    if dm is None:
        dm = streams.gather([(mods[s, 5] * gy[s]).astype(BF16) for s in range(2)])
    dm = side.open(dm)
    du = []
    for s in range(2):
        _, pull = jax.vjp(gelu, hidden[s].astype(F32))
        du.append(pull(mm(dm[s], down_t[s]))[0].astype(BF16))
    d_second = side.close([mm_nt(du[s], up[s]).astype(BF16) for s in range(2)])
    d_second = streams.scatter_side(d_second)
    du = d_second.close(d_second.open(du))
    late = [mm_tn(second[s], du[s]) for s in range(2)]
    late += [mm_tn(dm[s], active[s]) for s in range(2)]
    reduced_mlp = calls.reduce_grad(jnp.stack([part.astype(BF16) for part in late]))
    d_second = calls.settle(d_second.result())
    d_middle, d_shift2, d_scale2 = [], [], []
    for s in range(2):
        inner, d_shift, d_scale = modulate_back(middle[s], d_second[s], mods[s, 4])
        d_middle.append(gy[s] + inner)
        d_shift2.append(d_shift)
        d_scale2.append(d_scale)
    d_gate1 = [jnp.sum(d_middle[s] * branch[s], axis=0) for s in range(2)]
    da = streams.gather_side([(mods[s, 2] * d_middle[s]).astype(BF16) for s in range(2)])
    early = d_gate1, d_shift2, d_scale2
    if last:
        da = calls.before_end(early, da)
    else:
        da = da.result()
    d_mixed = side.open([mm(da[s], out_t[s]).astype(BF16) for s in range(2)])
    late = jnp.stack([mm_tn(da[s], mixed[s]).astype(BF16) for s in range(2)])
    reduced_out = calls.reduce_grad(late)
    d_image, d_text, gain_rows = calls.attend_back(
        raw[0], raw[1], gains, mixed[0], mixed[1], d_mixed[0], d_mixed[1], lse
    )
    d_raw = side.close((d_image, d_text))
    if last:
        late = jnp.stack([mm_tn(normed[s], d_raw[s]).astype(BF16) for s in range(2)])
        d_raw, late = tie(d_raw, late)
        d_first = [mm_nt(d_raw[s], qkv[s]).astype(BF16) for s in range(2)]
        d_first, reduced_mlp[0] = tie(d_first, reduced_mlp[0])
        d_first = streams.scatter_side(d_first)
    else:
        d_first = streams.scatter_side([mm_nt(d_raw[s], qkv[s]) for s in range(2)])
        d_raw = d_first.close(d_first.open(d_raw))
        late = jnp.stack([mm_tn(normed[s], d_raw[s]).astype(BF16) for s in range(2)])
    reduced_qkv = calls.reduce_grad(late)
    if last:
        for _ in range(2):
            calls.shared = d_first.close(d_first.open(calls.shared))
    d_first = d_first.result()
    if not last:
        d_first, reduced_mlp[0] = tie(d_first, reduced_mlp[0])
        calls.pending = [reduced_qkv, reduced_out]
    gx, late = [], []
    for s in range(2):
        inner, d_shift, d_scale = modulate_back(x[s], d_first[s], mods[s, 1])
        gx.append(d_middle[s] + inner)
        late += [d_shift, d_scale]
    return gx, early, gain_rows, late, (reduced_qkv, reduced_out, reduced_mlp)


class Calls:
    def __init__(self, attend_back, dp_axis):
        self.attend_back, self.axis, self.pending = attend_back, dp_axis, []
        self.before_end = self.shared = None

    def reduce_grad(self, grad):
        return [lax.psum_scatter(grad, self.axis, scatter_dimension=1, tiled=True)]

    def settle(self, token):
        for box in self.pending:
            token, box[0] = tie(token, box[0])
        self.pending = []
        return token


def on_device(dp, seq, width_of_group, *args):
    (
        image_in,
        text_input,
        condition,
        ada_weight,
        qkv_weight,
        out_weight,
        up_weight,
        down_weight,
        norm_gain,
        image_cotangent,
        text_cotangent,
    ) = args
    dp_axis, dp_size = dp
    seq_axis, seq_size = seq
    layers = qkv_weight.shape[0]
    width = image_in.shape[2]
    streams = Streams(image_in.shape[1], text_input.shape[1], seq_axis, seq_size)
    attend, attend_back = (
        (attention_forward, attention_backward)
        if width_of_group % 128 == 0
        else (plain_forward, plain_backward)
    )
    rows = qkv_weight.shape[2]

    act_cond, silu_pull = jax.vjp(jax.nn.silu, condition.astype(F32))
    act_low = act_cond.astype(BF16)
    partial_mods = jnp.einsum("nd,lsde->nlse", act_low, ada_weight, preferred_element_type=F32)
    x = [image_in[0].astype(F32), text_input[0].astype(F32)]
    plain = streams.gather_side([layer_stats(part)[0].astype(BF16) for part in x])
    plain.state = plain.steps.pop(0)(plain.state)

    given = [qkv_weight]

    def beside_tokens(parts):
        parts, plain.state, given[0] = tie(parts, plain.state, given[0])
        return parts

    own_mods = partial_mods.reshape(dp_size, -1)
    own_mods = bit_scatter(own_mods, dp_axis, dp_size, beside_tokens)
    plain = plain.result()
    qkv_weight, others = given[0], (out_weight, up_weight, down_weight)
    own_mods, plain, others = tie(own_mods, plain, others)
    out_weight, up_weight, down_weight = others

    def fetch(local):
        return lax.all_gather(local, dp_axis, axis=1, tiled=True)

    qkv_local = qkv_weight.reshape(layers, 2, rows, 3, -1, width_of_group)
    qkv_local = qkv_local.transpose(0, 1, 2, 4, 3, 5).reshape(layers, 2, rows, -1)
    out_local = out_weight.transpose(0, 1, 3, 2)
    down_local = down_weight.transpose(0, 1, 3, 2)
    weights = [
        tuple(fetch(w[l]) for w in (qkv_local, out_local, up_weight, down_local))
        for l in range(layers)
    ]

    own_mods = bit_sum(own_mods, seq_axis, seq_size).reshape(layers, 2, 6, width)
    gains_all = norm_gain.astype(F32)
    gain_columns = [gains_all[l].transpose(1, 0, 2).reshape(4, HEAD).T for l in range(layers)]

    gy = [image_cotangent[0].astype(F32), text_cotangent[0].astype(F32)]
    side = streams.gather_side(
        [(own_mods[layers - 1, s, 5] * gy[s]).astype(BF16) for s in range(2)]
    )
    saved_list, results = [], []
    for l in range(layers):
        x, saved, result = forward_layer(
            streams,
            x,
            own_mods[l],
            weights[l],
            gain_columns[l],
            attend,
            None if l else plain,
            side,
            l == layers - 1,
        )
        saved_list.append(saved)
        results.append(result)
    dm, side = side.result(), results[-1]

    def share(values):
        return bit_gather(bit_sum(values, seq_axis, seq_size), dp_axis, dp_size)

    gys, early_all, late_all = [None] * layers, [None] * layers, [None] * layers
    grads, gain_all = [None] * layers, [None] * layers

    def before_end(early, gather):
        early_all[0] = early
        results[-1] = side.result()
        layer_rows = []
        for l in range(layers):
            d_gate2 = [jnp.sum(gys[l][s] * results[l][s], axis=0) for s in range(2)]
            d_gate1, d_shift2, d_scale2 = early_all[l]
            first = late_all[l] if l else [jnp.zeros_like(d_gate2[0])] * 4
            layer_rows.append(
                [
                    first[2 * s : 2 * s + 2] + [d_gate1[s], d_shift2[s], d_scale2[s], d_gate2[s]]
                    for s in range(2)
                ]
            )
        layer_rows = gather.close(gather.open(layer_rows))
        rows = jnp.stack([jnp.stack([jnp.stack(r) for r in both]) for both in layer_rows])
        token, calls.shared = tie(gather.result(), rows)
        return token

    calls = Calls(attend_back, dp_axis)
    calls.before_end = before_end
    for l in reversed(range(layers)):
        gys[l] = gy
        gy, early_all[l], gain_all[l], late_all[l], grads[l] = backward_layer(
            streams,
            gy,
            dm,
            saved_list[l],
            own_mods[l],
            weights[l],
            gain_columns[l],
            calls,
            side,
            l == 0,
        )
        dm = None
    last_middle = saved_list[-1][6]
    outputs = [
        (last_middle[s] + own_mods[layers - 1, s, 5] * results[-1][s]).astype(BF16)[None]
        for s in range(2)
    ]

    there = jnp.array(bit_order(dp_size)[1], jnp.int32) ^ lax.axis_index(dp_axis)
    late_all[0], grads[0], gain_all = tie(late_all[0], grads[0], gain_all)
    rest = share(jnp.stack([jnp.stack(late_all[0][:2]), jnp.stack(late_all[0][2:])]))
    total_mods, total_gains = share(calls.shared), share(jnp.stack(gain_all))
    first = jnp.concatenate([rest, total_mods[:, 0, :, 2:]], axis=2)
    total_mods = jnp.concatenate([first[:, None], total_mods[:, 1:]], axis=1)
    total_mods = total_mods.reshape(dp_size, layers, 2, 6 * width)
    total_gains = jnp.sum(total_gains[there], axis=0)[:, :, :4]
    total_gains = total_gains.reshape(layers, HEAD, 2, 2).transpose(0, 3, 2, 1)
    act_there = act_low.astype(F32)[there]
    ada_grad = jnp.einsum("nd,nlse->lsde", act_there, total_mods, precision=HIGHEST)
    d_act = jnp.einsum("nlse,lsde->nd", total_mods, ada_weight.astype(F32), precision=HIGHEST)
    condition_grad = silu_pull(d_act[there])[0]

    def pieces(kind, first):
        return jnp.stack([grads[l][kind][0][first : first + 2] for l in range(layers)]).astype(F32)

    qkv_grad = pieces(0, 0).reshape(layers, 2, rows, -1, 3, width_of_group)
    qkv_grad = qkv_grad.transpose(0, 1, 2, 4, 3, 5).reshape(qkv_weight.shape)
    return (
        outputs[0],
        outputs[1],
        gy[0][None],
        gy[1][None],
        condition_grad,
        ada_grad,
        qkv_grad,
        pieces(1, 0).transpose(0, 1, 3, 2),
        pieces(2, 0),
        pieces(2, 2).transpose(0, 1, 3, 2),
        total_gains,
    )


def solution(mesh):
    tokens = P("dp", "seq", None)
    placed = (
        tokens,
        tokens,
        P(None, ("dp", "seq")),
        P(None, None, ("dp", "seq"), None),
        P(None, None, "dp", None, "seq"),
        P(None, None, "seq", "dp"),
        P(None, None, "dp", "seq"),
        P(None, None, "seq", "dp"),
        P(),
        tokens,
        tokens,
    )
    results = (tokens, tokens, tokens, tokens) + placed[2:8] + (P(),)

    def step(*args):
        heads = args[4].shape[4] // mesh.shape["seq"] // HEAD
        group = 2 * HEAD if heads % 2 == 0 else HEAD
        body = functools.partial(
            on_device, ("dp", mesh.shape["dp"]), ("seq", mesh.shape["seq"]), group
        )
        return jax.shard_map(
            body, mesh=mesh, in_specs=placed, out_specs=results, check_vma=False
        )(*args)

    return step
```

```python
import functools

import jax
import jax.numpy as jnp
from jax import lax
from jax.experimental import pallas as pl
from jax.experimental.pallas import tpu as pltpu
from jax.sharding import PartitionSpec as P

EPSILON = 1e-06
HIGHEST = lax.Precision.HIGHEST
F32 = jnp.float32
BF16 = jnp.bfloat16
HEAD = 64


def layer_stats(values):
    centred = values - jnp.mean(values, axis=-1, keepdims=True)
    root = lax.rsqrt(jnp.mean(centred * centred, axis=-1, keepdims=True) + EPSILON)
    return centred * root, root


def modulate(values, shift, scale):
    return layer_stats(values)[0] * (1.0 + scale) + shift


def modulate_back(values, grad, scale):
    normed, root = layer_stats(values)
    inner = grad * (1.0 + scale)
    first = jnp.mean(inner, axis=-1, keepdims=True)
    second = jnp.mean(inner * normed, axis=-1, keepdims=True)
    d_values = root * (inner - first - normed * second)
    return d_values, jnp.sum(grad, axis=0), jnp.sum(grad * normed, axis=0)


def mm(left, right):
    return lax.dot_general(left, right, (((1,), (0,)), ((), ())), preferred_element_type=F32)


def mm_nt(left, right):
    return lax.dot_general(left, right, (((1,), (1,)), ((), ())), preferred_element_type=F32)


def mm_tn(left, right):
    return lax.dot_general(left, right, (((0,), (0,)), ((), ())), preferred_element_type=F32)


def gelu(values):
    return jax.nn.gelu(values, approximate=True)


def head_factors(raw_t, gain_image, gain_text, image_len):
    root = lax.rsqrt(jnp.mean(raw_t * raw_t, axis=0, keepdims=True) + EPSILON)
    lanes = lax.broadcasted_iota(jnp.int32, raw_t.shape, 1)
    gain = jnp.where(lanes < image_len, gain_image, gain_text)
    return raw_t * root, root, gain


def transposed(first, second, low, high):
    return jnp.concatenate(
        [first[:, low:high].astype(F32).T, second[:, low:high].astype(F32).T], axis=1
    )


def attention_forward_kernel(step, image_ref, text_ref, gain_ref, o_image, o_text, lse_ref, o_scr):
    image_len, text_len = image_ref.shape[0], text_ref.shape[0]
    total = image_len + text_len
    wide = image_ref.shape[1] // 3
    factor = HEAD ** (-0.5)
    raw_q = transposed(image_ref, text_ref, 0, wide)
    raw_k = transposed(image_ref, text_ref, wide, 2 * wide)
    values_t = transposed(image_ref, text_ref, 2 * wide, 3 * wide).astype(BF16)
    for head in range(wide // HEAD):
        rows = slice(head * HEAD, (head + 1) * HEAD)
        q_hat, _, q_gain = head_factors(raw_q[rows], gain_ref[:, 0:1], gain_ref[:, 1:2], image_len)
        k_hat, _, k_gain = head_factors(raw_k[rows], gain_ref[:, 2:3], gain_ref[:, 3:4], image_len)
        q_t = ((q_hat * q_gain).astype(BF16).astype(F32) * factor).astype(BF16)
        keys = (k_hat * k_gain).T.astype(BF16)
        v_t = values_t[rows]
        for start in range(0, total, step):
            part = slice(start, start + step)
            scores = mm(keys, q_t[:, part])
            largest = jnp.max(scores, axis=0, keepdims=True)
            weights = jnp.exp(scores - largest)
            total_w = jnp.sum(weights, axis=0, keepdims=True)
            out = mm(v_t, weights.astype(BF16)) * (1.0 / total_w)
            o_scr[rows, part] = out
            lse_ref[head, :, part] = largest + jnp.log(total_w)
    o_image[...] = o_scr[:, :image_len].T.astype(BF16)
    o_text[...] = o_scr[:, image_len:].T.astype(BF16)


def attention_backward_kernel(
    step,
    image_ref,
    text_ref,
    gain_ref,
    o_image,
    o_text,
    do_image,
    do_text,
    lse_ref,
    d_image,
    d_text,
    gain_grad,
    dq_scr,
    dk_scr,
    dv_scr,
):
    image_len, text_len = image_ref.shape[0], text_ref.shape[0]
    total = image_len + text_len
    wide = image_ref.shape[1] // 3
    factor = HEAD ** (-0.5)
    raw_q = transposed(image_ref, text_ref, 0, wide)
    raw_k = transposed(image_ref, text_ref, wide, 2 * wide)
    o_t = transposed(o_image, o_text, 0, wide)
    do_t = transposed(do_image, do_text, 0, wide)
    lane_row = lax.broadcasted_iota(jnp.int32, (HEAD, 128), 1)
    gains_total = jnp.zeros((HEAD, 128), F32)
    for head in range(wide // HEAD):
        rows = slice(head * HEAD, (head + 1) * HEAD)
        low, high = 2 * wide + head * HEAD, 2 * wide + (head + 1) * HEAD
        q_hat, q_root, q_gain = head_factors(
            raw_q[rows], gain_ref[:, 0:1], gain_ref[:, 1:2], image_len
        )
        k_hat, k_root, k_gain = head_factors(
            raw_k[rows], gain_ref[:, 2:3], gain_ref[:, 3:4], image_len
        )
        q_full = (q_hat * q_gain).astype(BF16).astype(F32) * factor
        q_t = q_full.astype(BF16)
        queries = q_full.T.astype(BF16)
        k_t = (k_hat * k_gain).astype(BF16)
        keys = (k_hat * k_gain).T.astype(BF16)
        values = jnp.concatenate([image_ref[:, low:high], text_ref[:, low:high]], axis=0)
        d_out = jnp.concatenate([do_image[:, rows], do_text[:, rows]], axis=0)
        delta = jnp.sum(do_t[rows] * o_t[rows], axis=0, keepdims=True)
        d_out_t = do_t[rows].astype(BF16)
        d_keys = jnp.zeros((total, HEAD), F32)
        d_values = jnp.zeros((total, HEAD), F32)
        for start in range(0, total, step):
            part = slice(start, start + step)
            weights = jnp.exp(mm(keys, q_t[:, part]) - lse_ref[head, :, part])
            d_weights = mm(values, d_out_t[:, part])
            d_scores = (weights * (d_weights - delta[:, part])).astype(BF16)
            d_values += mm(weights.astype(BF16), d_out[part])
            d_keys += mm(d_scores, queries[part])
            dq_scr[rows, part] = mm(k_t, d_scores) * factor
        dv_scr[:, rows] = d_values
        dq = dq_scr[rows, :]
        dk = d_keys.T
        for slot, (grad, hat) in enumerate(((dq, q_hat), (dk, k_hat))):
            product = grad * hat
            image_sum = jnp.sum(product[:, :image_len], axis=1, keepdims=True)
            text_sum = jnp.sum(product[:, image_len:], axis=1, keepdims=True)
            gains_total += jnp.where(lane_row == 2 * slot, image_sum, 0.0)
            gains_total += jnp.where(lane_row == 2 * slot + 1, text_sum, 0.0)
        scaled = dq * q_gain
        dq_scr[rows, :] = q_root * (
            scaled - q_hat * jnp.mean(scaled * q_hat, axis=0, keepdims=True)
        )
        scaled = dk * k_gain
        dk_scr[rows, :] = k_root * (
            scaled - k_hat * jnp.mean(scaled * k_hat, axis=0, keepdims=True)
        )
    d_image[:, :wide] = dq_scr[:, :image_len].T.astype(BF16)
    d_text[:, :wide] = dq_scr[:, image_len:].T.astype(BF16)
    d_image[:, wide : 2 * wide] = dk_scr[:, :image_len].T.astype(BF16)
    d_text[:, wide : 2 * wide] = dk_scr[:, image_len:].T.astype(BF16)
    d_image[:, 2 * wide :] = dv_scr[:image_len].astype(BF16)
    d_text[:, 2 * wide :] = dv_scr[image_len:].astype(BF16)
    gain_grad[0] = gains_total


def query_step(total):
    for count in (3, 4, 2, 6, 9, 1):
        if total % (count * 128) == 0:
            return total // count
    return total


def kernel_cost(tokens, heads, products):
    return pl.CostEstimate(
        flops=2 * products * heads * tokens * tokens * HEAD * 4,
        transcendentals=heads * tokens * tokens,
        bytes_accessed=tokens * heads * HEAD * 2 * 8,
    )


def attention_forward(raw_image, raw_text, gains):
    groups = raw_image.shape[1] // (3 * 128)
    image_len, text_len = raw_image.shape[0], raw_text.shape[0]
    total = image_len + text_len
    return pl.pallas_call(
        functools.partial(attention_forward_kernel, query_step(total)),
        grid=(groups,),
        out_shape=(
            jax.ShapeDtypeStruct((image_len, groups * 128), BF16),
            jax.ShapeDtypeStruct((text_len, groups * 128), BF16),
            jax.ShapeDtypeStruct((groups * 2, 1, total), F32),
        ),
        in_specs=[
            pl.BlockSpec((image_len, 384), lambda g: (0, g)),
            pl.BlockSpec((text_len, 384), lambda g: (0, g)),
            pl.BlockSpec((HEAD, 4), lambda g: (0, 0)),
        ],
        out_specs=(
            pl.BlockSpec((image_len, 128), lambda g: (0, g)),
            pl.BlockSpec((text_len, 128), lambda g: (0, g)),
            pl.BlockSpec((2, 1, total), lambda g: (g, 0, 0)),
        ),
        scratch_shapes=[pltpu.VMEM((128, total), F32)],
        cost_estimate=kernel_cost(total, groups * 2, 2),
        name="attend_forward",
    )(raw_image, raw_text, gains)


def attention_backward(raw_image, raw_text, gains, o_image, o_text, do_image, do_text, lse):
    groups = raw_image.shape[1] // (3 * 128)
    image_len, text_len = raw_image.shape[0], raw_text.shape[0]
    total = image_len + text_len
    wide_image = pl.BlockSpec((image_len, 384), lambda g: (0, g))
    wide_text = pl.BlockSpec((text_len, 384), lambda g: (0, g))
    slim_image = pl.BlockSpec((image_len, 128), lambda g: (0, g))
    slim_text = pl.BlockSpec((text_len, 128), lambda g: (0, g))
    d_image, d_text, gain_grad = pl.pallas_call(
        functools.partial(attention_backward_kernel, query_step(total)),
        grid=(groups,),
        out_shape=(
            jax.ShapeDtypeStruct(raw_image.shape, BF16),
            jax.ShapeDtypeStruct(raw_text.shape, BF16),
            jax.ShapeDtypeStruct((groups, HEAD, 128), F32),
        ),
        in_specs=[
            wide_image,
            wide_text,
            pl.BlockSpec((HEAD, 4), lambda g: (0, 0)),
            slim_image,
            slim_text,
            slim_image,
            slim_text,
            pl.BlockSpec((2, 1, total), lambda g: (g, 0, 0)),
        ],
        out_specs=(wide_image, wide_text, pl.BlockSpec((1, HEAD, 128), lambda g: (g, 0, 0))),
        scratch_shapes=[
            pltpu.VMEM((128, total), F32),
            pltpu.VMEM((128, total), F32),
            pltpu.VMEM((total, 128), F32),
        ],
        cost_estimate=kernel_cost(total, groups * 2, 5),
        name="attend_backward",
    )(raw_image, raw_text, gains, o_image, o_text, do_image, do_text, lse)
    return d_image, d_text, jnp.sum(gain_grad, axis=0)


def plain_parts(raw_image, raw_text, gains):
    raw = jnp.concatenate([raw_image, raw_text], axis=0).astype(F32)
    raw = raw.reshape(raw.shape[0], -1, 3, HEAD)
    is_image = (jnp.arange(raw.shape[0]) < raw_image.shape[0])[:, None, None]
    hats, roots, scales, rounded = [], [], [], []
    for slot in range(2):
        part = raw[:, :, slot]
        root = lax.rsqrt(jnp.mean(part * part, axis=-1, keepdims=True) + EPSILON)
        scale = jnp.where(is_image, gains[:, 2 * slot], gains[:, 2 * slot + 1])
        hats.append(part * root)
        roots.append(root)
        scales.append(scale)
        rounded.append((part * root * scale).astype(BF16))
    return hats, roots, scales, rounded, raw[:, :, 2].astype(BF16)


def plain_forward(raw_image, raw_text, gains):
    _, _, _, (queries, keys), values = plain_parts(raw_image, raw_text, gains)
    scores = jnp.einsum("qhd,khd->hqk", queries, keys, preferred_element_type=F32)
    scores = scores * HEAD ** (-0.5)
    largest = jnp.max(scores, axis=-1, keepdims=True)
    lse = largest + jnp.log(jnp.sum(jnp.exp(scores - largest), axis=-1, keepdims=True))
    weights = jnp.exp(scores - lse).astype(BF16)
    out = jnp.einsum("hqk,khd->qhd", weights, values, preferred_element_type=F32)
    out = out.astype(BF16).reshape(out.shape[0], -1)
    return out[: raw_image.shape[0]], out[raw_image.shape[0] :], lse


def plain_backward(raw_image, raw_text, gains, o_image, o_text, do_image, do_text, lse):
    hats, roots, scales, (queries, keys), values = plain_parts(raw_image, raw_text, gains)
    factor = HEAD ** (-0.5)
    image_len = raw_image.shape[0]
    d_out = jnp.concatenate([do_image, do_text], axis=0).reshape(queries.shape)
    scores = jnp.einsum("qhd,khd->hqk", queries, keys, preferred_element_type=F32) * factor
    weights = jnp.exp(scores - lse)
    d_weights = jnp.einsum("qhd,khd->hqk", d_out, values, preferred_element_type=F32)
    inner = jnp.sum(weights * d_weights, axis=-1, keepdims=True)
    d_scores = (weights * (d_weights - inner)).astype(BF16)
    dq = jnp.einsum("hqk,khd->qhd", d_scores, keys, preferred_element_type=F32) * factor
    dk = jnp.einsum("hqk,qhd->khd", d_scores, queries, preferred_element_type=F32) * factor
    dv = jnp.einsum("hqk,qhd->khd", weights.astype(BF16), d_out, preferred_element_type=F32)
    gain_rows, parts = [], []
    for grad, hat, root, scale in zip((dq, dk), hats, roots, scales):
        product = grad * hat
        gain_rows += [jnp.sum(product[:image_len], (0, 1)), jnp.sum(product[image_len:], (0, 1))]
        scaled = grad * scale
        parts.append(root * (scaled - hat * jnp.mean(scaled * hat, axis=-1, keepdims=True)))
    joined = jnp.stack(parts + [dv], axis=2).astype(BF16).reshape(d_out.shape[0], -1)
    return joined[:image_len], joined[image_len:], jnp.stack(gain_rows, axis=1)


def tie(*groups):
    return lax.optimization_barrier(groups)


class Side:
    def __init__(self, state=(), steps=(), finish=None):
        self.state, self.steps, self.finish = state, list(steps), finish
        self.running = False

    def open(self, token):
        if self.steps:
            token, self.state = tie(token, self.state)
            self.state = self.steps.pop(0)(self.state)
            self.running = True
        return token

    def close(self, token):
        if self.running:
            token, self.state = tie(token, self.state)
            self.running = False
        return token

    def result(self):
        while self.steps:
            self.state = self.steps.pop(0)(self.state)
        return self.finish(self.state)


def join_kernel(size, cut, me_ref, own, *refs):
    after, before = refs[: size - 1], refs[size - 1 : 2 * size - 2]
    image, text, sems = refs[2 * size - 2 :]
    tail = own.shape[0] - cut

    def copies(source, k):
        return (
            pltpu.make_async_copy(
                source.at[pl.ds(0, cut)], image.at[pl.ds(k * cut, cut)], sems.at[k, 0]
            ),
            pltpu.make_async_copy(
                source.at[pl.ds(cut, tail)], text.at[pl.ds(k * tail, tail)], sems.at[k, 1]
            ),
        )

    def start(source, k):
        for copy in copies(source, k):
            copy.start()

    start(own, 0)
    for k in range(1, size):
        from_after = me_ref[0] + k < size
        pl.when(from_after)(functools.partial(start, after[k - 1], k))
        pl.when(jnp.logical_not(from_after))(functools.partial(start, before[size - k - 1], k))
    for k in range(size):
        for copy in copies(own, k):
            copy.wait()


def join_tokens(own, after, before, me, cut):
    size, (rows, width) = len(after) + 1, own.shape
    return pl.pallas_call(
        functools.partial(join_kernel, size, cut),
        out_shape=(
            jax.ShapeDtypeStruct((size * cut, width), own.dtype),
            jax.ShapeDtypeStruct((size * (rows - cut), width), own.dtype),
        ),
        in_specs=[pl.BlockSpec(memory_space=pltpu.SMEM)]
        + [pl.BlockSpec(memory_space=pl.ANY)] * (2 * size - 1),
        out_specs=(
            pl.BlockSpec(memory_space=pltpu.VMEM),
            pl.BlockSpec(memory_space=pltpu.VMEM),
        ),
        scratch_shapes=[pltpu.SemaphoreType.DMA((size, 2))],
        compiler_params=pltpu.CompilerParams(vmem_limit_bytes=16 * 2**20),
        cost_estimate=pl.CostEstimate(
            flops=0, transcendentals=0, bytes_accessed=4 * size * own.size
        ),
        name="join_tokens",
    )(me.astype(jnp.int32)[None], own, *after, *before)


class Streams:
    def __init__(self, image_len, text_len, axis, size):
        self.lengths = (image_len, text_len)
        self.axis, self.size = axis, size

    def gather_side(self, pair):
        size = self.size

        def step(state):
            own, after, before = state
            down, up = (after[-1], before[-1]) if after else (own, own)
            down = lax.ppermute(down, self.axis, [(i, i - 1) for i in range(1, size)])
            up = lax.ppermute(up, self.axis, [(i, i + 1) for i in range(size - 1)])
            return own, after + (down,), before + (up,)

        def finish(state):
            return join_tokens(*state, lax.axis_index(self.axis), self.lengths[0])

        return Side((jnp.concatenate(pair, axis=0), (), ()), [step] * (size - 1), finish)

    def scatter_side(self, pair):
        size, (image_len, text_len) = self.size, self.lengths
        image, text = (part.astype(BF16) for part in pair)
        cut = (image_len + text_len) // 32 * 16
        firsts = tuple(image[k * image_len : k * image_len + cut] for k in range(size))
        seconds = tuple(
            jnp.concatenate(
                [
                    image[k * image_len + cut : (k + 1) * image_len],
                    text[k * text_len : (k + 1) * text_len],
                ],
                axis=0,
            )
            for k in range(size)
        )

        def step(index, state):
            return tuple(half_step(index, *half) for half in state)

        def half_step(index, blocks, sums):
            k = size - 1 - index
            send_up, send_down = blocks[k], blocks[size - k]
            if sums:
                send_up, send_down = (
                    (send.astype(F32) + value.astype(F32)).astype(BF16)
                    for send, value in zip((send_up, send_down), sums)
                )
            up = lax.ppermute(send_up, self.axis, [(i, i + 1) for i in range(index + 1)])
            down = lax.ppermute(send_down, self.axis, [(i, i - 1) for i in range(k, size)])
            return blocks, (up, down)

        def finish(state):
            first, second = (
                blocks[0].astype(F32) + up.astype(F32) + down.astype(F32)
                for blocks, (up, down) in state
            )
            return (
                jnp.concatenate([first, second[: image_len - cut]], axis=0),
                second[image_len - cut :],
            )

        steps = [functools.partial(step, index) for index in range(size - 1)]
        return Side(((firsts, ()), (seconds, ())), steps, finish)

    def gather(self, pair):
        return self.gather_side(pair).result()

    def scatter(self, pair):
        return self.scatter_side(pair).result()


def bit_order(size):
    bits = [b for b in range(size.bit_length() - 1)]
    masks = [0]
    for b in bits:
        masks += [m | (1 << b) for m in masks]
    return bits, masks


def swap_bit(value, axis, size, bit):
    return lax.ppermute(value, axis, [(i, i ^ (1 << bit)) for i in range(size)])


def bit_gather(own, axis, size):
    blocks = own[None]
    for b in bit_order(size)[0]:
        blocks = jnp.concatenate([blocks, swap_bit(blocks, axis, size, b)], axis=0)
    return blocks


def bit_scatter(parts, axis, size, after_first):
    me = lax.axis_index(axis)
    for b in reversed(bit_order(size)[0]):
        half = parts.shape[0] // 2
        upper = ((me >> b) & 1) == 1
        keep = jnp.where(upper, parts[half:], parts[:half])
        send = jnp.where(upper, parts[:half], parts[half:])
        parts = keep + swap_bit(send, axis, size, b)
        if after_first is not None:
            parts, after_first = after_first(parts), None
    return parts[0]


def bit_sum(value, axis, size):
    for b in bit_order(size)[0]:
        value = value + swap_bit(value, axis, size, b)
    return value


def forward_layer(streams, x, mods, weights, gains, attend, plain, side, last):
    qkv, out_t, up, down_t = weights
    if plain is not None:
        normed = [
            (plain[s].astype(F32) * (1.0 + mods[s, 1]) + mods[s, 0]).astype(BF16)
            for s in range(2)
        ]
    else:
        normed = streams.gather(
            [modulate(x[s], mods[s, 0], mods[s, 1]).astype(BF16) for s in range(2)]
        )
    raw = side.open([mm(normed[s], qkv[s]).astype(BF16) for s in range(2)])
    o_image, o_text, lse = attend(raw[0], raw[1], gains)
    mixed = side.close((o_image, o_text))
    branch = streams.scatter([mm_nt(mixed[s], out_t[s]) for s in range(2)])
    middle = [x[s] + mods[s, 2] * branch[s] for s in range(2)]
    second = streams.gather(
        [modulate(middle[s], mods[s, 3], mods[s, 4]).astype(BF16) for s in range(2)]
    )
    second = side.open(second)
    hidden = [mm(second[s], up[s]) for s in range(2)]
    active = side.close([gelu(hidden[s]).astype(BF16) for s in range(2)])
    hidden = [hidden[s].astype(BF16) for s in range(2)]
    result = streams.scatter_side([mm_nt(active[s], down_t[s]) for s in range(2)])
    saved = (x, normed, raw, mixed, lse, branch, middle, second, hidden, active)
    if last:
        return None, saved, result
    result = result.result()
    return [middle[s] + mods[s, 5] * result[s] for s in range(2)], saved, result


def backward_layer(streams, gy, dm, saved, mods, weights, gains, calls, side, last):
    qkv, out_t, up, down_t = weights
    x, normed, raw, mixed, lse, branch, middle, second, hidden, active = saved
    if dm is None:
        dm = streams.gather([(mods[s, 5] * gy[s]).astype(BF16) for s in range(2)])
    dm = side.open(dm)
    du = []
    for s in range(2):
        _, pull = jax.vjp(gelu, hidden[s].astype(F32))
        du.append(pull(mm(dm[s], down_t[s]))[0].astype(BF16))
    d_second = side.close([mm_nt(du[s], up[s]).astype(BF16) for s in range(2)])
    d_second = streams.scatter_side(d_second)
    du = d_second.close(d_second.open(du))
    late = [mm_tn(second[s], du[s]) for s in range(2)]
    late += [mm_tn(dm[s], active[s]) for s in range(2)]
    reduced_mlp = calls.reduce_grad(jnp.stack([part.astype(BF16) for part in late]))
    d_second = calls.settle(d_second.result())
    d_middle, d_shift2, d_scale2 = [], [], []
    for s in range(2):
        inner, d_shift, d_scale = modulate_back(middle[s], d_second[s], mods[s, 4])
        d_middle.append(gy[s] + inner)
        d_shift2.append(d_shift)
        d_scale2.append(d_scale)
    d_gate1 = [jnp.sum(d_middle[s] * branch[s], axis=0) for s in range(2)]
    da = streams.gather_side([(mods[s, 2] * d_middle[s]).astype(BF16) for s in range(2)])
    early = d_gate1, d_shift2, d_scale2
    if last:
        da = calls.before_end(early, da)
    else:
        da = da.result()
    d_mixed = side.open([mm(da[s], out_t[s]).astype(BF16) for s in range(2)])
    late = jnp.stack([mm_tn(da[s], mixed[s]).astype(BF16) for s in range(2)])
    reduced_out = calls.reduce_grad(late)
    d_image, d_text, gain_rows = calls.attend_back(
        raw[0], raw[1], gains, mixed[0], mixed[1], d_mixed[0], d_mixed[1], lse
    )
    d_raw = side.close((d_image, d_text))
    if last:
        late = jnp.stack([mm_tn(normed[s], d_raw[s]).astype(BF16) for s in range(2)])
        d_raw, late = tie(d_raw, late)
        d_first = [mm_nt(d_raw[s], qkv[s]).astype(BF16) for s in range(2)]
        d_first, reduced_mlp[0] = tie(d_first, reduced_mlp[0])
        d_first = streams.scatter_side(d_first)
    else:
        d_first = streams.scatter_side([mm_nt(d_raw[s], qkv[s]) for s in range(2)])
        d_raw = d_first.close(d_first.open(d_raw))
        late = jnp.stack([mm_tn(normed[s], d_raw[s]).astype(BF16) for s in range(2)])
    reduced_qkv = calls.reduce_grad(late)
    if last:
        for _ in range(2):
            calls.shared = d_first.close(d_first.open(calls.shared))
    d_first = d_first.result()
    if not last:
        d_first, reduced_mlp[0] = tie(d_first, reduced_mlp[0])
        calls.pending = [reduced_qkv, reduced_out]
    gx, late = [], []
    for s in range(2):
        inner, d_shift, d_scale = modulate_back(x[s], d_first[s], mods[s, 1])
        gx.append(d_middle[s] + inner)
        late += [d_shift, d_scale]
    return gx, early, gain_rows, late, (reduced_qkv, reduced_out, reduced_mlp)


class Calls:
    def __init__(self, attend_back, dp_axis):
        self.attend_back, self.axis, self.pending = attend_back, dp_axis, []
        self.before_end = self.shared = None

    def reduce_grad(self, grad):
        return [lax.psum_scatter(grad, self.axis, scatter_dimension=1, tiled=True)]

    def settle(self, token):
        for box in self.pending:
            token, box[0] = tie(token, box[0])
        self.pending = []
        return token


def on_device(dp, seq, width_of_group, *args):
    (
        image_in,
        text_input,
        condition,
        ada_weight,
        qkv_weight,
        out_weight,
        up_weight,
        down_weight,
        norm_gain,
        image_cotangent,
        text_cotangent,
    ) = args
    dp_axis, dp_size = dp
    seq_axis, seq_size = seq
    layers = qkv_weight.shape[0]
    width = image_in.shape[2]
    streams = Streams(image_in.shape[1], text_input.shape[1], seq_axis, seq_size)
    attend, attend_back = (
        (attention_forward, attention_backward)
        if width_of_group % 128 == 0
        else (plain_forward, plain_backward)
    )
    rows = qkv_weight.shape[2]

    act_cond, silu_pull = jax.vjp(jax.nn.silu, condition.astype(F32))
    act_low = act_cond.astype(BF16)
    partial_mods = jnp.einsum("nd,lsde->nlse", act_low, ada_weight, preferred_element_type=F32)
    x = [image_in[0].astype(F32), text_input[0].astype(F32)]
    plain = streams.gather_side([layer_stats(part)[0].astype(BF16) for part in x])
    plain.state = plain.steps.pop(0)(plain.state)

    given = [qkv_weight]

    def beside_tokens(parts):
        parts, plain.state, given[0] = tie(parts, plain.state, given[0])
        return parts

    own_mods = partial_mods.reshape(dp_size, -1)
    own_mods = bit_scatter(own_mods, dp_axis, dp_size, beside_tokens)
    plain = plain.result()
    qkv_weight, others = given[0], (out_weight, up_weight, down_weight)
    own_mods, plain, others = tie(own_mods, plain, others)
    out_weight, up_weight, down_weight = others

    def fetch(local):
        return lax.all_gather(local, dp_axis, axis=1, tiled=True)

    qkv_local = qkv_weight.reshape(layers, 2, rows, 3, -1, width_of_group)
    qkv_local = qkv_local.transpose(0, 1, 2, 4, 3, 5).reshape(layers, 2, rows, -1)
    out_local = out_weight.transpose(0, 1, 3, 2)
    down_local = down_weight.transpose(0, 1, 3, 2)
    weights = [
        tuple(fetch(w[l]) for w in (qkv_local, out_local, up_weight, down_local))
        for l in range(layers)
    ]

    own_mods = bit_sum(own_mods, seq_axis, seq_size).reshape(layers, 2, 6, width)
    gains_all = norm_gain.astype(F32)
    gain_columns = [gains_all[l].transpose(1, 0, 2).reshape(4, HEAD).T for l in range(layers)]

    gy = [image_cotangent[0].astype(F32), text_cotangent[0].astype(F32)]
    side = streams.gather_side(
        [(own_mods[layers - 1, s, 5] * gy[s]).astype(BF16) for s in range(2)]
    )
    saved_list, results = [], []
    for l in range(layers):
        x, saved, result = forward_layer(
            streams,
            x,
            own_mods[l],
            weights[l],
            gain_columns[l],
            attend,
            None if l else plain,
            side,
            l == layers - 1,
        )
        saved_list.append(saved)
        results.append(result)
    dm, side = side.result(), results[-1]

    def share(values):
        return bit_gather(bit_sum(values, seq_axis, seq_size), dp_axis, dp_size)

    gys, early_all, late_all = [None] * layers, [None] * layers, [None] * layers
    grads, gain_all, stacked = [None] * layers, [None] * layers, [None] * layers

    def before_end(early, gather):
        early_all[0] = early
        results[-1] = side.result()
        layer_rows = []
        for l in range(layers):
            d_gate2 = [jnp.sum(gys[l][s] * results[l][s], axis=0) for s in range(2)]
            if l:
                layer_rows.append((stacked[l][0], d_gate2))
                continue
            d_gate1, d_shift2, d_scale2 = early_all[l]
            none = jnp.zeros_like(d_gate2[0])
            layer_rows.append(
                [
                    [none, none, d_gate1[s], d_shift2[s], d_scale2[s], d_gate2[s]]
                    for s in range(2)
                ]
            )
        layer_rows = gather.close(gather.open(layer_rows))
        rows = [jnp.stack([jnp.stack(r) for r in layer_rows[0]])]
        for five, d_gate2 in layer_rows[1:]:
            rows.append(jnp.concatenate([five, jnp.stack(d_gate2)[:, None]], axis=1))
        rows = jnp.stack(rows)
        token, calls.shared = tie(gather.result(), rows)
        return token

    calls = Calls(attend_back, dp_axis)
    calls.before_end = before_end
    for l in reversed(range(layers)):
        gys[l] = gy
        gy, early_all[l], gain_all[l], late_all[l], grads[l] = backward_layer(
            streams,
            gy,
            dm,
            saved_list[l],
            own_mods[l],
            weights[l],
            gain_columns[l],
            calls,
            side,
            l == 0,
        )
        dm = None
        if l:
            parts = zip(late_all[l][::2], late_all[l][1::2], *early_all[l])
            stacked[l] = [jnp.stack([jnp.stack(part) for part in parts])]
            calls.pending.append(stacked[l])
    last_middle = saved_list[-1][6]
    outputs = [
        (last_middle[s] + own_mods[layers - 1, s, 5] * results[-1][s]).astype(BF16)[None]
        for s in range(2)
    ]

    there = jnp.array(bit_order(dp_size)[1], jnp.int32) ^ lax.axis_index(dp_axis)
    late_all[0], grads[0], gain_all = tie(late_all[0], grads[0], gain_all)
    rest = share(jnp.stack([jnp.stack(late_all[0][:2]), jnp.stack(late_all[0][2:])]))
    total_mods, total_gains = share(calls.shared), share(jnp.stack(gain_all))
    first = jnp.concatenate([rest, total_mods[:, 0, :, 2:]], axis=2)
    total_mods = jnp.concatenate([first[:, None], total_mods[:, 1:]], axis=1)
    total_mods = total_mods.reshape(dp_size, layers, 2, 6 * width)
    total_gains = jnp.sum(total_gains[there], axis=0)[:, :, :4]
    total_gains = total_gains.reshape(layers, HEAD, 2, 2).transpose(0, 3, 2, 1)
    act_there = act_low.astype(F32)[there]
    ada_grad = jnp.einsum("nd,nlse->lsde", act_there, total_mods, precision=HIGHEST)
    d_act = jnp.einsum("nlse,lsde->nd", total_mods, ada_weight.astype(F32), precision=HIGHEST)
    condition_grad = silu_pull(d_act[there])[0]

    def pieces(kind, first):
        return jnp.stack([grads[l][kind][0][first : first + 2] for l in range(layers)]).astype(F32)

    qkv_grad = pieces(0, 0).reshape(layers, 2, rows, -1, 3, width_of_group)
    qkv_grad = qkv_grad.transpose(0, 1, 2, 4, 3, 5).reshape(qkv_weight.shape)
    return (
        outputs[0],
        outputs[1],
        gy[0][None],
        gy[1][None],
        condition_grad,
        ada_grad,
        qkv_grad,
        pieces(1, 0).transpose(0, 1, 3, 2),
        pieces(2, 0),
        pieces(2, 2).transpose(0, 1, 3, 2),
        total_gains,
    )


def solution(mesh):
    tokens = P("dp", "seq", None)
    placed = (
        tokens,
        tokens,
        P(None, ("dp", "seq")),
        P(None, None, ("dp", "seq"), None),
        P(None, None, "dp", None, "seq"),
        P(None, None, "seq", "dp"),
        P(None, None, "dp", "seq"),
        P(None, None, "seq", "dp"),
        P(),
        tokens,
        tokens,
    )
    results = (tokens, tokens, tokens, tokens) + placed[2:8] + (P(),)

    def step(*args):
        heads = args[4].shape[4] // mesh.shape["seq"] // HEAD
        group = 2 * HEAD if heads % 2 == 0 else HEAD
        body = functools.partial(
            on_device, ("dp", mesh.shape["dp"]), ("seq", mesh.shape["seq"]), group
        )
        return jax.shard_map(
            body, mesh=mesh, in_specs=placed, out_specs=results, check_vma=False
        )(*args)

    return step
```
